32 devices in a mesh: group: 2 (over y), ctx: 4 (over z), exp: 4 (over x, core).
Axes of the slice: x: 2, y: 2, z: 4, core: 2. Of those that a mesh axis runs over, the one named last changes fastest.
Arguments:
- queries: bfloat16 [512, 4096], P(('group', 'ctx'), 'exp'), parts along dimension 0, may hold values from -6 to 6
- new_keys: bfloat16 [512, 1024], P(('group', 'ctx'), 'exp'), parts along dimension 0, may hold values from -6 to 6
- new_values: bfloat16 [512, 1024], P(('group', 'ctx'), 'exp'), parts along dimension 0, may hold values from -6 to 6
- cache_keys: bfloat16 [2048, 1024], P(('group', 'ctx'), 'exp'), parts along dimension 0, may hold values from -6 to 6
- cache_values: bfloat16 [2048, 1024], P(('group', 'ctx'), 'exp'), parts along dimension 0, may hold values from -6 to 6
- offset: int32 [2], P('group'), parts along dimension 0, may hold values from 512 to 1024
- token_ids: int32 [512], P(('group', 'ctx')), parts along dimension 0, may hold values from 0 to 128255, as said below
- expert_table: int32 [256512], P('group'), parts along dimension 0, may hold values from 0 to 3
- norm_gain: float32 [4096], replicated, may hold values from 0.5 to 1.5
- w_gate: bfloat16 [4, 4096, 1792], P('exp', None, 'ctx'), may hold values from -0.09375 to 0.09375
- w_up: bfloat16 [4, 4096, 1792], P('exp', None, 'ctx'), may hold values from -0.09375 to 0.09375
- w_down: bfloat16 [4, 1792, 4096], P('exp', 'ctx'), may hold values from -0.125 to 0.125
Outputs:
- mixed: bfloat16 [512, 4096], P(('group', 'ctx'), 'exp'), parts along dimension 0
The draws below stay inside these ranges and needn't reach their ends.
There are 2 independent parts, one for each index of `group`. The reference program is written for one: setup_inputs(seed, part) draws one part's arguments, and reference() takes and returns one part's arrays. A program takes and returns all parts, laid end to end along the dimension named above; an argument that names none is the same for every part. Nothing has to cross between parts.
Inputs may be any that keep to these rules, and one draw needn't show every extreme that they name: Cache positions at or beyond offset are not yet filled. `token_ids`: in every block of 64 consecutive stretch tokens (one block per index of ctx) at most 32 tokens map to one expert through expert_table, and one expert takes exactly 32 tokens of every block.
All inputs are finite; a program needn't handle non-finite values.
Results may differ from the reference program's by a relative error of at most 0.025.
Values may be sent and summed in bfloat16 or wider, within the bound.
No kernel may reach another device: no remote copies, remote signals or barrier semaphores. Data moves between devices by JAX's collectives and lax.ppermute only.
A program may use at most 128 MiB of HBM per device.

```python
import math
import jax
import jax.numpy as jnp
from jax import lax

HEADS = 32
KV_HEADS = 8
HEAD_DIM = 128
VOCAB = 128256
FF_DEV = 448
Q_DEV = 64
D = 4096
CAP = 32
STRETCH = 256
CACHE = 1024
EXPERTS = 4
FF = 1792
N_CTX = 4


def drawn_field(key, shape):
    return jnp.clip(jax.random.normal(key, shape, jnp.float32), -6.0, 6.0)


def draw_queries(key, part):
    drawn = drawn_field(jax.random.fold_in(key, 3), (STRETCH, HEADS, HEAD_DIM))
    return drawn.reshape(STRETCH, HEADS * HEAD_DIM).astype(jnp.bfloat16)


def draw_cache_keys(key, part):
    drawn = drawn_field(jax.random.fold_in(key, 4), (CACHE, KV_HEADS, HEAD_DIM))
    return drawn.reshape(CACHE, KV_HEADS * HEAD_DIM).astype(jnp.bfloat16)


def routing_pair(key):
    base = jax.random.fold_in(key, 29)
    table_key, hot_key, rest_key, order_key, pick_key = jax.random.split(base, 5)
    table = jax.random.randint(table_key, (VOCAB,), 0, EXPERTS).astype(jnp.int32)
    table = table.at[:EXPERTS].set(jnp.arange(EXPERTS, dtype=jnp.int32))
    favored = jax.random.randint(hot_key, (), 0, EXPERTS).astype(jnp.int32)
    others = (favored + jax.random.randint(rest_key, (N_CTX, Q_DEV - CAP), 1, EXPERTS)) % EXPERTS
    labels = jnp.concatenate([jnp.full((N_CTX, CAP), favored, jnp.int32), others.astype(jnp.int32)], axis=1)
    orders = jax.vmap(lambda sub_key: jax.random.permutation(sub_key, Q_DEV))(jax.random.split(order_key, N_CTX))
    labels = jnp.take_along_axis(labels, orders, axis=1).reshape(STRETCH)
    candidates = jax.random.randint(pick_key, (STRETCH, 64), EXPERTS, VOCAB).astype(jnp.int32)
    matches = table[candidates] == labels[:, None]
    first = jnp.argmax(matches, axis=1)
    found = jnp.any(matches, axis=1)
    picked_ids = jnp.take_along_axis(candidates, first[:, None], axis=1)[:, 0]
    token_list = jnp.where(found, picked_ids, labels).astype(jnp.int32)
    return (table, token_list)


def draw_token_ids(key, part):
    return routing_pair(key)[1]


def draw_expert_table(key, part):
    return routing_pair(key)[0]


def block_scale(rng, dims, cuts, low, high):
    def one(axis_at, parts):
        draws = jax.random.uniform(jax.random.fold_in(jax.random.fold_in(rng, 6), axis_at), (parts,), jnp.float32, low / len(cuts), high / len(cuts))
        return jnp.repeat(jnp.exp(draws), dims[axis_at] // parts).reshape((-1,) + (1,) * (len(dims) - axis_at - 1))

    gain = one(*cuts[0])
    for cut in cuts[1:]:
        gain = gain * one(*cut)
    return gain


def noise(key, dims, spread, bound, cuts=(), kind=jnp.bfloat16):
    entries = spread * jax.random.normal(key, dims, jnp.float32)
    if cuts:
        entries = entries * block_scale(key, dims, cuts, -0.22, 0.18)
    return jnp.clip(entries, -bound, bound).astype(kind)


def setup_inputs(seed: int = 0, part: int = 0) -> dict:
    seeds = jax.random.split(jax.random.key(seed), 13)
    part_keys = jax.random.split(jax.random.fold_in(seeds[12], part), 13)
    queries = draw_queries(jax.random.fold_in(jax.random.fold_in(seeds[12], part), 71), part)
    new_keys = noise(part_keys[1], (STRETCH, KV_HEADS * HEAD_DIM), 1.0, 6.0, ((0, 4), (1, 4)))
    new_values = noise(part_keys[2], (STRETCH, KV_HEADS * HEAD_DIM), 1.0, 6.0, ((0, 4), (1, 4)))
    cache_keys = draw_cache_keys(jax.random.fold_in(jax.random.fold_in(seeds[12], part), 71), part)
    cache_values = noise(part_keys[4], (CACHE, KV_HEADS * HEAD_DIM), 1.0, 6.0, ((0, 4), (1, 4)))
    offset = jax.random.randint(part_keys[5], (1,), CACHE // 2, CACHE + 1).astype(jnp.int32)
    token_ids = draw_token_ids(jax.random.fold_in(jax.random.fold_in(seeds[12], part), 71), part)
    expert_table = draw_expert_table(jax.random.fold_in(jax.random.fold_in(seeds[12], part), 71), part)
    norm_gain = jnp.clip(1.0 + 0.1 * jax.random.normal(seeds[8], (D,), jnp.float32), 0.5, 1.5)
    w_gate = noise(seeds[9], (EXPERTS, D, FF), D ** -0.5, 0.09375, ((0, 4), (2, 4)))
    w_up = noise(seeds[10], (EXPERTS, D, FF), D ** -0.5, 0.09375, ((0, 4), (2, 4)))
    w_down = noise(seeds[11], (EXPERTS, FF, D), FF ** -0.5, 0.125, ((0, 4), (1, 4)))
    return dict(queries=queries, new_keys=new_keys, new_values=new_values, cache_keys=cache_keys, cache_values=cache_values, offset=offset, token_ids=token_ids, expert_table=expert_table, norm_gain=norm_gain, w_gate=w_gate, w_up=w_up, w_down=w_down)


def reference(queries, new_keys, new_values, cache_keys, cache_values, offset, token_ids, expert_table, norm_gain, w_gate, w_up, w_down):
    group = HEADS // KV_HEADS
    total_keys = CACHE + STRETCH
    grouped = queries.astype(jnp.float32).reshape(STRETCH, KV_HEADS, group, HEAD_DIM)
    key_rows = jnp.concatenate([cache_keys, new_keys], axis=0).astype(jnp.float32).reshape(total_keys, KV_HEADS, HEAD_DIM)
    value_rows = jnp.concatenate([cache_values, new_values], axis=0).astype(jnp.float32).reshape(total_keys, KV_HEADS, HEAD_DIM)
    stretch_index = jnp.arange(STRETCH, dtype=jnp.int32)
    cache_ok = jnp.arange(CACHE, dtype=jnp.int32) < offset[0]
    allowed = jnp.concatenate([jnp.broadcast_to(cache_ok[None, :], (STRETCH, CACHE)), stretch_index[None, :] <= stretch_index[:, None]], axis=1)

    def per_head(head):
        query_head = lax.dynamic_index_in_dim(grouped, head, 1, keepdims=False)
        key_head = lax.dynamic_index_in_dim(key_rows, head, 1, keepdims=False)
        value_head = lax.dynamic_index_in_dim(value_rows, head, 1, keepdims=False)
        scores = jnp.einsum('tgd,sd->tgs', query_head, key_head) * (1.0 / math.sqrt(HEAD_DIM))
        usable = allowed[:, None, :]
        peak = lax.optimization_barrier(jnp.max(jnp.where(usable, scores, -1e+30), axis=-1))
        unnorm = jnp.where(usable, jnp.exp(scores - peak[..., None]), 0.0)
        total = lax.optimization_barrier(jnp.sum(unnorm, axis=-1))
        rounded = lax.optimization_barrier(unnorm.astype(jnp.bfloat16)).astype(jnp.float32)
        numer = jnp.einsum('tgs,sd->tgd', rounded, value_head)
        return numer / total[..., None]
    heads_out = lax.map(per_head, jnp.arange(KV_HEADS, dtype=jnp.int32))
    attended = jnp.transpose(heads_out, (1, 0, 2, 3)).reshape(STRETCH, D).astype(jnp.bfloat16)
    chosen = expert_table[token_ids]
    blocks = chosen.reshape(N_CTX, Q_DEV)
    onehot = (blocks[..., None] == jnp.arange(EXPERTS, dtype=jnp.int32)).astype(jnp.int32)
    earlier = jnp.cumsum(onehot, axis=1) - onehot
    slot = lax.optimization_barrier(jnp.sum(earlier * onehot, axis=-1))
    row_of = (jnp.arange(N_CTX, dtype=jnp.int32)[:, None] * CAP + slot).reshape(STRETCH).astype(jnp.int32)
    values32 = attended.astype(jnp.float32)
    scale = lax.rsqrt(lax.optimization_barrier(jnp.mean(values32 * values32, axis=-1, keepdims=True)) + 1e-05)
    normed = (values32 * scale * norm_gain).astype(jnp.bfloat16)

    def per_expert(carry, which):
        select = chosen == which
        place = jnp.where(select, row_of, N_CTX * CAP).astype(jnp.int32)
        buffer = jnp.zeros((N_CTX * CAP, D), jnp.bfloat16).at[place].set(normed, mode='drop')
        gate_w = lax.dynamic_index_in_dim(w_gate, which, 0, keepdims=False)
        up_w = lax.dynamic_index_in_dim(w_up, which, 0, keepdims=False)
        down_w = lax.dynamic_index_in_dim(w_down, which, 0, keepdims=False)
        gate = jnp.dot(buffer, gate_w, preferred_element_type=jnp.float32)
        upper = jnp.dot(buffer, up_w, preferred_element_type=jnp.float32)
        hidden = (jax.nn.silu(gate) * upper).astype(jnp.bfloat16)

        def add_slice(acc, piece):
            start = (piece * FF_DEV).astype(jnp.int32)
            part_h = lax.dynamic_slice_in_dim(hidden, start, FF_DEV, 1)
            part_w = lax.dynamic_slice_in_dim(down_w, start, FF_DEV, 0)
            partial_sum = jnp.dot(part_h, part_w, preferred_element_type=jnp.float32)
            partial_sum = lax.optimization_barrier(partial_sum.astype(jnp.bfloat16)).astype(jnp.float32)
            return (acc + partial_sum, None)
        summed, _ = lax.scan(add_slice, jnp.zeros((N_CTX * CAP, D), jnp.float32), jnp.arange(N_CTX, dtype=jnp.int32))
        picked = summed[jnp.clip(row_of, 0, N_CTX * CAP - 1)]
        return (carry + jnp.where(select[:, None], picked, 0.0), None)
    expert_out, _ = lax.scan(per_expert, jnp.zeros((STRETCH, D), jnp.float32), jnp.arange(EXPERTS, dtype=jnp.int32))
    return (normed.astype(jnp.float32) + expert_out).astype(jnp.bfloat16)
```

```python
import functools
import math

import jax
import jax.numpy as jnp
from jax import lax
from jax.experimental import pallas as pl
from jax.experimental.pallas import tpu as pltpu
from jax.sharding import PartitionSpec as P

HEADS = 32
KV_HEADS = 8
HEAD_DIM = 128


masked_score = -1e30
f32 = jnp.float32
bf16 = jnp.bfloat16


def split_heads(flat, heads):
    return flat.reshape(flat.shape[0], heads, flat.shape[1] // heads)


def partial_attend(query_rows, key_rows, value_rows, allowed):
    width = query_rows.shape[3]
    scores = jnp.einsum("rkgd,skd->rkgs", query_rows, key_rows, preferred_element_type=jnp.float32)
    scores = scores * (1.0 / math.sqrt(width))
    usable = allowed[:, None, None, :]
    peak = jnp.max(jnp.where(usable, scores, masked_score), axis=-1)
    unnorm = jnp.where(usable, jnp.exp(scores - peak[..., None]), 0.0)
    total = jnp.sum(unnorm, axis=-1)
    numer = jnp.einsum(
        "rkgs,skd->rkgd",
        unnorm.astype(jnp.bfloat16),
        value_rows,
        preferred_element_type=jnp.float32,
    )
    return (numer, peak, total)


def general_path(
    queries,
    new_keys,
    new_values,
    cache_keys,
    cache_values,
    offset,
    token_ids,
    expert_table,
    norm_gain,
    w_gate,
    w_up,
    w_down,
):
    owners = lax.axis_size("exp")
    heads_local = HEADS // owners
    kv_local = KV_HEADS // owners
    group = HEADS // KV_HEADS
    tok_count = queries.shape[0]
    cache_len = cache_keys.shape[0]
    shard = lax.axis_index("ctx")
    limit = offset[0]
    key_rows = jnp.concatenate([cache_keys, new_keys], axis=0)
    value_rows = jnp.concatenate([cache_values, new_values], axis=0)
    span = key_rows.shape[0]
    own_index = shard * tok_count + jnp.arange(tok_count, dtype=jnp.int32)
    grouped = queries.reshape(tok_count, kv_local, group, HEAD_DIM)
    piece_keys = lax.all_gather(key_rows, "ctx", axis=0, tiled=True)
    piece_values = lax.all_gather(value_rows, "ctx", axis=0, tiled=True)
    flat = jnp.arange(piece_keys.shape[0], dtype=jnp.int32)
    source = flat // span
    inner = flat % span
    cache_ok = source * cache_len + inner < limit
    stretch_ok = (source * tok_count + inner - cache_len)[None, :] <= own_index[:, None]
    allowed = jnp.where((inner < cache_len)[None, :], cache_ok[None, :], stretch_ok)
    numer, peak, total = partial_attend(
        grouped, split_heads(piece_keys, kv_local), split_heads(piece_values, kv_local), allowed
    )
    attended = (numer / total[..., None]).reshape(tok_count, heads_local * HEAD_DIM).astype(jnp.bfloat16)
    capacity = tok_count // 2
    chosen = expert_table[token_ids]
    onehot = (chosen[:, None] == jnp.arange(owners, dtype=jnp.int32)[None, :]).astype(jnp.int32)
    earlier = jnp.cumsum(onehot, axis=0) - onehot
    slot = jnp.sum(earlier * onehot, axis=1)
    target = chosen * capacity + slot
    dispatch = (jnp.arange(owners * capacity, dtype=jnp.int32)[:, None] == target[None, :]).astype(
        jnp.bfloat16
    )
    packed = jnp.dot(dispatch, attended, preferred_element_type=jnp.float32).astype(jnp.bfloat16)
    arrived = lax.all_to_all(packed, "exp", split_axis=0, concat_axis=1, tiled=True)
    values32 = arrived.astype(jnp.float32)
    scale = lax.rsqrt(jnp.mean(values32 * values32, axis=-1, keepdims=True) + 1e-05)
    normed = (values32 * scale * norm_gain).astype(jnp.bfloat16)
    piece = lax.all_gather(normed, "ctx", axis=0, tiled=True)
    gate = jnp.dot(piece, w_gate[0], preferred_element_type=jnp.float32)
    upper = jnp.dot(piece, w_up[0], preferred_element_type=jnp.float32)
    hidden = (jax.nn.silu(gate) * upper).astype(jnp.bfloat16)
    summed = lax.psum_scatter(
        jnp.dot(hidden, w_down[0], preferred_element_type=jnp.float32).astype(jnp.bfloat16),
        "ctx",
        scatter_dimension=0,
        tiled=True,
    ).astype(jnp.float32)
    combined = (normed.astype(jnp.float32) + summed).astype(jnp.bfloat16)
    returned = lax.all_to_all(combined, "exp", split_axis=1, concat_axis=0, tiled=True)
    collect = (target[:, None] == jnp.arange(owners * capacity, dtype=jnp.int32)[None, :]).astype(
        jnp.bfloat16
    )
    return jnp.dot(collect, returned, preferred_element_type=jnp.float32).astype(jnp.bfloat16)


def iota(shape, axis):
    return lax.broadcasted_iota(jnp.int32, shape, axis)


def call(kernel, out_shapes, name, mib, scratch=(), smem=0):
    def run(*args):
        vmem = pl.BlockSpec(memory_space=pltpu.VMEM)
        specs = [pl.BlockSpec(memory_space=pltpu.SMEM)] * smem + [vmem] * (len(args) - smem)
        return pl.pallas_call(
            kernel,
            out_shape=[jax.ShapeDtypeStruct(s, d) for s, d in out_shapes],
            in_specs=specs,
            out_specs=[vmem] * len(out_shapes),
            scratch_shapes=list(scratch),
            compiler_params=pltpu.CompilerParams(vmem_limit_bytes=mib << 20),
            name=name,
        )(*args)

    return run


def expert_rows(marks, first, cap):
    tokens = marks.shape[1]
    slots = (iota((cap, tokens), 0) + first).astype(f32)
    return (marks == slots).astype(bf16)


def dot(a, b):
    return jnp.dot(a, b, preferred_element_type=f32)


def dot_nt(a, b):
    return lax.dot_general(a, b, (((1,), (1,)), ((), ())), preferred_element_type=f32)


def dot_tn(a, b):
    return lax.dot_general(a, b, (((0,), (0,)), ((), ())), preferred_element_type=f32)


def pack_kernel(q, nk, nv, ck, cv, chosen, p0, p1):
    z = lax.axis_index("ctx")
    tokens, cache = q.shape[0], ck.shape[0]
    span = cache + tokens
    width = p0.shape[1]
    wide = q.shape[1] // 2
    cap = tokens // 2
    who = chosen[...]
    row = iota(who.shape, 0)
    onehot = (who == row).astype(f32)
    before = (iota((tokens, tokens), 0) < iota((tokens, tokens), 1)).astype(bf16)
    rank = dot(onehot.astype(bf16), before)
    target = jnp.sum(onehot * ((row * cap).astype(f32) + rank), axis=0, keepdims=True)

    def fill(p, h):
        lanes = slice(h * HEAD_DIM, (h + 1) * HEAD_DIM)
        p[0:cache, 0:HEAD_DIM] = ck[:, lanes]
        p[cache:span, 0:HEAD_DIM] = nk[:, lanes]
        p[0:cache, HEAD_DIM:] = cv[:, lanes]
        p[cache:span, HEAD_DIM:] = nv[:, lanes]
        for part in range(wide // width):
            lo = h * wide + part * width
            p[span + part * tokens : span + (part + 1) * tokens, :] = q[:, lo : lo + width]
        top = span + (wide // width) * tokens
        p[top:, :tokens] = jnp.broadcast_to(target, (p.shape[0] - top, tokens)).astype(bf16)

    @pl.when(z < 2)
    def _():
        fill(p0, 0)
        fill(p1, 1)

    @pl.when(z >= 2)
    def _():
        fill(p0, 1)
        fill(p1, 0)


def attend_kernel(cache, tokens, offset, r0, r1, s0, s1, za, xb0, xb1, xb2, xb3, route):
    z, e = lax.axis_index("ctx"), lax.axis_index("exp")
    core = e % 2
    span = cache + tokens
    cap = tokens // 2
    width = r0.shape[1]
    group = HEADS // KV_HEADS
    per_row = width // HEAD_DIM
    top = span + (group // per_row) * tokens
    limit = offset[0]
    scale = 1.0 / math.sqrt(HEAD_DIM)
    halves = (z % 2, 1 - z % 2)
    keys = [(r, 2 * hi + core) for r, hi in zip((r0, r1), halves)]
    keys += [(s, 2 * hi + 1 - core) for s, hi in zip((s0, s1), halves)]
    rows = group * tokens
    pos = iota((rows, span), 0) % tokens
    col = iota((rows, span), 1)
    for ref, block in keys:
        route[block] = ref[top:, :tokens].astype(f32)
    for r, hi in zip((r0, r1), halves):
        base = (2 * hi + core) * tokens
        q = jnp.concatenate(
            [
                r[span + (g // per_row) * tokens : span + (g // per_row + 1) * tokens,
                  (g % per_row) * HEAD_DIM : (g % per_row + 1) * HEAD_DIM]
                for g in range(group)
            ],
            axis=0,
        )
        scores = []
        for ref, block in keys:
            s = dot_nt(q, ref[0:span, 0:HEAD_DIM]) * scale
            edge = jnp.where(col < cache, limit - block * cache, pos + (base - block * tokens + cache + 1))
            scores.append(jnp.where(col < edge, s, masked_score))
        peak = functools.reduce(jnp.maximum, [jnp.max(s, axis=1, keepdims=True) for s in scores])
        total = jnp.zeros((rows, 1), f32)
        numer = jnp.zeros((rows, HEAD_DIM), f32)
        for (ref, _), s in zip(keys, scores):
            w = jnp.exp(s - peak)
            total += jnp.sum(w, axis=1, keepdims=True)
            numer += dot(w.astype(bf16), ref[0:span, HEAD_DIM:])
        out = (numer / total).astype(bf16)
        for g in range(group - 1):
            za[hi, :, g * HEAD_DIM : (g + 1) * HEAD_DIM] = out[g * tokens : (g + 1) * tokens]
        last = out[(group - 1) * tokens :]
        marks = r[top : top + 1, :tokens].astype(f32)
        for m, xb in enumerate((xb0, xb1, xb2, xb3)):
            xb[hi] = dot(expert_rows(marks, (e ^ m) * cap, cap), last).astype(bf16)


def regroup_kernel(route, a0, a1, a2, a3, b0, b1, b2, b3, c0, c1, c2, c3, zd):
    e = lax.axis_index("exp")
    core = e % 2
    cap = b0.shape[1]
    for j in range(2):
        marks = route[2 * j + core][0:1]
        pick = jnp.concatenate([expert_rows(marks, (e ^ m) * cap, cap) for m in range(4)], axis=0)
        for n, a in enumerate((a0, a1, a2, a3)):
            got = dot(pick, a[j]).astype(bf16)
            for m, c in enumerate((c0, c1, c2, c3)):
                c[n, j] = got[m * cap : (m + 1) * cap]
    for m, b in enumerate((b0, b1, b2, b3)):
        src = e ^ m
        for j in range(2):
            zd[src // 2, 2 * j + src % 2] = b[j]


def expert_kernel(
    c0, c1, c2, c3, d0, d1, d2, d3, gain, wg, wu, wd,
    y0, y1, y2, y3, t0, t1, t2, t3, xs, ns, ys,
):
    z, e = lax.axis_index("ctx"), lax.axis_index("exp")
    slices, blocks, cap, wide = xs.shape
    part = c0.shape[3]
    rows = blocks * cap
    for m, c in enumerate((c0, c1, c2, c3)):
        src = e ^ m
        for n in range(4):
            for j in range(2):
                xs[4 * (src // 2) + (z ^ n), 2 * j + src % 2, :, 0:part] = c[n, j]
    for m, d in enumerate((d0, d1, d2, d3)):
        for x in range(2):
            xs[4 * x + (z ^ m), :, :, part:] = d[x]
    total = jnp.zeros((rows, 1), f32)
    for s in range(slices):
        v = xs[s].reshape(rows, wide).astype(f32)
        total += jnp.sum(v * v, axis=1, keepdims=True)
    scale = lax.rsqrt(total * (1.0 / (slices * wide)) + 1e-05)
    for s in range(slices):
        v = xs[s].reshape(rows, wide).astype(f32)
        lanes = slice(s * wide, (s + 1) * wide)
        ns[:, lanes] = (v * scale * gain[0:1, lanes]).astype(bf16)
    normed = ns[...]
    gate = dot_nt(normed, wg[...])
    upper = dot_nt(normed, wu[...])
    hidden = (gate / (1.0 + jnp.exp(-gate)) * upper).astype(bf16)
    owners = ys.shape[0]
    span = ys.shape[2]
    mine = iota((rows, span), 0) // cap == z
    for o in range(owners):
        lanes = slice(o * span, (o + 1) * span)
        v = dot(hidden, wd[:, lanes])
        ys[o] = (v + jnp.where(mine, ns[:, lanes].astype(f32), 0.0)).astype(bf16)
    keep = y0.shape[1]
    for m, (y, t) in enumerate(zip((y0, y1, y2, y3), (t0, t1, t2, t3))):
        y[...] = ys[e ^ m, :, 0:keep]
        for o in range(owners):
            t[o] = ys[o, pl.ds(pl.multiple_of((z ^ m) * cap, cap), cap), keep:]


def turn_kernel(route, y0, y1, y2, y3, t0, t1, t2, t3, g0, g1, g2, g3, h0, h1, h2, h3, ts):
    z, e = lax.axis_index("ctx"), lax.axis_index("exp")
    cap = h0.shape[0]
    for m, g in enumerate((g0, g1, g2, g3)):
        block = z ^ m
        marks = route[block][0:1]
        pick = jnp.concatenate([expert_rows(marks, (e ^ n) * cap, cap) for n in range(4)], axis=0)
        at = pl.ds(pl.multiple_of(block * cap, cap), cap)
        got = jnp.concatenate([y[at, :] for y in (y0, y1, y2, y3)], axis=0)
        g[...] = dot_tn(pick, got).astype(bf16)
    ts[...] = sum(t[...].astype(f32) for t in (t0, t1, t2, t3)).astype(bf16)
    for m, h in enumerate((h0, h1, h2, h3)):
        h[...] = ts[e ^ m]


def final_kernel(route, g0, g1, g2, g3, h0, h1, h2, h3, out):
    z, e = lax.axis_index("ctx"), lax.axis_index("exp")
    cap = h0.shape[0]
    keep = g0.shape[1]
    out[:, 0:keep] = sum(g[...].astype(f32) for g in (g0, g1, g2, g3)).astype(bf16)
    marks = route[z][0:1]
    pick = jnp.concatenate([expert_rows(marks, (e ^ n) * cap, cap) for n in range(4)], axis=0)
    got = jnp.concatenate([h[...] for h in (h0, h1, h2, h3)], axis=0)
    out[:, keep:] = dot_tn(pick, got).astype(bf16)


def paired_path(
    queries,
    new_keys,
    new_values,
    cache_keys,
    cache_values,
    offset,
    token_ids,
    expert_table,
    norm_gain,
    w_gate,
    w_up,
    w_down,
):
    n_ctx, n_exp = lax.axis_size("ctx"), lax.axis_size("exp")
    tokens = queries.shape[0]
    cache = cache_keys.shape[0]
    width = new_keys.shape[1]
    group = HEADS // KV_HEADS
    wide = group * HEAD_DIM
    cap = tokens // 2
    span = cache + tokens
    part = wide - HEAD_DIM
    own = queries.shape[1]
    back = own * 3 // 8
    keep = own - back
    rows = n_ctx * cap

    def over_ctx(v, m):
        return lax.ppermute(v, "ctx", [(i, i ^ m) for i in range(n_ctx)])

    def over_exp(v, m):
        return lax.ppermute(v, "exp", [(i, i ^ m) for i in range(n_exp)])

    def head_step(v, o):
        pairs = []
        for z in range(n_ctx):
            for e in range(n_exp):
                core = e % 2
                to_z = 2 * core + ((z // 2) ^ o)
                pairs.append((z * n_exp + e, to_z * n_exp + e - core + z % 2))
        return lax.ppermute(v, ("ctx", "exp"), pairs)

    chosen = expert_table.at[token_ids].get(mode="promise_in_bounds")
    chosen = jnp.broadcast_to(chosen[None, :], (8, tokens))
    height = span + tokens * wide // width + 16
    p0, p1 = call(pack_kernel, [((height, width), bf16)] * 2, "pack", 8)(
        queries, new_keys, new_values, cache_keys, cache_values, chosen
    )
    r0, r1 = head_step(p0, 0), head_step(p1, 1)
    s0, s1 = over_exp(r0, 1), over_exp(r1, 1)
    za, xb0, xb1, xb2, xb3, route = call(
        functools.partial(attend_kernel, cache, tokens),
        [((2, tokens, part), bf16)] + [((2, cap, HEAD_DIM), bf16)] * 4 + [((n_ctx, 16, tokens), f32)],
        "attend",
        16,
        smem=1,
    )(offset, r0, r1, s0, s1)
    a = [za] + [over_ctx(za, m) for m in (1, 2, 3)]
    b = [xb0] + [over_exp(v, m) for m, v in ((1, xb1), (2, xb2), (3, xb3))]
    c0, c1, c2, c3, zd = call(
        regroup_kernel,
        [((4, 2, cap, part), bf16)] * 4 + [((2, n_ctx, cap, HEAD_DIM), bf16)],
        "regroup",
        8,
    )(route, *a, *b)
    c = [c0] + [over_exp(v, m) for m, v in ((1, c1), (2, c2), (3, c3))]
    d = [zd] + [over_ctx(zd, m) for m in (1, 2, 3)]
    outs = call(
        expert_kernel,
        [((rows, keep), bf16)] * 4 + [((n_exp, cap, back), bf16)] * 4,
        "expert",
        28,
        scratch=[
            pltpu.VMEM((KV_HEADS, n_ctx, cap, wide), bf16),
            pltpu.VMEM((rows, KV_HEADS * wide), bf16),
            pltpu.VMEM((n_exp, rows, own), bf16),
        ],
    )(
        *c,
        *d,
        norm_gain.reshape(1, -1),
        jnp.swapaxes(w_gate[0], 0, 1),
        jnp.swapaxes(w_up[0], 0, 1),
        w_down[0],
    )
    y, t = outs[:4], outs[4:]
    t = [t[0]] + [over_ctx(t[m], m) for m in (1, 2, 3)]
    y = [y[0]] + [over_exp(y[m], m) for m in (1, 2, 3)]
    outs = call(
        turn_kernel,
        [((tokens, keep), bf16)] * 4 + [((cap, back), bf16)] * 4,
        "turn",
        8,
        scratch=[pltpu.VMEM((n_exp, cap, back), bf16)],
    )(route, *y, *t)
    g, h = outs[:4], outs[4:]
    g = [g[0]] + [over_ctx(g[m], m) for m in (1, 2, 3)]
    h = [h[0]] + [over_exp(h[m], m) for m in (1, 2, 3)]
    (out,) = call(final_kernel, [((tokens, own), bf16)], "final", 8)(route, *g, *h)
    return out


def solution(mesh):
    placed = (
        P(("group", "ctx"), "exp"),
        P(("group", "ctx"), "exp"),
        P(("group", "ctx"), "exp"),
        P(("group", "ctx"), "exp"),
        P(("group", "ctx"), "exp"),
        P("group"),
        P(("group", "ctx")),
        P("group"),
        P(),
        P("exp", None, "ctx"),
        P("exp", None, "ctx"),
        P("exp", "ctx", None),
    )
    n_ctx, n_exp = mesh.shape["ctx"], mesh.shape["exp"]
    paired = n_ctx == n_exp == 4 and KV_HEADS == 2 * n_exp
    return jax.shard_map(
        paired_path if paired else general_path,
        mesh=mesh,
        in_specs=placed,
        out_specs=P(("group", "ctx"), "exp"),
        check_vma=False,
    )
```

```python
import functools
import math

import jax
import jax.numpy as jnp
from jax import lax
from jax.experimental import pallas as pl
from jax.experimental.pallas import tpu as pltpu
from jax.sharding import PartitionSpec as P

HEADS = 32
KV_HEADS = 8
HEAD_DIM = 128


masked_score = -1e30
f32 = jnp.float32
bf16 = jnp.bfloat16


def split_heads(flat, heads):
    return flat.reshape(flat.shape[0], heads, flat.shape[1] // heads)


def partial_attend(query_rows, key_rows, value_rows, allowed):
    width = query_rows.shape[3]
    scores = jnp.einsum("rkgd,skd->rkgs", query_rows, key_rows, preferred_element_type=jnp.float32)
    scores = scores * (1.0 / math.sqrt(width))
    usable = allowed[:, None, None, :]
    peak = jnp.max(jnp.where(usable, scores, masked_score), axis=-1)
    unnorm = jnp.where(usable, jnp.exp(scores - peak[..., None]), 0.0)
    total = jnp.sum(unnorm, axis=-1)
    numer = jnp.einsum(
        "rkgs,skd->rkgd",
        unnorm.astype(jnp.bfloat16),
        value_rows,
        preferred_element_type=jnp.float32,
    )
    return (numer, peak, total)


def general_path(
    queries,
    new_keys,
    new_values,
    cache_keys,
    cache_values,
    offset,
    token_ids,
    expert_table,
    norm_gain,
    w_gate,
    w_up,
    w_down,
):
    owners = lax.axis_size("exp")
    heads_local = HEADS // owners
    kv_local = KV_HEADS // owners
    group = HEADS // KV_HEADS
    tok_count = queries.shape[0]
    cache_len = cache_keys.shape[0]
    shard = lax.axis_index("ctx")
    limit = offset[0]
    key_rows = jnp.concatenate([cache_keys, new_keys], axis=0)
    value_rows = jnp.concatenate([cache_values, new_values], axis=0)
    span = key_rows.shape[0]
    own_index = shard * tok_count + jnp.arange(tok_count, dtype=jnp.int32)
    grouped = queries.reshape(tok_count, kv_local, group, HEAD_DIM)
    piece_keys = lax.all_gather(key_rows, "ctx", axis=0, tiled=True)
    piece_values = lax.all_gather(value_rows, "ctx", axis=0, tiled=True)
    flat = jnp.arange(piece_keys.shape[0], dtype=jnp.int32)
    source = flat // span
    inner = flat % span
    cache_ok = source * cache_len + inner < limit
    stretch_ok = (source * tok_count + inner - cache_len)[None, :] <= own_index[:, None]
    allowed = jnp.where((inner < cache_len)[None, :], cache_ok[None, :], stretch_ok)
    numer, peak, total = partial_attend(
        grouped, split_heads(piece_keys, kv_local), split_heads(piece_values, kv_local), allowed
    )
    attended = (numer / total[..., None]).reshape(tok_count, heads_local * HEAD_DIM).astype(jnp.bfloat16)
    capacity = tok_count // 2
    chosen = expert_table[token_ids]
    onehot = (chosen[:, None] == jnp.arange(owners, dtype=jnp.int32)[None, :]).astype(jnp.int32)
    earlier = jnp.cumsum(onehot, axis=0) - onehot
    slot = jnp.sum(earlier * onehot, axis=1)
    target = chosen * capacity + slot
    dispatch = (jnp.arange(owners * capacity, dtype=jnp.int32)[:, None] == target[None, :]).astype(
        jnp.bfloat16
    )
    packed = jnp.dot(dispatch, attended, preferred_element_type=jnp.float32).astype(jnp.bfloat16)
    arrived = lax.all_to_all(packed, "exp", split_axis=0, concat_axis=1, tiled=True)
    values32 = arrived.astype(jnp.float32)
    scale = lax.rsqrt(jnp.mean(values32 * values32, axis=-1, keepdims=True) + 1e-05)
    normed = (values32 * scale * norm_gain).astype(jnp.bfloat16)
    piece = lax.all_gather(normed, "ctx", axis=0, tiled=True)
    gate = jnp.dot(piece, w_gate[0], preferred_element_type=jnp.float32)
    upper = jnp.dot(piece, w_up[0], preferred_element_type=jnp.float32)
    hidden = (jax.nn.silu(gate) * upper).astype(jnp.bfloat16)
    summed = lax.psum_scatter(
        jnp.dot(hidden, w_down[0], preferred_element_type=jnp.float32).astype(jnp.bfloat16),
        "ctx",
        scatter_dimension=0,
        tiled=True,
    ).astype(jnp.float32)
    combined = (normed.astype(jnp.float32) + summed).astype(jnp.bfloat16)
    returned = lax.all_to_all(combined, "exp", split_axis=1, concat_axis=0, tiled=True)
    collect = (target[:, None] == jnp.arange(owners * capacity, dtype=jnp.int32)[None, :]).astype(
        jnp.bfloat16
    )
    return jnp.dot(collect, returned, preferred_element_type=jnp.float32).astype(jnp.bfloat16)


def iota(shape, axis):
    return lax.broadcasted_iota(jnp.int32, shape, axis)


def call(kernel, out_shapes, name, mib, scratch=(), hbm=0, cost=None):
    def run(*args):
        args = [pltpu.with_memory_space_constraint(v, pltpu.HBM) if i < hbm else v for i, v in enumerate(args)]
        vmem = pl.BlockSpec(memory_space=pltpu.VMEM)
        specs = [pl.BlockSpec(memory_space=pltpu.HBM)] * hbm + [vmem] * (len(args) - hbm)
        return pl.pallas_call(
            kernel,
            out_shape=[jax.ShapeDtypeStruct(s, d) for s, d in out_shapes],
            in_specs=specs,
            out_specs=[vmem] * len(out_shapes),
            scratch_shapes=list(scratch),
            compiler_params=pltpu.CompilerParams(vmem_limit_bytes=mib << 20),
            cost_estimate=cost,
            name=name,
        )(*args)

    return run


def expert_rows(marks, first, cap):
    tokens = marks.shape[1]
    slots = (iota((cap, tokens), 0) + first).astype(f32)
    return (marks == slots).astype(bf16)


def dot(a, b):
    return jnp.dot(a, b, preferred_element_type=f32)


def dot_nt(a, b):
    return lax.dot_general(a, b, (((1,), (1,)), ((), ())), preferred_element_type=f32)


def dot_tn(a, b):
    return lax.dot_general(a, b, (((0,), (0,)), ((), ())), preferred_element_type=f32)


def pack_kernel(q, nk, nv, ck, cv, ids, table, p0, p1, id_row, id_smem, found, sems, row_sems):
    z = lax.axis_index("ctx")
    tokens, cache = q.shape[0], ck.shape[0]
    span = cache + tokens
    width = p0.shape[1]
    wide = q.shape[1] // 2
    cap = tokens // 2
    top = span + (wide // width) * tokens
    lanes = found.shape[1]
    swap = (z // 2) == 1

    first = [
        pltpu.make_async_copy(ids, id_smem, sems.at[0]),
        pltpu.make_async_copy(ids, id_row.at[0], sems.at[1]),
    ]
    for copy in first:
        copy.start()

    def pieces(p, h, base):
        at = pl.ds(h * HEAD_DIM, HEAD_DIM)
        moves = [
            (ck.at[:, at], p.at[0:cache, 0:HEAD_DIM]),
            (cv.at[:, at], p.at[0:cache, HEAD_DIM:]),
            (nk.at[:, at], p.at[cache:span, 0:HEAD_DIM]),
            (nv.at[:, at], p.at[cache:span, HEAD_DIM:]),
        ]
        for part in range(wide // width):
            lo = h * wide + part * width
            moves.append((q.at[:, pl.ds(lo, width)], p.at[span + part * tokens : span + (part + 1) * tokens, :]))
        return [pltpu.make_async_copy(src, dst, sems.at[base + i]) for i, (src, dst) in enumerate(moves)]

    count = 4 + wide // width

    @pl.when(jnp.logical_not(swap))
    def _():
        for copy in pieces(p0, 0, 2) + pieces(p1, 1, 2 + count):
            copy.start()

    @pl.when(swap)
    def _():
        for copy in pieces(p0, 1, 2) + pieces(p1, 0, 2 + count):
            copy.start()

    first[0].wait()

    def lookup(t):
        at = pl.ds(pl.multiple_of(id_smem[t] // lanes * lanes, lanes), lanes)
        return pltpu.make_async_copy(table.at[at], found.at[t], row_sems.at[t])

    for t in range(tokens):
        lookup(t).start()
    first[1].wait()
    same = iota((tokens, tokens), 0) == iota((tokens, tokens), 1)
    id_col = jnp.sum(jnp.where(same, (id_row[0:1, :] % lanes).astype(f32), 0.0), axis=1, keepdims=True)
    hit = iota((tokens, lanes), 1).astype(f32) == id_col
    for t in range(tokens):
        lookup(t).wait()
    who = jnp.sum(jnp.where(hit, found[...].astype(f32), 0.0), axis=1, keepdims=True)
    expert = iota((tokens, 128), 1).astype(f32)
    onehot = (who == expert).astype(f32)
    before = (iota((tokens, tokens), 1) < iota((tokens, tokens), 0)).astype(bf16)
    rank = dot(before, onehot.astype(bf16))
    target = jnp.sum(onehot * (expert * cap + rank), axis=1, keepdims=True)
    marks = jnp.sum(jnp.where(same, target, 0.0), axis=0, keepdims=True)
    for p in (p0, p1):
        p[top:, :tokens] = jnp.broadcast_to(marks, (p.shape[0] - top, tokens)).astype(bf16)
    for copy in pieces(p0, 0, 2) + pieces(p1, 1, 2 + count):
        copy.wait()


def fetch_kernel(wg, wu, wd, gain, og, ou, od, ogain, sems):
    copies = [
        pltpu.make_async_copy(src, dst, sems.at[i])
        for i, (src, dst) in enumerate(((wg, og), (wu, ou), (wd, od), (gain, ogain)))
    ]
    for copy in copies:
        copy.start()
    for copy in copies:
        copy.wait()


def attend_kernel(cache, tokens, offset, r0, r1, s0, s1, za, xb0, xb1, xb2, xb3, route):
    z, e = lax.axis_index("ctx"), lax.axis_index("exp")
    core = e % 2
    span = cache + tokens
    cap = tokens // 2
    width = r0.shape[1]
    group = HEADS // KV_HEADS
    per_row = width // HEAD_DIM
    top = span + (group // per_row) * tokens
    limit = offset[0:1, 0:1]
    scale = 1.0 / math.sqrt(HEAD_DIM)
    halves = (z % 2, 1 - z % 2)
    keys = [(r, 2 * hi + core) for r, hi in zip((r0, r1), halves)]
    keys += [(s, 2 * hi + 1 - core) for s, hi in zip((s0, s1), halves)]
    rows = group * tokens
    pos = iota((rows, span), 0) % tokens
    col = iota((rows, span), 1)
    for ref, block in keys:
        route[block] = ref[top:, :tokens].astype(f32)
    for r, hi in zip((r0, r1), halves):
        base = (2 * hi + core) * tokens
        q = jnp.concatenate(
            [
                r[span + (g // per_row) * tokens : span + (g // per_row + 1) * tokens,
                  (g % per_row) * HEAD_DIM : (g % per_row + 1) * HEAD_DIM]
                for g in range(group)
            ],
            axis=0,
        )
        scores = []
        for ref, block in keys:
            s = dot_nt(q, ref[0:span, 0:HEAD_DIM]) * scale
            edge = jnp.where(col < cache, limit - block * cache, pos + (base - block * tokens + cache + 1))
            scores.append(jnp.where(col < edge, s, masked_score))
        peak = functools.reduce(jnp.maximum, [jnp.max(s, axis=1, keepdims=True) for s in scores])
        total = jnp.zeros((rows, 1), f32)
        numer = jnp.zeros((rows, HEAD_DIM), f32)
        for (ref, _), s in zip(keys, scores):
            w = jnp.exp(s - peak)
            total += jnp.sum(w, axis=1, keepdims=True)
            numer += dot(w.astype(bf16), ref[0:span, HEAD_DIM:])
        out = (numer / total).astype(bf16)
        for g in range(group - 1):
            za[hi, :, g * HEAD_DIM : (g + 1) * HEAD_DIM] = out[g * tokens : (g + 1) * tokens]
        last = out[(group - 1) * tokens :]
        marks = r[top : top + 1, :tokens].astype(f32)
        for m, xb in enumerate((xb0, xb1, xb2, xb3)):
            xb[hi] = dot(expert_rows(marks, (e ^ m) * cap, cap), last).astype(bf16)


def regroup_kernel(route, a0, a1, a2, a3, b0, b1, b2, b3, c0, c1, c2, c3, zd):
    e = lax.axis_index("exp")
    core = e % 2
    cap = b0.shape[1]
    for j in range(2):
        marks = route[2 * j + core][0:1]
        pick = jnp.concatenate([expert_rows(marks, (e ^ m) * cap, cap) for m in range(4)], axis=0)
        for n, a in enumerate((a0, a1, a2, a3)):
            got = dot(pick, a[j]).astype(bf16)
            for m, c in enumerate((c0, c1, c2, c3)):
                c[n, j] = got[m * cap : (m + 1) * cap]
    for m, b in enumerate((b0, b1, b2, b3)):
        src = e ^ m
        for j in range(2):
            zd[src // 2, 2 * j + src % 2] = b[j]


def expert_kernel(
    c0, c1, c2, c3, d0, d1, d2, d3, gain, wg, wu, wd,
    y0, y1, y2, y3, t0, t1, t2, t3, xs, ns, ys,
):
    z, e = lax.axis_index("ctx"), lax.axis_index("exp")
    slices, blocks, cap, wide = xs.shape
    part = c0.shape[3]
    rows = blocks * cap
    for m, c in enumerate((c0, c1, c2, c3)):
        src = e ^ m
        for n in range(4):
            for j in range(2):
                xs[4 * (src // 2) + (z ^ n), 2 * j + src % 2, :, 0:part] = c[n, j]
    for m, d in enumerate((d0, d1, d2, d3)):
        for x in range(2):
            xs[4 * x + (z ^ m), :, :, part:] = d[x]
    total = jnp.zeros((rows, 1), f32)
    for s in range(slices):
        v = xs[s].reshape(rows, wide).astype(f32)
        total += jnp.sum(v * v, axis=1, keepdims=True)
    scale = lax.rsqrt(total * (1.0 / (slices * wide)) + 1e-05)
    for s in range(slices):
        v = xs[s].reshape(rows, wide).astype(f32)
        lanes = slice(s * wide, (s + 1) * wide)
        ns[:, lanes] = (v * scale * gain[0:1, lanes]).astype(bf16)
    normed = ns[...]
    gate = dot_nt(normed, wg[...])
    upper = dot_nt(normed, wu[...])
    hidden = (gate / (1.0 + jnp.exp(-gate)) * upper).astype(bf16)
    owners = ys.shape[0]
    span = ys.shape[2]
    mine = iota((rows, span), 0) // cap == z
    for o in range(owners):
        lanes = slice(o * span, (o + 1) * span)
        v = dot(hidden, wd[:, lanes])
        ys[o] = (v + jnp.where(mine, ns[:, lanes].astype(f32), 0.0)).astype(bf16)
    keep = y0.shape[1]
    for m, (y, t) in enumerate(zip((y0, y1, y2, y3), (t0, t1, t2, t3))):
        y[...] = ys[e ^ m, :, 0:keep]
        for o in range(owners):
            t[o] = ys[o, pl.ds(pl.multiple_of((z ^ m) * cap, cap), cap), keep:]


def turn_kernel(route, y0, y1, y2, y3, t0, t1, t2, t3, g0, g1, g2, g3, h0, h1, h2, h3, ts):
    z, e = lax.axis_index("ctx"), lax.axis_index("exp")
    cap = h0.shape[0]
    for m, g in enumerate((g0, g1, g2, g3)):
        block = z ^ m
        marks = route[block][0:1]
        pick = jnp.concatenate([expert_rows(marks, (e ^ n) * cap, cap) for n in range(4)], axis=0)
        at = pl.ds(pl.multiple_of(block * cap, cap), cap)
        got = jnp.concatenate([y[at, :] for y in (y0, y1, y2, y3)], axis=0)
        g[...] = dot_tn(pick, got).astype(bf16)
    ts[...] = sum(t[...].astype(f32) for t in (t0, t1, t2, t3)).astype(bf16)
    for m, h in enumerate((h0, h1, h2, h3)):
        h[...] = ts[e ^ m]


def final_kernel(route, g0, g1, g2, g3, h0, h1, h2, h3, out):
    z, e = lax.axis_index("ctx"), lax.axis_index("exp")
    cap = h0.shape[0]
    keep = g0.shape[1]
    out[:, 0:keep] = sum(g[...].astype(f32) for g in (g0, g1, g2, g3)).astype(bf16)
    marks = route[z][0:1]
    pick = jnp.concatenate([expert_rows(marks, (e ^ n) * cap, cap) for n in range(4)], axis=0)
    got = jnp.concatenate([h[...] for h in (h0, h1, h2, h3)], axis=0)
    out[:, keep:] = dot_tn(pick, got).astype(bf16)


def paired_path(
    queries,
    new_keys,
    new_values,
    cache_keys,
    cache_values,
    offset,
    token_ids,
    expert_table,
    norm_gain,
    w_gate,
    w_up,
    w_down,
):
    n_ctx, n_exp = lax.axis_size("ctx"), lax.axis_size("exp")
    tokens = queries.shape[0]
    cache = cache_keys.shape[0]
    width = new_keys.shape[1]
    group = HEADS // KV_HEADS
    wide = group * HEAD_DIM
    cap = tokens // 2
    span = cache + tokens
    part = wide - HEAD_DIM
    own = queries.shape[1]
    back = own * 3 // 8
    keep = own - back
    rows = n_ctx * cap

    def over_ctx(v, m):
        return lax.ppermute(v, "ctx", [(i, i ^ m) for i in range(n_ctx)])

    def over_exp(v, m):
        return lax.ppermute(v, "exp", [(i, i ^ m) for i in range(n_exp)])

    def head_step(v, o):
        pairs = []
        for z in range(n_ctx):
            for e in range(n_exp):
                core = e % 2
                to_z = 2 * core + ((z // 2) ^ o)
                pairs.append((z * n_exp + e, to_z * n_exp + e - core + z % 2))
        return lax.ppermute(v, ("ctx", "exp"), pairs)

    height = span + tokens * wide // width + 16
    copies = 2 + 2 * (4 + wide // width)
    p0, p1 = call(
        pack_kernel,
        [((height, width), bf16)] * 2,
        "pack",
        8,
        scratch=[
            pltpu.VMEM((8, tokens), jnp.int32),
            pltpu.SMEM((tokens,), jnp.int32),
            pltpu.VMEM((tokens, 128), jnp.int32),
            pltpu.SemaphoreType.DMA((copies,)),
            pltpu.SemaphoreType.DMA((tokens,)),
        ],
        hbm=7,
    )(queries, new_keys, new_values, cache_keys, cache_values, token_ids, expert_table)
    limit = jnp.broadcast_to(offset[None, :], (8, 128))
    gate_t, up_t, down = jnp.swapaxes(w_gate[0], 0, 1), jnp.swapaxes(w_up[0], 0, 1), w_down[0]
    weight_bytes = 2 * (gate_t.size + up_t.size + down.size)
    gate_t, up_t, down, gain = call(
        fetch_kernel,
        [(w.shape, bf16) for w in (gate_t, up_t, down)] + [((1, norm_gain.shape[0]), f32)],
        "fetch",
        4,
        scratch=[pltpu.SemaphoreType.DMA((4,))],
        hbm=4,
        cost=pl.CostEstimate(flops=1000 * weight_bytes, transcendentals=0, bytes_accessed=2 * weight_bytes),
    )(gate_t, up_t, down, norm_gain.reshape(1, -1))
    r0, r1 = head_step(p0, 0), head_step(p1, 1)
    s0, s1 = over_exp(r0, 1), over_exp(r1, 1)
    za, xb0, xb1, xb2, xb3, route = call(
        functools.partial(attend_kernel, cache, tokens),
        [((2, tokens, part), bf16)] + [((2, cap, HEAD_DIM), bf16)] * 4 + [((n_ctx, 16, tokens), f32)],
        "attend",
        16,
    )(limit, r0, r1, s0, s1)
    a = [za] + [over_ctx(za, m) for m in (1, 2, 3)]
    b = [xb0] + [over_exp(v, m) for m, v in ((1, xb1), (2, xb2), (3, xb3))]
    c0, c1, c2, c3, zd = call(
        regroup_kernel,
        [((4, 2, cap, part), bf16)] * 4 + [((2, n_ctx, cap, HEAD_DIM), bf16)],
        "regroup",
        8,
    )(route, *a, *b)
    c = [c0] + [over_exp(v, m) for m, v in ((1, c1), (2, c2), (3, c3))]
    d = [zd] + [over_ctx(zd, m) for m in (1, 2, 3)]
    outs = call(
        expert_kernel,
        [((rows, keep), bf16)] * 4 + [((n_exp, cap, back), bf16)] * 4,
        "expert",
        28,
        scratch=[
            pltpu.VMEM((KV_HEADS, n_ctx, cap, wide), bf16),
            pltpu.VMEM((rows, KV_HEADS * wide), bf16),
            pltpu.VMEM((n_exp, rows, own), bf16),
        ],
    )(
        *c,
        *d,
        gain,
        gate_t,
        up_t,
        down,
    )
    y, t = outs[:4], outs[4:]
    t = [t[0]] + [over_ctx(t[m], m) for m in (1, 2, 3)]
    y = [y[0]] + [over_exp(y[m], m) for m in (1, 2, 3)]
    outs = call(
        turn_kernel,
        [((tokens, keep), bf16)] * 4 + [((cap, back), bf16)] * 4,
        "turn",
        8,
        scratch=[pltpu.VMEM((n_exp, cap, back), bf16)],
    )(route, *y, *t)
    g, h = outs[:4], outs[4:]
    g = [g[0]] + [over_ctx(g[m], m) for m in (1, 2, 3)]
    h = [h[0]] + [over_exp(h[m], m) for m in (1, 2, 3)]
    (out,) = call(final_kernel, [((tokens, own), bf16)], "final", 8)(route, *g, *h)
    return out


def solution(mesh):
    placed = (
        P(("group", "ctx"), "exp"),
        P(("group", "ctx"), "exp"),
        P(("group", "ctx"), "exp"),
        P(("group", "ctx"), "exp"),
        P(("group", "ctx"), "exp"),
        P("group"),
        P(("group", "ctx")),
        P("group"),
        P(),
        P("exp", None, "ctx"),
        P("exp", None, "ctx"),
        P("exp", "ctx", None),
    )
    n_ctx, n_exp = mesh.shape["ctx"], mesh.shape["exp"]
    paired = n_ctx == n_exp == 4 and KV_HEADS == 2 * n_exp
    return jax.shard_map(
        paired_path if paired else general_path,
        mesh=mesh,
        in_specs=placed,
        out_specs=P(("group", "ctx"), "exp"),
        check_vma=False,
    )
```

```python
import functools
import math

import jax
import jax.numpy as jnp
from jax import lax
from jax.experimental import pallas as pl
from jax.experimental.pallas import tpu as pltpu
from jax.sharding import PartitionSpec as P

HEADS = 32
KV_HEADS = 8
HEAD_DIM = 128


masked_score = -1e30
f32 = jnp.float32
bf16 = jnp.bfloat16


def split_heads(flat, heads):
    return flat.reshape(flat.shape[0], heads, flat.shape[1] // heads)


def partial_attend(query_rows, key_rows, value_rows, allowed):
    width = query_rows.shape[3]
    scores = jnp.einsum("rkgd,skd->rkgs", query_rows, key_rows, preferred_element_type=jnp.float32)
    scores = scores * (1.0 / math.sqrt(width))
    usable = allowed[:, None, None, :]
    peak = jnp.max(jnp.where(usable, scores, masked_score), axis=-1)
    unnorm = jnp.where(usable, jnp.exp(scores - peak[..., None]), 0.0)
    total = jnp.sum(unnorm, axis=-1)
    numer = jnp.einsum(
        "rkgs,skd->rkgd",
        unnorm.astype(jnp.bfloat16),
        value_rows,
        preferred_element_type=jnp.float32,
    )
    return (numer, peak, total)


def general_path(
    queries,
    new_keys,
    new_values,
    cache_keys,
    cache_values,
    offset,
    token_ids,
    expert_table,
    norm_gain,
    w_gate,
    w_up,
    w_down,
):
    owners = lax.axis_size("exp")
    heads_local = HEADS // owners
    kv_local = KV_HEADS // owners
    group = HEADS // KV_HEADS
    tok_count = queries.shape[0]
    cache_len = cache_keys.shape[0]
    shard = lax.axis_index("ctx")
    limit = offset[0]
    key_rows = jnp.concatenate([cache_keys, new_keys], axis=0)
    value_rows = jnp.concatenate([cache_values, new_values], axis=0)
    span = key_rows.shape[0]
    own_index = shard * tok_count + jnp.arange(tok_count, dtype=jnp.int32)
    grouped = queries.reshape(tok_count, kv_local, group, HEAD_DIM)
    piece_keys = lax.all_gather(key_rows, "ctx", axis=0, tiled=True)
    piece_values = lax.all_gather(value_rows, "ctx", axis=0, tiled=True)
    flat = jnp.arange(piece_keys.shape[0], dtype=jnp.int32)
    source = flat // span
    inner = flat % span
    cache_ok = source * cache_len + inner < limit
    stretch_ok = (source * tok_count + inner - cache_len)[None, :] <= own_index[:, None]
    allowed = jnp.where((inner < cache_len)[None, :], cache_ok[None, :], stretch_ok)
    numer, peak, total = partial_attend(
        grouped, split_heads(piece_keys, kv_local), split_heads(piece_values, kv_local), allowed
    )
    attended = (numer / total[..., None]).reshape(tok_count, heads_local * HEAD_DIM).astype(jnp.bfloat16)
    capacity = tok_count // 2
    chosen = expert_table[token_ids]
    onehot = (chosen[:, None] == jnp.arange(owners, dtype=jnp.int32)[None, :]).astype(jnp.int32)
    earlier = jnp.cumsum(onehot, axis=0) - onehot
    slot = jnp.sum(earlier * onehot, axis=1)
    target = chosen * capacity + slot
    dispatch = (jnp.arange(owners * capacity, dtype=jnp.int32)[:, None] == target[None, :]).astype(
        jnp.bfloat16
    )
    packed = jnp.dot(dispatch, attended, preferred_element_type=jnp.float32).astype(jnp.bfloat16)
    arrived = lax.all_to_all(packed, "exp", split_axis=0, concat_axis=1, tiled=True)
    values32 = arrived.astype(jnp.float32)
    scale = lax.rsqrt(jnp.mean(values32 * values32, axis=-1, keepdims=True) + 1e-05)
    normed = (values32 * scale * norm_gain).astype(jnp.bfloat16)
    piece = lax.all_gather(normed, "ctx", axis=0, tiled=True)
    gate = jnp.dot(piece, w_gate[0], preferred_element_type=jnp.float32)
    upper = jnp.dot(piece, w_up[0], preferred_element_type=jnp.float32)
    hidden = (jax.nn.silu(gate) * upper).astype(jnp.bfloat16)
    summed = lax.psum_scatter(
        jnp.dot(hidden, w_down[0], preferred_element_type=jnp.float32).astype(jnp.bfloat16),
        "ctx",
        scatter_dimension=0,
        tiled=True,
    ).astype(jnp.float32)
    combined = (normed.astype(jnp.float32) + summed).astype(jnp.bfloat16)
    returned = lax.all_to_all(combined, "exp", split_axis=1, concat_axis=0, tiled=True)
    collect = (target[:, None] == jnp.arange(owners * capacity, dtype=jnp.int32)[None, :]).astype(
        jnp.bfloat16
    )
    return jnp.dot(collect, returned, preferred_element_type=jnp.float32).astype(jnp.bfloat16)


def iota(shape, axis):
    return lax.broadcasted_iota(jnp.int32, shape, axis)


def call(kernel, out_shapes, name, mib, scratch=(), hbm=0, cost=None):
    def run(*args):
        args = [pltpu.with_memory_space_constraint(v, pltpu.HBM) if i < hbm else v for i, v in enumerate(args)]
        vmem = pl.BlockSpec(memory_space=pltpu.VMEM)
        specs = [pl.BlockSpec(memory_space=pltpu.HBM)] * hbm + [vmem] * (len(args) - hbm)
        return pl.pallas_call(
            kernel,
            out_shape=[jax.ShapeDtypeStruct(s, d) for s, d in out_shapes],
            in_specs=specs,
            out_specs=[vmem] * len(out_shapes),
            scratch_shapes=list(scratch),
            compiler_params=pltpu.CompilerParams(vmem_limit_bytes=mib << 20),
            cost_estimate=cost,
            name=name,
        )(*args)

    return run


def expert_rows(marks, first, cap):
    tokens = marks.shape[1]
    slots = (iota((cap, tokens), 0) + first).astype(f32)
    return (marks == slots).astype(bf16)


def dot(a, b):
    return jnp.dot(a, b, preferred_element_type=f32)


def dot_nt(a, b):
    return lax.dot_general(a, b, (((1,), (1,)), ((), ())), preferred_element_type=f32)


def dot_tn(a, b):
    return lax.dot_general(a, b, (((0,), (0,)), ((), ())), preferred_element_type=f32)


def pack_kernel(q, nk, nv, ck, cv, ids, table, p0, p1, id_row, id_smem, found, sems, row_sems):
    z = lax.axis_index("ctx")
    tokens, cache = q.shape[0], ck.shape[0]
    span = cache + tokens
    width = p0.shape[1]
    wide = q.shape[1] // 2
    cap = tokens // 2
    top = span + (wide // width) * tokens
    lanes = found.shape[1]
    swap = (z // 2) == 1

    first = [
        pltpu.make_async_copy(ids, id_smem, sems.at[0]),
        pltpu.make_async_copy(ids, id_row.at[0], sems.at[1]),
    ]
    for copy in first:
        copy.start()

    def pieces(p, h, base):
        at = pl.ds(h * HEAD_DIM, HEAD_DIM)
        moves = [
            (ck.at[:, at], p.at[0:cache, 0:HEAD_DIM]),
            (cv.at[:, at], p.at[0:cache, HEAD_DIM:]),
            (nk.at[:, at], p.at[cache:span, 0:HEAD_DIM]),
            (nv.at[:, at], p.at[cache:span, HEAD_DIM:]),
        ]
        for part in range(wide // width):
            lo = h * wide + part * width
            moves.append((q.at[:, pl.ds(lo, width)], p.at[span + part * tokens : span + (part + 1) * tokens, :]))
        return [pltpu.make_async_copy(src, dst, sems.at[base + i]) for i, (src, dst) in enumerate(moves)]

    count = 4 + wide // width

    @pl.when(jnp.logical_not(swap))
    def _():
        for copy in pieces(p0, 0, 2) + pieces(p1, 1, 2 + count):
            copy.start()

    @pl.when(swap)
    def _():
        for copy in pieces(p0, 1, 2) + pieces(p1, 0, 2 + count):
            copy.start()

    first[0].wait()

    def lookup(t):
        at = pl.ds(pl.multiple_of(id_smem[t] // lanes * lanes, lanes), lanes)
        return pltpu.make_async_copy(table.at[at], found.at[t], row_sems.at[t])

    for t in range(tokens):
        lookup(t).start()
    first[1].wait()
    same = iota((tokens, tokens), 0) == iota((tokens, tokens), 1)
    id_col = jnp.sum(jnp.where(same, (id_row[0:1, :] % lanes).astype(f32), 0.0), axis=1, keepdims=True)
    hit = iota((tokens, lanes), 1).astype(f32) == id_col
    for t in range(tokens):
        lookup(t).wait()
    who = jnp.sum(jnp.where(hit, found[...].astype(f32), 0.0), axis=1, keepdims=True)
    expert = iota((tokens, 128), 1).astype(f32)
    onehot = (who == expert).astype(f32)
    before = (iota((tokens, tokens), 1) < iota((tokens, tokens), 0)).astype(bf16)
    rank = dot(before, onehot.astype(bf16))
    target = jnp.sum(onehot * (expert * cap + rank), axis=1, keepdims=True)
    marks = jnp.sum(jnp.where(same, target, 0.0), axis=0, keepdims=True)
    for p in (p0, p1):
        p[top:, :tokens] = jnp.broadcast_to(marks, (p.shape[0] - top, tokens)).astype(bf16)
    for copy in pieces(p0, 0, 2) + pieces(p1, 1, 2 + count):
        copy.wait()


def fetch_kernel(wg, wu, wd, gain, og, ou, od, ogain, sems):
    copies = [
        pltpu.make_async_copy(src, dst, sems.at[i])
        for i, (src, dst) in enumerate(((wg, og), (wu, ou), (wd, od), (gain, ogain)))
    ]
    for copy in copies:
        copy.start()
    for copy in copies:
        copy.wait()


def units(heads):
    lots = [(j, h) for j in range(2) for h in range(heads)]
    early = [(j, h) for j, h in lots if h >= heads - 1 - j]
    return [lot for lot in lots if lot not in early], early


def attend_kernel(cache, tokens, offset, r0, r1, s0, s1, za, xb0, xb1, xb2, xb3, route, held):
    z, e = lax.axis_index("ctx"), lax.axis_index("exp")
    core = e % 2
    span = cache + tokens
    cap = tokens // 2
    width = r0.shape[1]
    group = HEADS // KV_HEADS
    per_row = width // HEAD_DIM
    top = span + (group // per_row) * tokens
    limit = offset[0:1, 0:1]
    scale = 1.0 / math.sqrt(HEAD_DIM)
    halves = (z % 2, 1 - z % 2)
    keys = [(r, 2 * hi + core) for r, hi in zip((r0, r1), halves)]
    keys += [(s, 2 * hi + 1 - core) for s, hi in zip((s0, s1), halves)]
    rows = group * tokens
    pos = iota((rows, span), 0) % tokens
    col = iota((rows, span), 1)
    for ref, block in keys:
        route[block] = ref[top:, :tokens].astype(f32)
    for r, hi in zip((r0, r1), halves):
        base = (2 * hi + core) * tokens
        q = jnp.concatenate(
            [
                r[span + (g // per_row) * tokens : span + (g // per_row + 1) * tokens,
                  (g % per_row) * HEAD_DIM : (g % per_row + 1) * HEAD_DIM]
                for g in range(group)
            ],
            axis=0,
        )
        scores = []
        for ref, block in keys:
            s = dot_nt(q, ref[0:span, 0:HEAD_DIM]) * scale
            edge = jnp.where(col < cache, limit - block * cache, pos + (base - block * tokens + cache + 1))
            scores.append(jnp.where(col < edge, s, masked_score))
        peak = functools.reduce(jnp.maximum, [jnp.max(s, axis=1, keepdims=True) for s in scores])
        total = jnp.zeros((rows, 1), f32)
        numer = jnp.zeros((rows, HEAD_DIM), f32)
        for (ref, _), s in zip(keys, scores):
            w = jnp.exp(s - peak)
            total += jnp.sum(w, axis=1, keepdims=True)
            numer += dot(w.astype(bf16), ref[0:span, HEAD_DIM:])
        out = (numer / total).astype(bf16)
        held[hi] = jnp.concatenate([out[g * tokens : (g + 1) * tokens] for g in range(group)], axis=1)
    over_z, over_x = units(group)
    for u, (j, h) in enumerate(over_z):
        za[u] = held[j, :, h * HEAD_DIM : (h + 1) * HEAD_DIM]
    for m, xb in enumerate((xb0, xb1, xb2, xb3)):
        for j in range(2):
            pick = expert_rows(route[2 * j + core][0:1], (e ^ m) * cap, cap)
            mine = [(u, h) for u, (i, h) in enumerate(over_x) if i == j]
            lo = mine[0][1] * HEAD_DIM
            got = dot(pick, held[j, :, lo : lo + len(mine) * HEAD_DIM]).astype(bf16)
            for i, (u, _) in enumerate(mine):
                xb[u] = got[:, i * HEAD_DIM : (i + 1) * HEAD_DIM]


def join_kernel(b0, b1, b2, b3, d):
    e = lax.axis_index("exp")
    for m, b in enumerate((b0, b1, b2, b3)):
        d[e ^ m] = b[...]


def regroup_kernel(route, a0, a1, a2, a3, c0, c1, c2, c3):
    e = lax.axis_index("exp")
    core = e % 2
    cap = c0.shape[2]
    over_z, _ = units(HEADS // KV_HEADS)
    for j in range(2):
        marks = route[2 * j + core][0:1]
        pick = jnp.concatenate([expert_rows(marks, (e ^ m) * cap, cap) for m in range(4)], axis=0)
        for u, (i, _) in enumerate(over_z):
            if i == j:
                for n, a in enumerate((a0, a1, a2, a3)):
                    got = dot(pick, a[u]).astype(bf16)
                    for m, c in enumerate((c0, c1, c2, c3)):
                        c[n, u] = got[m * cap : (m + 1) * cap]


def expert_kernel(
    c0, c1, c2, c3, d0, d1, d2, d3, gain, wg, wu, wd,
    y0, y1, y2, y3, t0, t1, t2, t3, xs, ns, ys,
):
    z, e = lax.axis_index("ctx"), lax.axis_index("exp")
    slices, blocks, cap, wide = xs.shape
    rows = blocks * cap
    over_z, over_x = units(HEADS // KV_HEADS)

    def lanes_of(h):
        return slice(h * HEAD_DIM, (h + 1) * HEAD_DIM)

    for m, d in enumerate((d0, d1, d2, d3)):
        for src in range(4):
            for u, (j, h) in enumerate(over_x):
                xs[4 * (src // 2) + (z ^ m), 2 * j + src % 2, :, lanes_of(h)] = d[src, u]
    for m, c in enumerate((c0, c1, c2, c3)):
        src = e ^ m
        for n in range(4):
            for u, (j, h) in enumerate(over_z):
                xs[4 * (src // 2) + (z ^ n), 2 * j + src % 2, :, lanes_of(h)] = c[n, u]
    total = jnp.zeros((rows, 1), f32)
    for s in range(slices):
        v = xs[s].reshape(rows, wide).astype(f32)
        total += jnp.sum(v * v, axis=1, keepdims=True)
    scale = lax.rsqrt(total * (1.0 / (slices * wide)) + 1e-05)
    for s in range(slices):
        v = xs[s].reshape(rows, wide).astype(f32)
        lanes = slice(s * wide, (s + 1) * wide)
        ns[:, lanes] = (v * scale * gain[0:1, lanes]).astype(bf16)
    normed = ns[...]
    gate = dot_nt(normed, wg[...])
    upper = dot_nt(normed, wu[...])
    hidden = (gate / (1.0 + jnp.exp(-gate)) * upper).astype(bf16)
    owners = ys.shape[0]
    span = ys.shape[2]
    mine = iota((rows, span), 0) // cap == z
    for o in range(owners):
        lanes = slice(o * span, (o + 1) * span)
        v = dot(hidden, wd[:, lanes])
        ys[o] = (v + jnp.where(mine, ns[:, lanes].astype(f32), 0.0)).astype(bf16)
    keep = y0.shape[1]
    for m, (y, t) in enumerate(zip((y0, y1, y2, y3), (t0, t1, t2, t3))):
        y[...] = ys[e ^ m, :, 0:keep]
        for o in range(owners):
            t[o] = ys[o, pl.ds(pl.multiple_of((z ^ m) * cap, cap), cap), keep:]


def turn_kernel(route, y0, y1, y2, y3, g0, g1, g2, g3):
    z, e = lax.axis_index("ctx"), lax.axis_index("exp")
    cap = y0.shape[0] // 4
    for m, g in enumerate((g0, g1, g2, g3)):
        block = z ^ m
        marks = route[block][0:1]
        pick = jnp.concatenate([expert_rows(marks, (e ^ n) * cap, cap) for n in range(4)], axis=0)
        at = pl.ds(pl.multiple_of(block * cap, cap), cap)
        got = jnp.concatenate([y[at, :] for y in (y0, y1, y2, y3)], axis=0)
        g[...] = dot_tn(pick, got).astype(bf16)


def total_kernel(t0, t1, t2, t3, h0, h1, h2, h3, ts):
    e = lax.axis_index("exp")
    ts[...] = sum(t[...].astype(f32) for t in (t0, t1, t2, t3)).astype(bf16)
    for m, h in enumerate((h0, h1, h2, h3)):
        h[...] = ts[e ^ m]


def final_kernel(route, g0, g1, g2, g3, h0, h1, h2, h3, out):
    z, e = lax.axis_index("ctx"), lax.axis_index("exp")
    cap = h0.shape[0]
    keep = g0.shape[1]
    out[:, 0:keep] = sum(g[...].astype(f32) for g in (g0, g1, g2, g3)).astype(bf16)
    marks = route[z][0:1]
    pick = jnp.concatenate([expert_rows(marks, (e ^ n) * cap, cap) for n in range(4)], axis=0)
    got = jnp.concatenate([h[...] for h in (h0, h1, h2, h3)], axis=0)
    out[:, keep:] = dot_tn(pick, got).astype(bf16)


def paired_path(
    queries,
    new_keys,
    new_values,
    cache_keys,
    cache_values,
    offset,
    token_ids,
    expert_table,
    norm_gain,
    w_gate,
    w_up,
    w_down,
):
    n_ctx, n_exp = lax.axis_size("ctx"), lax.axis_size("exp")
    tokens = queries.shape[0]
    cache = cache_keys.shape[0]
    width = new_keys.shape[1]
    group = HEADS // KV_HEADS
    wide = group * HEAD_DIM
    cap = tokens // 2
    span = cache + tokens
    over_z, over_x = units(group)
    own = queries.shape[1]
    back = own * 3 // 8
    keep = own - back
    rows = n_ctx * cap

    def over_ctx(v, m):
        return lax.ppermute(v, "ctx", [(i, i ^ m) for i in range(n_ctx)])

    def over_exp(v, m):
        return lax.ppermute(v, "exp", [(i, i ^ m) for i in range(n_exp)])

    def head_step(v, o):
        pairs = []
        for z in range(n_ctx):
            for e in range(n_exp):
                core = e % 2
                to_z = 2 * core + ((z // 2) ^ o)
                pairs.append((z * n_exp + e, to_z * n_exp + e - core + z % 2))
        return lax.ppermute(v, ("ctx", "exp"), pairs)

    height = span + tokens * wide // width + 16
    copies = 2 + 2 * (4 + wide // width)
    p0, p1 = call(
        pack_kernel,
        [((height, width), bf16)] * 2,
        "pack",
        8,
        scratch=[
            pltpu.VMEM((8, tokens), jnp.int32),
            pltpu.SMEM((tokens,), jnp.int32),
            pltpu.VMEM((tokens, 128), jnp.int32),
            pltpu.SemaphoreType.DMA((copies,)),
            pltpu.SemaphoreType.DMA((tokens,)),
        ],
        hbm=7,
    )(queries, new_keys, new_values, cache_keys, cache_values, token_ids, expert_table)
    limit = jnp.broadcast_to(offset[None, :], (8, 128))
    gate_t, up_t, down = jnp.swapaxes(w_gate[0], 0, 1), jnp.swapaxes(w_up[0], 0, 1), w_down[0]
    weight_bytes = 2 * (gate_t.size + up_t.size + down.size)
    gate_t, up_t, down, gain = call(
        fetch_kernel,
        [(w.shape, bf16) for w in (gate_t, up_t, down)] + [((1, norm_gain.shape[0]), f32)],
        "fetch",
        4,
        scratch=[pltpu.SemaphoreType.DMA((4,))],
        hbm=4,
        cost=pl.CostEstimate(flops=1000 * weight_bytes, transcendentals=0, bytes_accessed=2 * weight_bytes),
    )(gate_t, up_t, down, norm_gain.reshape(1, -1))
    r0, r1 = head_step(p0, 0), head_step(p1, 1)
    s0, s1 = over_exp(r0, 1), over_exp(r1, 1)
    za, xb0, xb1, xb2, xb3, route = call(
        functools.partial(attend_kernel, cache, tokens),
        [((len(over_z), tokens, HEAD_DIM), bf16)]
        + [((len(over_x), cap, HEAD_DIM), bf16)] * 4
        + [((n_ctx, 16, tokens), f32)],
        "attend",
        16,
        scratch=[pltpu.VMEM((2, tokens, wide), bf16)],
    )(limit, r0, r1, s0, s1)
    a = [za] + [over_ctx(za, m) for m in (1, 2, 3)]
    b = [xb0] + [over_exp(v, m) for m, v in ((1, xb1), (2, xb2), (3, xb3))]
    (zd,) = call(join_kernel, [((n_exp, len(over_x), cap, HEAD_DIM), bf16)], "join", 4)(*b)
    d = [zd] + [over_ctx(zd, m) for m in (1, 2, 3)]
    c0, c1, c2, c3 = call(
        regroup_kernel, [((n_ctx, len(over_z), cap, HEAD_DIM), bf16)] * 4, "regroup", 8
    )(route, *a)
    c = [c0] + [over_exp(v, m) for m, v in ((1, c1), (2, c2), (3, c3))]
    outs = call(
        expert_kernel,
        [((rows, keep), bf16)] * 4 + [((n_exp, cap, back), bf16)] * 4,
        "expert",
        28,
        scratch=[
            pltpu.VMEM((KV_HEADS, n_ctx, cap, wide), bf16),
            pltpu.VMEM((rows, KV_HEADS * wide), bf16),
            pltpu.VMEM((n_exp, rows, own), bf16),
        ],
    )(
        *c,
        *d,
        gain,
        gate_t,
        up_t,
        down,
    )
    y, t = outs[:4], outs[4:]
    t = [t[0]] + [over_ctx(t[m], m) for m in (1, 2, 3)]
    y = [y[0]] + [over_exp(y[m], m) for m in (1, 2, 3)]
    g = call(turn_kernel, [((tokens, keep), bf16)] * 4, "turn", 8)(route, *y)
    g = [g[0]] + [over_ctx(g[m], m) for m in (1, 2, 3)]
    h = call(
        total_kernel,
        [((cap, back), bf16)] * 4,
        "total",
        8,
        scratch=[pltpu.VMEM((n_exp, cap, back), bf16)],
    )(*t)
    h = [h[0]] + [over_exp(h[m], m) for m in (1, 2, 3)]
    (out,) = call(final_kernel, [((tokens, own), bf16)], "final", 8)(route, *g, *h)
    return out


def solution(mesh):
    placed = (
        P(("group", "ctx"), "exp"),
        P(("group", "ctx"), "exp"),
        P(("group", "ctx"), "exp"),
        P(("group", "ctx"), "exp"),
        P(("group", "ctx"), "exp"),
        P("group"),
        P(("group", "ctx")),
        P("group"),
        P(),
        P("exp", None, "ctx"),
        P("exp", None, "ctx"),
        P("exp", "ctx", None),
    )
    n_ctx, n_exp = mesh.shape["ctx"], mesh.shape["exp"]
    paired = n_ctx == n_exp == 4 and KV_HEADS == 2 * n_exp
    return jax.shard_map(
        paired_path if paired else general_path,
        mesh=mesh,
        in_specs=placed,
        out_specs=P(("group", "ctx"), "exp"),
        check_vma=False,
    )
```

```python
import functools
import math

import jax
import jax.numpy as jnp
from jax import lax
from jax.experimental import pallas as pl
from jax.experimental.pallas import tpu as pltpu
from jax.sharding import PartitionSpec as P


HEADS = 32
KV_HEADS = 8
HEAD_DIM = 128


masked_score = -1e30
f32 = jnp.float32
bf16 = jnp.bfloat16


def split_heads(flat, heads):
    return flat.reshape(flat.shape[0], heads, flat.shape[1] // heads)


def partial_attend(query_rows, key_rows, value_rows, allowed):
    width = query_rows.shape[3]
    scores = jnp.einsum("rkgd,skd->rkgs", query_rows, key_rows, preferred_element_type=jnp.float32)
    scores = scores * (1.0 / math.sqrt(width))
    usable = allowed[:, None, None, :]
    peak = jnp.max(jnp.where(usable, scores, masked_score), axis=-1)
    unnorm = jnp.where(usable, jnp.exp(scores - peak[..., None]), 0.0)
    total = jnp.sum(unnorm, axis=-1)
    numer = jnp.einsum(
        "rkgs,skd->rkgd",
        unnorm.astype(jnp.bfloat16),
        value_rows,
        preferred_element_type=jnp.float32,
    )
    return (numer, peak, total)


def general_path(
    queries,
    new_keys,
    new_values,
    cache_keys,
    cache_values,
    offset,
    token_ids,
    expert_table,
    norm_gain,
    w_gate,
    w_up,
    w_down,
):
    owners = lax.axis_size("exp")
    heads_local = HEADS // owners
    kv_local = KV_HEADS // owners
    group = HEADS // KV_HEADS
    tok_count = queries.shape[0]
    cache_len = cache_keys.shape[0]
    shard = lax.axis_index("ctx")
    limit = offset[0]
    key_rows = jnp.concatenate([cache_keys, new_keys], axis=0)
    value_rows = jnp.concatenate([cache_values, new_values], axis=0)
    span = key_rows.shape[0]
    own_index = shard * tok_count + jnp.arange(tok_count, dtype=jnp.int32)
    grouped = queries.reshape(tok_count, kv_local, group, HEAD_DIM)
    piece_keys = lax.all_gather(key_rows, "ctx", axis=0, tiled=True)
    piece_values = lax.all_gather(value_rows, "ctx", axis=0, tiled=True)
    flat = jnp.arange(piece_keys.shape[0], dtype=jnp.int32)
    source = flat // span
    inner = flat % span
    cache_ok = source * cache_len + inner < limit
    stretch_ok = (source * tok_count + inner - cache_len)[None, :] <= own_index[:, None]
    allowed = jnp.where((inner < cache_len)[None, :], cache_ok[None, :], stretch_ok)
    numer, _, total = partial_attend(
        grouped, split_heads(piece_keys, kv_local), split_heads(piece_values, kv_local), allowed
    )
    attended = (numer / total[..., None]).reshape(tok_count, heads_local * HEAD_DIM).astype(jnp.bfloat16)
    capacity = tok_count // 2
    chosen = expert_table[token_ids]
    onehot = (chosen[:, None] == jnp.arange(owners, dtype=jnp.int32)[None, :]).astype(jnp.int32)
    earlier = jnp.cumsum(onehot, axis=0) - onehot
    slot = jnp.sum(earlier * onehot, axis=1)
    target = chosen * capacity + slot
    dispatch = (jnp.arange(owners * capacity, dtype=jnp.int32)[:, None] == target[None, :]).astype(
        jnp.bfloat16
    )
    packed = jnp.dot(dispatch, attended, preferred_element_type=jnp.float32).astype(jnp.bfloat16)
    arrived = lax.all_to_all(packed, "exp", split_axis=0, concat_axis=1, tiled=True)
    values32 = arrived.astype(jnp.float32)
    scale = lax.rsqrt(jnp.mean(values32 * values32, axis=-1, keepdims=True) + 1e-05)
    normed = (values32 * scale * norm_gain).astype(jnp.bfloat16)
    piece = lax.all_gather(normed, "ctx", axis=0, tiled=True)
    gate = jnp.dot(piece, w_gate[0], preferred_element_type=jnp.float32)
    upper = jnp.dot(piece, w_up[0], preferred_element_type=jnp.float32)
    hidden = (jax.nn.silu(gate) * upper).astype(jnp.bfloat16)
    summed = lax.psum_scatter(
        jnp.dot(hidden, w_down[0], preferred_element_type=jnp.float32).astype(jnp.bfloat16),
        "ctx",
        scatter_dimension=0,
        tiled=True,
    ).astype(jnp.float32)
    combined = (normed.astype(jnp.float32) + summed).astype(jnp.bfloat16)
    returned = lax.all_to_all(combined, "exp", split_axis=1, concat_axis=0, tiled=True)
    collect = (target[:, None] == jnp.arange(owners * capacity, dtype=jnp.int32)[None, :]).astype(
        jnp.bfloat16
    )
    return jnp.dot(collect, returned, preferred_element_type=jnp.float32).astype(jnp.bfloat16)


def iota(shape, axis):
    return lax.broadcasted_iota(jnp.int32, shape, axis)


def call(kernel, out_shapes, mib, scratch=(), hbm=0, cost=None):
    def run(*args):
        args = [pltpu.with_memory_space_constraint(v, pltpu.HBM) if i < hbm else v for i, v in enumerate(args)]
        vmem = pl.BlockSpec(memory_space=pltpu.VMEM)
        specs = [pl.BlockSpec(memory_space=pltpu.HBM)] * hbm + [vmem] * (len(args) - hbm)
        return pl.pallas_call(
            kernel,
            out_shape=[jax.ShapeDtypeStruct(s, d) for s, d in out_shapes],
            in_specs=specs,
            out_specs=[vmem] * len(out_shapes),
            scratch_shapes=list(scratch),
            compiler_params=pltpu.CompilerParams(vmem_limit_bytes=mib << 20),
            cost_estimate=cost,
        )(*args)

    return run


def expert_rows(marks, first, cap):
    tokens = marks.shape[1]
    slots = (iota((cap, tokens), 0) + first).astype(f32)
    return (marks == slots).astype(bf16)


def dot(a, b):
    return jnp.dot(a, b, preferred_element_type=f32)


def dot_nt(a, b):
    return lax.dot_general(a, b, (((1,), (1,)), ((), ())), preferred_element_type=f32)


def dot_tn(a, b):
    return lax.dot_general(a, b, (((0,), (0,)), ((), ())), preferred_element_type=f32)


def pack_kernel(q, nk, nv, ck, cv, ids, table, p0, p1, id_row, id_smem, rows, found, sems):
    z = lax.axis_index("ctx")
    tokens, cache = q.shape[0], ck.shape[0]
    span = cache + tokens
    width = p0.shape[1]
    wide = q.shape[1] // 2
    cap = tokens // 2
    top = span + (wide // width) * tokens
    lanes = found.shape[1]
    swap = (z // 2) == 1

    first = [
        pltpu.make_async_copy(ids, id_smem, sems.at[0]),
        pltpu.make_async_copy(ids, id_row.at[0], sems.at[1]),
        pltpu.make_async_copy(table, rows, sems.at[2]),
    ]
    for copy in first:
        copy.start()

    def pieces(p, h, base):
        at = pl.ds(h * HEAD_DIM, HEAD_DIM)
        moves = [
            (ck.at[:, at], p.at[0:cache, 0:HEAD_DIM]),
            (cv.at[:, at], p.at[0:cache, HEAD_DIM:]),
            (nk.at[:, at], p.at[cache:span, 0:HEAD_DIM]),
            (nv.at[:, at], p.at[cache:span, HEAD_DIM:]),
        ]
        for part in range(wide // width):
            lo = h * wide + part * width
            moves.append((q.at[:, pl.ds(lo, width)], p.at[span + part * tokens : span + (part + 1) * tokens, :]))
        return [pltpu.make_async_copy(src, dst, sems.at[base + i]) for i, (src, dst) in enumerate(moves)]

    count = 4 + wide // width

    @pl.when(jnp.logical_not(swap))
    def _():
        for copy in pieces(p0, 0, 3) + pieces(p1, 1, 3 + count):
            copy.start()

    @pl.when(swap)
    def _():
        for copy in pieces(p0, 1, 3) + pieces(p1, 0, 3 + count):
            copy.start()

    for copy in first:
        copy.wait()
    for t in range(tokens):
        found[t : t + 1, :] = rows[pl.ds(id_smem[t] // lanes, 1), :]
    same = iota((tokens, tokens), 0) == iota((tokens, tokens), 1)
    id_col = jnp.sum(jnp.where(same, (id_row[0:1, :] % lanes).astype(f32), 0.0), axis=1, keepdims=True)
    hit = iota((tokens, lanes), 1).astype(f32) == id_col
    who = jnp.sum(jnp.where(hit, found[...].astype(f32), 0.0), axis=1, keepdims=True)
    expert = iota((tokens, 128), 1).astype(f32)
    onehot = (who == expert).astype(f32)
    before = (iota((tokens, tokens), 1) < iota((tokens, tokens), 0)).astype(bf16)
    rank = dot(before, onehot.astype(bf16))
    target = jnp.sum(onehot * (expert * cap + rank), axis=1, keepdims=True)
    marks = jnp.sum(jnp.where(same, target, 0.0), axis=0, keepdims=True)
    for p in (p0, p1):
        p[top:, :tokens] = jnp.broadcast_to(marks, (p.shape[0] - top, tokens)).astype(bf16)
    for copy in pieces(p0, 0, 3) + pieces(p1, 1, 3 + count):
        copy.wait()


def fetch_kernel(wg, wu, wd, gain, og, ou, od, ogain, sems):
    copies = [
        pltpu.make_async_copy(src, dst, sems.at[i])
        for i, (src, dst) in enumerate(((wg, og), (wu, ou), (wd, od), (gain, ogain)))
    ]
    for copy in copies:
        copy.start()
    for copy in copies:
        copy.wait()


def units(heads):
    lots = [(j, h) for j in range(2) for h in range(heads)]
    early = [(j, h) for j, h in lots if h >= heads - 1 - j]
    return [lot for lot in lots if lot not in early], early


def attend_kernel(cache, tokens, offset, r0, r1, s0, s1, za, xb0, xb1, xb2, xb3, route, held):
    z, e = lax.axis_index("ctx"), lax.axis_index("exp")
    core = e % 2
    span = cache + tokens
    cap = tokens // 2
    width = r0.shape[1]
    group = HEADS // KV_HEADS
    per_row = width // HEAD_DIM
    top = span + (group // per_row) * tokens
    limit = offset[0:1, 0:1]
    scale = 1.0 / math.sqrt(HEAD_DIM)
    halves = (z % 2, 1 - z % 2)
    keys = [(r, 2 * hi + core) for r, hi in zip((r0, r1), halves)]
    keys += [(s, 2 * hi + 1 - core) for s, hi in zip((s0, s1), halves)]
    rows = group * tokens
    pos = iota((rows, span), 0) % tokens
    col = iota((rows, span), 1)
    for ref, block in keys:
        route[block] = ref[top:, :tokens].astype(f32)
    for r, hi in zip((r0, r1), halves):
        base = (2 * hi + core) * tokens
        q = jnp.concatenate(
            [
                r[span + (g // per_row) * tokens : span + (g // per_row + 1) * tokens,
                  (g % per_row) * HEAD_DIM : (g % per_row + 1) * HEAD_DIM]
                for g in range(group)
            ],
            axis=0,
        )
        scores = []
        for ref, block in keys:
            s = dot_nt(q, ref[0:span, 0:HEAD_DIM]) * scale
            edge = jnp.where(col < cache, limit - block * cache, pos + (base - block * tokens + cache + 1))
            scores.append(jnp.where(col < edge, s, masked_score))
        peak = functools.reduce(jnp.maximum, [jnp.max(s, axis=1, keepdims=True) for s in scores])
        total = jnp.zeros((rows, 1), f32)
        numer = jnp.zeros((rows, HEAD_DIM), f32)
        for (ref, _), s in zip(keys, scores):
            w = jnp.exp(s - peak)
            total += jnp.sum(w, axis=1, keepdims=True)
            numer += dot(w.astype(bf16), ref[0:span, HEAD_DIM:])
        out = (numer / total).astype(bf16)
        held[hi] = jnp.concatenate([out[g * tokens : (g + 1) * tokens] for g in range(group)], axis=1)
    over_z, over_x = units(group)
    for u, (j, h) in enumerate(over_z):
        za[u] = held[j, :, h * HEAD_DIM : (h + 1) * HEAD_DIM]
    for m, xb in enumerate((xb0, xb1, xb2, xb3)):
        for j in range(2):
            pick = expert_rows(route[2 * j + core][0:1], (e ^ m) * cap, cap)
            mine = [(u, h) for u, (i, h) in enumerate(over_x) if i == j]
            lo = mine[0][1] * HEAD_DIM
            got = dot(pick, held[j, :, lo : lo + len(mine) * HEAD_DIM]).astype(bf16)
            for i, (u, _) in enumerate(mine):
                xb[u] = got[:, i * HEAD_DIM : (i + 1) * HEAD_DIM]


def join_kernel(b0, b1, b2, b3, d):
    e = lax.axis_index("exp")
    for m, b in enumerate((b0, b1, b2, b3)):
        d[e ^ m] = b[...]


def regroup_kernel(route, a0, a1, a2, a3, c0, c1, c2, c3):
    e = lax.axis_index("exp")
    core = e % 2
    cap = c0.shape[2]
    over_z, _ = units(HEADS // KV_HEADS)
    for j in range(2):
        marks = route[2 * j + core][0:1]
        pick = jnp.concatenate([expert_rows(marks, (e ^ m) * cap, cap) for m in range(4)], axis=0)
        for u, (i, _) in enumerate(over_z):
            if i == j:
                for n, a in enumerate((a0, a1, a2, a3)):
                    got = dot(pick, a[u]).astype(bf16)
                    for m, c in enumerate((c0, c1, c2, c3)):
                        c[n, u] = got[m * cap : (m + 1) * cap]


def expert_kernel(
    c0, c1, c2, c3, d0, d1, d2, d3, gain, wg, wu, wd,
    y0, y1, y2, y3, t0, t1, t2, t3, xs, ns, ys,
):
    z, e = lax.axis_index("ctx"), lax.axis_index("exp")
    slices, blocks, cap, wide = xs.shape
    rows = blocks * cap
    over_z, over_x = units(HEADS // KV_HEADS)

    def lanes_of(h):
        return slice(h * HEAD_DIM, (h + 1) * HEAD_DIM)

    for m, d in enumerate((d0, d1, d2, d3)):
        for src in range(4):
            for u, (j, h) in enumerate(over_x):
                xs[4 * (src // 2) + (z ^ m), 2 * j + src % 2, :, lanes_of(h)] = d[src, u]
    for m, c in enumerate((c0, c1, c2, c3)):
        src = e ^ m
        for n in range(4):
            for u, (j, h) in enumerate(over_z):
                xs[4 * (src // 2) + (z ^ n), 2 * j + src % 2, :, lanes_of(h)] = c[n, u]
    total = jnp.zeros((rows, 1), f32)
    for s in range(slices):
        v = xs[s].reshape(rows, wide).astype(f32)
        total += jnp.sum(v * v, axis=1, keepdims=True)
    scale = lax.rsqrt(total * (1.0 / (slices * wide)) + 1e-05)
    for s in range(slices):
        v = xs[s].reshape(rows, wide).astype(f32)
        lanes = slice(s * wide, (s + 1) * wide)
        ns[:, lanes] = (v * scale * gain[0:1, lanes]).astype(bf16)
    normed = ns[...]
    gate = dot_nt(normed, wg[...])
    upper = dot_nt(normed, wu[...])
    hidden = (gate / (1.0 + jnp.exp(-gate)) * upper).astype(bf16)
    owners = ys.shape[0]
    span = ys.shape[2]
    mine = iota((rows, span), 0) // cap == z
    for o in range(owners):
        lanes = slice(o * span, (o + 1) * span)
        v = dot(hidden, wd[:, lanes])
        ys[o] = (v + jnp.where(mine, ns[:, lanes].astype(f32), 0.0)).astype(bf16)
    keep = y0.shape[1]
    for m, (y, t) in enumerate(zip((y0, y1, y2, y3), (t0, t1, t2, t3))):
        y[...] = ys[e ^ m, :, 0:keep]
        for o in range(owners):
            t[o] = ys[o, pl.ds(pl.multiple_of((z ^ m) * cap, cap), cap), keep:]


def turn_kernel(route, y0, y1, y2, y3, g0, g1, g2, g3):
    z, e = lax.axis_index("ctx"), lax.axis_index("exp")
    cap = y0.shape[0] // 4
    for m, g in enumerate((g0, g1, g2, g3)):
        block = z ^ m
        marks = route[block][0:1]
        pick = jnp.concatenate([expert_rows(marks, (e ^ n) * cap, cap) for n in range(4)], axis=0)
        at = pl.ds(pl.multiple_of(block * cap, cap), cap)
        got = jnp.concatenate([y[at, :] for y in (y0, y1, y2, y3)], axis=0)
        g[...] = dot_tn(pick, got).astype(bf16)


def total_kernel(t0, t1, t2, t3, h0, h1, h2, h3, ts):
    e = lax.axis_index("exp")
    ts[...] = sum(t[...].astype(f32) for t in (t0, t1, t2, t3)).astype(bf16)
    for m, h in enumerate((h0, h1, h2, h3)):
        h[...] = ts[e ^ m]


def final_kernel(route, g0, g1, g2, g3, h0, h1, h2, h3, out):
    z, e = lax.axis_index("ctx"), lax.axis_index("exp")
    cap = h0.shape[0]
    keep = g0.shape[1]
    out[:, 0:keep] = sum(g[...].astype(f32) for g in (g0, g1, g2, g3)).astype(bf16)
    marks = route[z][0:1]
    pick = jnp.concatenate([expert_rows(marks, (e ^ n) * cap, cap) for n in range(4)], axis=0)
    got = jnp.concatenate([h[...] for h in (h0, h1, h2, h3)], axis=0)
    out[:, keep:] = dot_tn(pick, got).astype(bf16)


def paired_path(*args):
    return paired_steps(*args)


def paired_steps(
    queries,
    new_keys,
    new_values,
    cache_keys,
    cache_values,
    offset,
    token_ids,
    expert_table,
    norm_gain,
    w_gate,
    w_up,
    w_down,
):
    n_ctx, n_exp = lax.axis_size("ctx"), lax.axis_size("exp")
    tokens = queries.shape[0]
    cache = cache_keys.shape[0]
    width = new_keys.shape[1]
    group = HEADS // KV_HEADS
    wide = group * HEAD_DIM
    cap = tokens // 2
    span = cache + tokens
    over_z, over_x = units(group)
    own = queries.shape[1]
    back = own * 3 // 8
    keep = own - back
    rows = n_ctx * cap

    def over_ctx(v, m):
        return lax.ppermute(v, "ctx", [(i, i ^ m) for i in range(n_ctx)])

    def over_exp(v, m):
        return lax.ppermute(v, "exp", [(i, i ^ m) for i in range(n_exp)])

    def head_step(v, o):
        pairs = []
        for z in range(n_ctx):
            for e in range(n_exp):
                core = e % 2
                to_z = 2 * core + ((z // 2) ^ o)
                pairs.append((z * n_exp + e, to_z * n_exp + e - core + z % 2))
        return lax.ppermute(v, ("ctx", "exp"), pairs)

    height = span + tokens * wide // width + 8
    copies = 3 + 2 * (4 + wide // width)
    table_rows = expert_table.reshape(-1, 128)
    p0, p1 = call(
        pack_kernel,
        [((height, width), bf16)] * 2,
        8,
        scratch=[
            pltpu.VMEM((8, tokens), jnp.int32),
            pltpu.SMEM((tokens,), jnp.int32),
            pltpu.VMEM(table_rows.shape, jnp.int32),
            pltpu.VMEM((tokens, table_rows.shape[1]), jnp.int32),
            pltpu.SemaphoreType.DMA((copies,)),
        ],
        hbm=7,
    )(queries, new_keys, new_values, cache_keys, cache_values, token_ids, table_rows)
    limit = jnp.broadcast_to(offset[None, :], (8, 128))
    gate_t, up_t, down = jnp.swapaxes(w_gate[0], 0, 1), jnp.swapaxes(w_up[0], 0, 1), w_down[0]
    weight_bytes = 2 * (gate_t.size + up_t.size + down.size)
    gate_t, up_t, down, gain = call(
        fetch_kernel,
        [(w.shape, bf16) for w in (gate_t, up_t, down)] + [((1, norm_gain.shape[0]), f32)],
        4,
        scratch=[pltpu.SemaphoreType.DMA((4,))],
        hbm=4,
        cost=pl.CostEstimate(flops=1000 * weight_bytes, transcendentals=0, bytes_accessed=2 * weight_bytes),
    )(gate_t, up_t, down, norm_gain.reshape(1, -1))
    r0, r1 = head_step(p0, 0), head_step(p1, 1)
    r0, limit = lax.optimization_barrier((r0, limit))
    s0, s1 = over_exp(r0, 1), over_exp(r1, 1)
    za, xb0, xb1, xb2, xb3, route = call(
        functools.partial(attend_kernel, cache, tokens),
        [((len(over_z), tokens, HEAD_DIM), bf16)]
        + [((len(over_x), cap, HEAD_DIM), bf16)] * 4
        + [((n_ctx, 8, tokens), f32)],
        16,
        scratch=[pltpu.VMEM((2, tokens, wide), bf16)],
    )(limit, r0, r1, s0, s1)
    a = [za] + [over_ctx(za, m) for m in (1, 2, 3)]
    b = [xb0] + [over_exp(v, m) for m, v in ((1, xb1), (2, xb2), (3, xb3))]
    (zd,) = call(join_kernel, [((n_exp, len(over_x), cap, HEAD_DIM), bf16)], 4)(*b)
    d = [zd] + [over_ctx(zd, m) for m in (1, 2, 3)]
    c0, c1, c2, c3 = call(
        regroup_kernel, [((n_ctx, len(over_z), cap, HEAD_DIM), bf16)] * 4, 8
    )(route, *a)
    c = [c0] + [over_exp(v, m) for m, v in ((1, c1), (2, c2), (3, c3))]
    outs = call(
        expert_kernel,
        [((rows, keep), bf16)] * 4 + [((n_exp, cap, back), bf16)] * 4,
        28,
        scratch=[
            pltpu.VMEM((KV_HEADS, n_ctx, cap, wide), bf16),
            pltpu.VMEM((rows, KV_HEADS * wide), bf16),
            pltpu.VMEM((n_exp, rows, own), bf16),
        ],
    )(
        *c,
        *d,
        gain,
        gate_t,
        up_t,
        down,
    )
    y, t = outs[:4], outs[4:]
    t = [t[0]] + [over_ctx(t[m], m) for m in (1, 2, 3)]
    y2 = over_exp(y[2], 2)
    y = [y[0], over_exp(y[1], 1), y2, over_exp(y[3], 3)]
    g = call(turn_kernel, [((tokens, keep), bf16)] * 4, 8)(route, *y)
    g = [g[0]] + [over_ctx(g[m], m) for m in (1, 2, 3)]
    h = call(
        total_kernel, [((cap, back), bf16)] * 4, 8, scratch=[pltpu.VMEM((n_exp, cap, back), bf16)]
    )(*t)
    h = [h[0]] + [over_exp(h[m], m) for m in (1, 2, 3)]
    (out,) = call(final_kernel, [((tokens, own), bf16)], 8)(route, *g, *h)
    return out


def solution(mesh):
    placed = (
        P(("group", "ctx"), "exp"),
        P(("group", "ctx"), "exp"),
        P(("group", "ctx"), "exp"),
        P(("group", "ctx"), "exp"),
        P(("group", "ctx"), "exp"),
        P("group"),
        P(("group", "ctx")),
        P("group"),
        P(),
        P("exp", None, "ctx"),
        P("exp", None, "ctx"),
        P("exp", "ctx", None),
    )
    n_ctx, n_exp = mesh.shape["ctx"], mesh.shape["exp"]
    paired = n_ctx == n_exp == 4 and KV_HEADS == 2 * n_exp
    return jax.shard_map(
        paired_path if paired else general_path,
        mesh=mesh,
        in_specs=placed,
        out_specs=P(("group", "ctx"), "exp"),
        check_vma=False,
    )
```

```python
import functools
import math

import jax
import jax.numpy as jnp
from jax import lax
from jax.experimental import pallas as pl
from jax.experimental.pallas import tpu as pltpu
from jax.sharding import PartitionSpec as P


HEADS = 32
KV_HEADS = 8
HEAD_DIM = 128


masked_score = -1e30
f32 = jnp.float32
bf16 = jnp.bfloat16


def split_heads(flat, heads):
    return flat.reshape(flat.shape[0], heads, flat.shape[1] // heads)


def partial_attend(query_rows, key_rows, value_rows, allowed):
    width = query_rows.shape[3]
    scores = jnp.einsum("rkgd,skd->rkgs", query_rows, key_rows, preferred_element_type=jnp.float32)
    scores = scores * (1.0 / math.sqrt(width))
    usable = allowed[:, None, None, :]
    peak = jnp.max(jnp.where(usable, scores, masked_score), axis=-1)
    unnorm = jnp.where(usable, jnp.exp(scores - peak[..., None]), 0.0)
    total = jnp.sum(unnorm, axis=-1)
    numer = jnp.einsum(
        "rkgs,skd->rkgd",
        unnorm.astype(jnp.bfloat16),
        value_rows,
        preferred_element_type=jnp.float32,
    )
    return (numer, peak, total)


def general_path(
    queries,
    new_keys,
    new_values,
    cache_keys,
    cache_values,
    offset,
    token_ids,
    expert_table,
    norm_gain,
    w_gate,
    w_up,
    w_down,
):
    owners = lax.axis_size("exp")
    heads_local = HEADS // owners
    kv_local = KV_HEADS // owners
    group = HEADS // KV_HEADS
    tok_count = queries.shape[0]
    cache_len = cache_keys.shape[0]
    shard = lax.axis_index("ctx")
    limit = offset[0]
    key_rows = jnp.concatenate([cache_keys, new_keys], axis=0)
    value_rows = jnp.concatenate([cache_values, new_values], axis=0)
    span = key_rows.shape[0]
    own_index = shard * tok_count + jnp.arange(tok_count, dtype=jnp.int32)
    grouped = queries.reshape(tok_count, kv_local, group, HEAD_DIM)
    piece_keys = lax.all_gather(key_rows, "ctx", axis=0, tiled=True)
    piece_values = lax.all_gather(value_rows, "ctx", axis=0, tiled=True)
    flat = jnp.arange(piece_keys.shape[0], dtype=jnp.int32)
    source = flat // span
    inner = flat % span
    cache_ok = source * cache_len + inner < limit
    stretch_ok = (source * tok_count + inner - cache_len)[None, :] <= own_index[:, None]
    allowed = jnp.where((inner < cache_len)[None, :], cache_ok[None, :], stretch_ok)
    numer, _, total = partial_attend(
        grouped, split_heads(piece_keys, kv_local), split_heads(piece_values, kv_local), allowed
    )
    attended = (numer / total[..., None]).reshape(tok_count, heads_local * HEAD_DIM).astype(jnp.bfloat16)
    capacity = tok_count // 2
    chosen = expert_table[token_ids]
    onehot = (chosen[:, None] == jnp.arange(owners, dtype=jnp.int32)[None, :]).astype(jnp.int32)
    earlier = jnp.cumsum(onehot, axis=0) - onehot
    slot = jnp.sum(earlier * onehot, axis=1)
    target = chosen * capacity + slot
    dispatch = (jnp.arange(owners * capacity, dtype=jnp.int32)[:, None] == target[None, :]).astype(
        jnp.bfloat16
    )
    packed = jnp.dot(dispatch, attended, preferred_element_type=jnp.float32).astype(jnp.bfloat16)
    arrived = lax.all_to_all(packed, "exp", split_axis=0, concat_axis=1, tiled=True)
    values32 = arrived.astype(jnp.float32)
    scale = lax.rsqrt(jnp.mean(values32 * values32, axis=-1, keepdims=True) + 1e-05)
    normed = (values32 * scale * norm_gain).astype(jnp.bfloat16)
    piece = lax.all_gather(normed, "ctx", axis=0, tiled=True)
    gate = jnp.dot(piece, w_gate[0], preferred_element_type=jnp.float32)
    upper = jnp.dot(piece, w_up[0], preferred_element_type=jnp.float32)
    hidden = (jax.nn.silu(gate) * upper).astype(jnp.bfloat16)
    summed = lax.psum_scatter(
        jnp.dot(hidden, w_down[0], preferred_element_type=jnp.float32).astype(jnp.bfloat16),
        "ctx",
        scatter_dimension=0,
        tiled=True,
    ).astype(jnp.float32)
    combined = (normed.astype(jnp.float32) + summed).astype(jnp.bfloat16)
    returned = lax.all_to_all(combined, "exp", split_axis=1, concat_axis=0, tiled=True)
    collect = (target[:, None] == jnp.arange(owners * capacity, dtype=jnp.int32)[None, :]).astype(
        jnp.bfloat16
    )
    return jnp.dot(collect, returned, preferred_element_type=jnp.float32).astype(jnp.bfloat16)


def iota(shape, axis):
    return lax.broadcasted_iota(jnp.int32, shape, axis)


def call(kernel, out_shapes, mib, scratch=(), hbm=0, cost=None):
    def run(*args):
        args = [pltpu.with_memory_space_constraint(v, pltpu.HBM) if i < hbm else v for i, v in enumerate(args)]
        vmem = pl.BlockSpec(memory_space=pltpu.VMEM)
        specs = [pl.BlockSpec(memory_space=pltpu.HBM)] * hbm + [vmem] * (len(args) - hbm)
        return pl.pallas_call(
            kernel,
            out_shape=[jax.ShapeDtypeStruct(s, d) for s, d in out_shapes],
            in_specs=specs,
            out_specs=[vmem] * len(out_shapes),
            scratch_shapes=list(scratch),
            compiler_params=pltpu.CompilerParams(vmem_limit_bytes=mib << 20),
            cost_estimate=cost,
        )(*args)

    return run


def expert_rows(marks, first, cap):
    tokens = marks.shape[1]
    slots = (iota((cap, tokens), 0) + first).astype(f32)
    return (marks == slots).astype(bf16)


def dot(a, b):
    return jnp.dot(a, b, preferred_element_type=f32)


def dot_nt(a, b):
    return lax.dot_general(a, b, (((1,), (1,)), ((), ())), preferred_element_type=f32)


def dot_tn(a, b):
    return lax.dot_general(a, b, (((0,), (0,)), ((), ())), preferred_element_type=f32)


def pack_kernel(q, nk, nv, ck, cv, ids, table, p0, p1, id_row, id_smem, rows, found, sems):
    z = lax.axis_index("ctx")
    tokens, cache = q.shape[0], ck.shape[0]
    span = cache + tokens
    width = p0.shape[1]
    wide = q.shape[1] // 2
    cap = tokens // 2
    top = span + (wide // width) * tokens
    lanes = found.shape[1]
    swap = (z // 2) == 1

    first = [
        pltpu.make_async_copy(ids, id_smem, sems.at[0]),
        pltpu.make_async_copy(ids, id_row.at[0], sems.at[1]),
        pltpu.make_async_copy(table, rows, sems.at[2]),
    ]
    for copy in first:
        copy.start()

    def pieces(p, h, base):
        at = pl.ds(h * HEAD_DIM, HEAD_DIM)
        moves = [
            (ck.at[:, at], p.at[0:cache, 0:HEAD_DIM]),
            (cv.at[:, at], p.at[0:cache, HEAD_DIM:]),
            (nk.at[:, at], p.at[cache:span, 0:HEAD_DIM]),
            (nv.at[:, at], p.at[cache:span, HEAD_DIM:]),
        ]
        for part in range(wide // width):
            lo = h * wide + part * width
            moves.append((q.at[:, pl.ds(lo, width)], p.at[span + part * tokens : span + (part + 1) * tokens, :]))
        return [pltpu.make_async_copy(src, dst, sems.at[base + i]) for i, (src, dst) in enumerate(moves)]

    count = 4 + wide // width

    @pl.when(jnp.logical_not(swap))
    def _():
        for copy in pieces(p0, 0, 3) + pieces(p1, 1, 3 + count):
            copy.start()

    @pl.when(swap)
    def _():
        for copy in pieces(p0, 1, 3) + pieces(p1, 0, 3 + count):
            copy.start()

    for copy in first:
        copy.wait()
    for t in range(tokens):
        found[t : t + 1, :] = rows[pl.ds(id_smem[t] // lanes, 1), :]
    same = iota((tokens, tokens), 0) == iota((tokens, tokens), 1)
    id_col = jnp.sum(jnp.where(same, (id_row[0:1, :] % lanes).astype(f32), 0.0), axis=1, keepdims=True)
    hit = iota((tokens, lanes), 1).astype(f32) == id_col
    who = jnp.sum(jnp.where(hit, found[...].astype(f32), 0.0), axis=1, keepdims=True)
    expert = iota((tokens, 128), 1).astype(f32)
    onehot = (who == expert).astype(f32)
    before = (iota((tokens, tokens), 1) < iota((tokens, tokens), 0)).astype(bf16)
    rank = dot(before, onehot.astype(bf16))
    target = jnp.sum(onehot * (expert * cap + rank), axis=1, keepdims=True)
    marks = jnp.sum(jnp.where(same, target, 0.0), axis=0, keepdims=True)
    for p in (p0, p1):
        p[top:, :tokens] = jnp.broadcast_to(marks, (p.shape[0] - top, tokens)).astype(bf16)
    for copy in pieces(p0, 0, 3) + pieces(p1, 1, 3 + count):
        copy.wait()


def fetch_kernel(wg, wu, wd, gain, og, ou, od, ogain, sems):
    copies = [
        pltpu.make_async_copy(src, dst, sems.at[i])
        for i, (src, dst) in enumerate(((wg, og), (wu, ou), (wd, od), (gain, ogain)))
    ]
    for copy in copies:
        copy.start()
    for copy in copies:
        copy.wait()


def units(heads):
    lots = [(j, h) for j in range(2) for h in range(heads)]
    early = [(j, h) for j, h in lots if h >= heads - 1]
    return [lot for lot in lots if lot not in early], early


def attend_kernel(cache, tokens, offset, r0, r1, s0, s1, za, xb0, xb1, xb2, xb3, route, held):
    z, e = lax.axis_index("ctx"), lax.axis_index("exp")
    core = e % 2
    span = cache + tokens
    cap = tokens // 2
    width = r0.shape[1]
    group = HEADS // KV_HEADS
    per_row = width // HEAD_DIM
    top = span + (group // per_row) * tokens
    limit = offset[0:1, 0:1]
    scale = 1.0 / math.sqrt(HEAD_DIM)
    halves = (z % 2, 1 - z % 2)
    keys = [(r, 2 * hi + core) for r, hi in zip((r0, r1), halves)]
    keys += [(s, 2 * hi + 1 - core) for s, hi in zip((s0, s1), halves)]
    rows = group * tokens
    pos = iota((rows, span), 0) % tokens
    col = iota((rows, span), 1)
    for ref, block in keys:
        route[block] = ref[top:, :tokens].astype(f32)
    for r, hi in zip((r0, r1), halves):
        base = (2 * hi + core) * tokens
        q = jnp.concatenate(
            [
                r[span + (g // per_row) * tokens : span + (g // per_row + 1) * tokens,
                  (g % per_row) * HEAD_DIM : (g % per_row + 1) * HEAD_DIM]
                for g in range(group)
            ],
            axis=0,
        )
        scores = []
        for ref, block in keys:
            s = dot_nt(q, ref[0:span, 0:HEAD_DIM]) * scale
            edge = jnp.where(col < cache, limit - block * cache, pos + (base - block * tokens + cache + 1))
            scores.append(jnp.where(col < edge, s, masked_score))
        peak = functools.reduce(jnp.maximum, [jnp.max(s, axis=1, keepdims=True) for s in scores])
        total = jnp.zeros((rows, 1), f32)
        numer = jnp.zeros((rows, HEAD_DIM), f32)
        for (ref, _), s in zip(keys, scores):
            w = jnp.exp(s - peak)
            total += jnp.sum(w, axis=1, keepdims=True)
            numer += dot(w.astype(bf16), ref[0:span, HEAD_DIM:])
        out = (numer / total).astype(bf16)
        held[hi] = jnp.concatenate([out[g * tokens : (g + 1) * tokens] for g in range(group)], axis=1)
    over_z, over_x = units(group)
    for u, (j, h) in enumerate(over_z):
        za[u] = held[j, :, h * HEAD_DIM : (h + 1) * HEAD_DIM]
    for m, xb in enumerate((xb0, xb1, xb2, xb3)):
        for j in range(2):
            pick = expert_rows(route[2 * j + core][0:1], (e ^ m) * cap, cap)
            mine = [(u, h) for u, (i, h) in enumerate(over_x) if i == j]
            lo = mine[0][1] * HEAD_DIM
            got = dot(pick, held[j, :, lo : lo + len(mine) * HEAD_DIM]).astype(bf16)
            for i, (u, _) in enumerate(mine):
                xb[u] = got[:, i * HEAD_DIM : (i + 1) * HEAD_DIM]


def join_kernel(b0, b1, b2, b3, d):
    e = lax.axis_index("exp")
    for m, b in enumerate((b0, b1, b2, b3)):
        d[e ^ m] = b[...]


def regroup_kernel(route, a0, a1, a2, a3, c0, c1, c2, c3):
    e = lax.axis_index("exp")
    core = e % 2
    cap = c0.shape[2]
    over_z, _ = units(HEADS // KV_HEADS)
    for j in range(2):
        marks = route[2 * j + core][0:1]
        pick = jnp.concatenate([expert_rows(marks, (e ^ m) * cap, cap) for m in range(4)], axis=0)
        for u, (i, _) in enumerate(over_z):
            if i == j:
                for n, a in enumerate((a0, a1, a2, a3)):
                    got = dot(pick, a[u]).astype(bf16)
                    for m, c in enumerate((c0, c1, c2, c3)):
                        c[n, u] = got[m * cap : (m + 1) * cap]


def expert_kernel(
    c0, c1, c2, c3, d0, d1, d2, d3, gain, wg, wu, wd,
    y0, y1, y2, y3, t0, t1, t2, t3, xs, ns, ys,
):
    z, e = lax.axis_index("ctx"), lax.axis_index("exp")
    slices, blocks, cap, wide = xs.shape
    rows = blocks * cap
    over_z, over_x = units(HEADS // KV_HEADS)

    def lanes_of(h):
        return slice(h * HEAD_DIM, (h + 1) * HEAD_DIM)

    for m, d in enumerate((d0, d1, d2, d3)):
        for src in range(4):
            for u, (j, h) in enumerate(over_x):
                xs[4 * (src // 2) + (z ^ m), 2 * j + src % 2, :, lanes_of(h)] = d[src, u]
    for m, c in enumerate((c0, c1, c2, c3)):
        src = e ^ m
        for n in range(4):
            for u, (j, h) in enumerate(over_z):
                xs[4 * (src // 2) + (z ^ n), 2 * j + src % 2, :, lanes_of(h)] = c[n, u]
    total = jnp.zeros((rows, 1), f32)
    for s in range(slices):
        v = xs[s].reshape(rows, wide).astype(f32)
        total += jnp.sum(v * v, axis=1, keepdims=True)
    scale = lax.rsqrt(total * (1.0 / (slices * wide)) + 1e-05)
    for s in range(slices):
        v = xs[s].reshape(rows, wide).astype(f32)
        lanes = slice(s * wide, (s + 1) * wide)
        ns[:, lanes] = (v * scale * gain[0:1, lanes]).astype(bf16)
    normed = ns[...]
    gate = dot_nt(normed, wg[...])
    upper = dot_nt(normed, wu[...])
    hidden = (gate / (1.0 + jnp.exp(-gate)) * upper).astype(bf16)
    owners = ys.shape[0]
    span = ys.shape[2]
    mine = iota((rows, span), 0) // cap == z
    for o in range(owners):
        lanes = slice(o * span, (o + 1) * span)
        v = dot(hidden, wd[:, lanes])
        ys[o] = (v + jnp.where(mine, ns[:, lanes].astype(f32), 0.0)).astype(bf16)
    keep = y0.shape[1]
    for m, (y, t) in enumerate(zip((y0, y1, y2, y3), (t0, t1, t2, t3))):
        y[...] = ys[e ^ m, :, 0:keep]
        for o in range(owners):
            t[o] = ys[o, pl.ds(pl.multiple_of((z ^ m) * cap, cap), cap), keep:]


def turn_kernel(route, y0, y1, y2, y3, g0, g1, g2, g3):
    z, e = lax.axis_index("ctx"), lax.axis_index("exp")
    cap = y0.shape[0] // 4
    for m, g in enumerate((g0, g1, g2, g3)):
        block = z ^ m
        marks = route[block][0:1]
        pick = jnp.concatenate([expert_rows(marks, (e ^ n) * cap, cap) for n in range(4)], axis=0)
        at = pl.ds(pl.multiple_of(block * cap, cap), cap)
        got = jnp.concatenate([y[at, :] for y in (y0, y1, y2, y3)], axis=0)
        g[...] = dot_tn(pick, got).astype(bf16)


def total_kernel(t0, t1, t2, t3, h0, h1, h2, h3, ts):
    e = lax.axis_index("exp")
    ts[...] = sum(t[...].astype(f32) for t in (t0, t1, t2, t3)).astype(bf16)
    for m, h in enumerate((h0, h1, h2, h3)):
        h[...] = ts[e ^ m]


def final_kernel(route, g0, g1, g2, g3, h0, h1, h2, h3, out):
    z, e = lax.axis_index("ctx"), lax.axis_index("exp")
    cap = h0.shape[0]
    keep = g0.shape[1]
    out[:, 0:keep] = sum(g[...].astype(f32) for g in (g0, g1, g2, g3)).astype(bf16)
    marks = route[z][0:1]
    pick = jnp.concatenate([expert_rows(marks, (e ^ n) * cap, cap) for n in range(4)], axis=0)
    got = jnp.concatenate([h[...] for h in (h0, h1, h2, h3)], axis=0)
    out[:, keep:] = dot_tn(pick, got).astype(bf16)


def paired_path(*args):
    return paired_steps(*args)


def paired_steps(
    queries,
    new_keys,
    new_values,
    cache_keys,
    cache_values,
    offset,
    token_ids,
    expert_table,
    norm_gain,
    w_gate,
    w_up,
    w_down,
):
    n_ctx, n_exp = lax.axis_size("ctx"), lax.axis_size("exp")
    tokens = queries.shape[0]
    cache = cache_keys.shape[0]
    width = new_keys.shape[1]
    group = HEADS // KV_HEADS
    wide = group * HEAD_DIM
    cap = tokens // 2
    span = cache + tokens
    over_z, over_x = units(group)
    own = queries.shape[1]
    back = own * 3 // 8
    keep = own - back
    rows = n_ctx * cap

    def over_ctx(v, m):
        return lax.ppermute(v, "ctx", [(i, i ^ m) for i in range(n_ctx)])

    def over_exp(v, m):
        return lax.ppermute(v, "exp", [(i, i ^ m) for i in range(n_exp)])

    def head_step(v, o):
        pairs = []
        for z in range(n_ctx):
            for e in range(n_exp):
                core = e % 2
                to_z = 2 * core + ((z // 2) ^ o)
                pairs.append((z * n_exp + e, to_z * n_exp + e - core + z % 2))
        return lax.ppermute(v, ("ctx", "exp"), pairs)

    height = span + tokens * wide // width + 8
    copies = 3 + 2 * (4 + wide // width)
    table_rows = expert_table.reshape(-1, 128)
    p0, p1 = call(
        pack_kernel,
        [((height, width), bf16)] * 2,
        8,
        scratch=[
            pltpu.VMEM((8, tokens), jnp.int32),
            pltpu.SMEM((tokens,), jnp.int32),
            pltpu.VMEM(table_rows.shape, jnp.int32),
            pltpu.VMEM((tokens, table_rows.shape[1]), jnp.int32),
            pltpu.SemaphoreType.DMA((copies,)),
        ],
        hbm=7,
    )(queries, new_keys, new_values, cache_keys, cache_values, token_ids, table_rows)
    limit = jnp.broadcast_to(offset[None, :], (8, 128))
    gate_t, up_t, down = jnp.swapaxes(w_gate[0], 0, 1), jnp.swapaxes(w_up[0], 0, 1), w_down[0]
    weight_bytes = 2 * (gate_t.size + up_t.size + down.size)
    gate_t, up_t, down, gain = call(
        fetch_kernel,
        [(w.shape, bf16) for w in (gate_t, up_t, down)] + [((1, norm_gain.shape[0]), f32)],
        4,
        scratch=[pltpu.SemaphoreType.DMA((4,))],
        hbm=4,
        cost=pl.CostEstimate(flops=1000 * weight_bytes, transcendentals=0, bytes_accessed=2 * weight_bytes),
    )(gate_t, up_t, down, norm_gain.reshape(1, -1))
    r0, r1 = head_step(p0, 0), head_step(p1, 1)
    r0, limit = lax.optimization_barrier((r0, limit))
    s0, s1 = over_exp(r0, 1), over_exp(r1, 1)
    za, xb0, xb1, xb2, xb3, route = call(
        functools.partial(attend_kernel, cache, tokens),
        [((len(over_z), tokens, HEAD_DIM), bf16)]
        + [((len(over_x), cap, HEAD_DIM), bf16)] * 4
        + [((n_ctx, 8, tokens), f32)],
        16,
        scratch=[pltpu.VMEM((2, tokens, wide), bf16)],
    )(limit, r0, r1, s0, s1)
    a = [za] + [over_ctx(za, m) for m in (1, 2, 3)]
    b = [xb0] + [over_exp(v, m) for m, v in ((1, xb1), (2, xb2), (3, xb3))]
    (zd,) = call(join_kernel, [((n_exp, len(over_x), cap, HEAD_DIM), bf16)], 4)(*b)
    d = [zd] + [over_ctx(zd, m) for m in (1, 2, 3)]
    c0, c1, c2, c3 = call(regroup_kernel, [((n_ctx, len(over_z), cap, HEAD_DIM), bf16)] * 4, 8)(route, *a)
    c = [c0] + [over_exp(v, m) for m, v in ((1, c1), (2, c2), (3, c3))]
    outs = call(
        expert_kernel,
        [((rows, keep), bf16)] * 4 + [((n_exp, cap, back), bf16)] * 4,
        28,
        scratch=[
            pltpu.VMEM((KV_HEADS, n_ctx, cap, wide), bf16),
            pltpu.VMEM((rows, KV_HEADS * wide), bf16),
            pltpu.VMEM((n_exp, rows, own), bf16),
        ],
    )(
        *c,
        *d,
        gain,
        gate_t,
        up_t,
        down,
    )
    y, t = outs[:4], outs[4:]
    t = [t[0]] + [over_ctx(t[m], m) for m in (1, 2, 3)]
    y = [y[0]] + [over_exp(y[m], m) for m in (1, 2, 3)]
    g = call(turn_kernel, [((tokens, keep), bf16)] * 4, 8)(route, *y)
    g = [g[0]] + [over_ctx(g[m], m) for m in (1, 2, 3)]
    h = call(total_kernel, [((cap, back), bf16)] * 4, 8, scratch=[pltpu.VMEM((n_exp, cap, back), bf16)])(*t)
    h = [h[0]] + [over_exp(h[m], m) for m in (1, 2, 3)]
    (out,) = call(final_kernel, [((tokens, own), bf16)], 8)(route, *g, *h)
    return out


def solution(mesh):
    placed = (
        P(("group", "ctx"), "exp"),
        P(("group", "ctx"), "exp"),
        P(("group", "ctx"), "exp"),
        P(("group", "ctx"), "exp"),
        P(("group", "ctx"), "exp"),
        P("group"),
        P(("group", "ctx")),
        P("group"),
        P(),
        P("exp", None, "ctx"),
        P("exp", None, "ctx"),
        P("exp", "ctx", None),
    )
    n_ctx, n_exp = mesh.shape["ctx"], mesh.shape["exp"]
    paired = n_ctx == n_exp == 4 and KV_HEADS == 2 * n_exp
    return jax.shard_map(
        paired_path if paired else general_path,
        mesh=mesh,
        in_specs=placed,
        out_specs=P(("group", "ctx"), "exp"),
        check_vma=False,
    )
```

```python
import functools
import math

import jax
import jax.numpy as jnp
from jax import lax
from jax.experimental import pallas as pl
from jax.experimental.pallas import tpu as pltpu
from jax.sharding import PartitionSpec as P


HEADS = 32
KV_HEADS = 8
HEAD_DIM = 128


masked_score = -1e30
f32 = jnp.float32
bf16 = jnp.bfloat16


def split_heads(flat, heads):
    return flat.reshape(flat.shape[0], heads, flat.shape[1] // heads)


def partial_attend(query_rows, key_rows, value_rows, allowed):
    width = query_rows.shape[3]
    scores = jnp.einsum("rkgd,skd->rkgs", query_rows, key_rows, preferred_element_type=jnp.float32)
    scores = scores * (1.0 / math.sqrt(width))
    usable = allowed[:, None, None, :]
    peak = jnp.max(jnp.where(usable, scores, masked_score), axis=-1)
    unnorm = jnp.where(usable, jnp.exp(scores - peak[..., None]), 0.0)
    total = jnp.sum(unnorm, axis=-1)
    numer = jnp.einsum(
        "rkgs,skd->rkgd",
        unnorm.astype(jnp.bfloat16),
        value_rows,
        preferred_element_type=jnp.float32,
    )
    return (numer, peak, total)


def general_path(
    queries,
    new_keys,
    new_values,
    cache_keys,
    cache_values,
    offset,
    token_ids,
    expert_table,
    norm_gain,
    w_gate,
    w_up,
    w_down,
):
    owners = lax.axis_size("exp")
    heads_local = HEADS // owners
    kv_local = KV_HEADS // owners
    group = HEADS // KV_HEADS
    tok_count = queries.shape[0]
    cache_len = cache_keys.shape[0]
    shard = lax.axis_index("ctx")
    limit = offset[0]
    key_rows = jnp.concatenate([cache_keys, new_keys], axis=0)
    value_rows = jnp.concatenate([cache_values, new_values], axis=0)
    span = key_rows.shape[0]
    own_index = shard * tok_count + jnp.arange(tok_count, dtype=jnp.int32)
    grouped = queries.reshape(tok_count, kv_local, group, HEAD_DIM)
    piece_keys = lax.all_gather(key_rows, "ctx", axis=0, tiled=True)
    piece_values = lax.all_gather(value_rows, "ctx", axis=0, tiled=True)
    flat = jnp.arange(piece_keys.shape[0], dtype=jnp.int32)
    source = flat // span
    inner = flat % span
    cache_ok = source * cache_len + inner < limit
    stretch_ok = (source * tok_count + inner - cache_len)[None, :] <= own_index[:, None]
    allowed = jnp.where((inner < cache_len)[None, :], cache_ok[None, :], stretch_ok)
    numer, _, total = partial_attend(
        grouped, split_heads(piece_keys, kv_local), split_heads(piece_values, kv_local), allowed
    )
    attended = (numer / total[..., None]).reshape(tok_count, heads_local * HEAD_DIM).astype(jnp.bfloat16)
    capacity = tok_count // 2
    chosen = expert_table[token_ids]
    onehot = (chosen[:, None] == jnp.arange(owners, dtype=jnp.int32)[None, :]).astype(jnp.int32)
    earlier = jnp.cumsum(onehot, axis=0) - onehot
    slot = jnp.sum(earlier * onehot, axis=1)
    target = chosen * capacity + slot
    dispatch = (jnp.arange(owners * capacity, dtype=jnp.int32)[:, None] == target[None, :]).astype(
        jnp.bfloat16
    )
    packed = jnp.dot(dispatch, attended, preferred_element_type=jnp.float32).astype(jnp.bfloat16)
    arrived = lax.all_to_all(packed, "exp", split_axis=0, concat_axis=1, tiled=True)
    values32 = arrived.astype(jnp.float32)
    scale = lax.rsqrt(jnp.mean(values32 * values32, axis=-1, keepdims=True) + 1e-05)
    normed = (values32 * scale * norm_gain).astype(jnp.bfloat16)
    piece = lax.all_gather(normed, "ctx", axis=0, tiled=True)
    gate = jnp.dot(piece, w_gate[0], preferred_element_type=jnp.float32)
    upper = jnp.dot(piece, w_up[0], preferred_element_type=jnp.float32)
    hidden = (jax.nn.silu(gate) * upper).astype(jnp.bfloat16)
    summed = lax.psum_scatter(
        jnp.dot(hidden, w_down[0], preferred_element_type=jnp.float32).astype(jnp.bfloat16),
        "ctx",
        scatter_dimension=0,
        tiled=True,
    ).astype(jnp.float32)
    combined = (normed.astype(jnp.float32) + summed).astype(jnp.bfloat16)
    returned = lax.all_to_all(combined, "exp", split_axis=1, concat_axis=0, tiled=True)
    collect = (target[:, None] == jnp.arange(owners * capacity, dtype=jnp.int32)[None, :]).astype(
        jnp.bfloat16
    )
    return jnp.dot(collect, returned, preferred_element_type=jnp.float32).astype(jnp.bfloat16)


def iota(shape, axis):
    return lax.broadcasted_iota(jnp.int32, shape, axis)


def call(kernel, out_shapes, mib, scratch=(), hbm=0, cost=None):
    def run(*args):
        args = [pltpu.with_memory_space_constraint(v, pltpu.HBM) if i < hbm else v for i, v in enumerate(args)]
        vmem = pl.BlockSpec(memory_space=pltpu.VMEM)
        specs = [pl.BlockSpec(memory_space=pltpu.HBM)] * hbm + [vmem] * (len(args) - hbm)
        return pl.pallas_call(
            kernel,
            out_shape=[jax.ShapeDtypeStruct(s, d) for s, d in out_shapes],
            in_specs=specs,
            out_specs=[vmem] * len(out_shapes),
            scratch_shapes=list(scratch),
            compiler_params=pltpu.CompilerParams(vmem_limit_bytes=mib << 20),
            cost_estimate=cost,
        )(*args)

    return run


def expert_rows(marks, first, cap):
    tokens = marks.shape[1]
    slots = (iota((cap, tokens), 0) + first).astype(f32)
    return (marks == slots).astype(bf16)


def dot(a, b):
    return jnp.dot(a, b, preferred_element_type=f32)


def dot_nt(a, b):
    return lax.dot_general(a, b, (((1,), (1,)), ((), ())), preferred_element_type=f32)


def dot_tn(a, b):
    return lax.dot_general(a, b, (((0,), (0,)), ((), ())), preferred_element_type=f32)


def pack_kernel(q, nk, nv, ck, cv, ids, table, p0, p1, id_row, id_smem, rows, found, sems):
    z = lax.axis_index("ctx")
    tokens, cache = q.shape[0], ck.shape[0]
    span = cache + tokens
    width = p0.shape[1]
    wide = q.shape[1] // 2
    cap = tokens // 2
    top = span + (wide // width) * tokens
    lanes = found.shape[1]
    swap = (z // 2) == 1

    first = [
        pltpu.make_async_copy(ids, id_smem, sems.at[0]),
        pltpu.make_async_copy(ids, id_row.at[0], sems.at[1]),
        pltpu.make_async_copy(table, rows, sems.at[2]),
    ]
    for copy in first:
        copy.start()

    def pieces(p, h, base):
        at = pl.ds(h * HEAD_DIM, HEAD_DIM)
        moves = [
            (ck.at[:, at], p.at[0:cache, 0:HEAD_DIM]),
            (cv.at[:, at], p.at[0:cache, HEAD_DIM:]),
            (nk.at[:, at], p.at[cache:span, 0:HEAD_DIM]),
            (nv.at[:, at], p.at[cache:span, HEAD_DIM:]),
        ]
        for part in range(wide // width):
            lo = h * wide + part * width
            moves.append((q.at[:, pl.ds(lo, width)], p.at[span + part * tokens : span + (part + 1) * tokens, :]))
        return [pltpu.make_async_copy(src, dst, sems.at[base + i]) for i, (src, dst) in enumerate(moves)]

    count = 4 + wide // width

    @pl.when(jnp.logical_not(swap))
    def _():
        for copy in pieces(p0, 0, 3) + pieces(p1, 1, 3 + count):
            copy.start()

    @pl.when(swap)
    def _():
        for copy in pieces(p0, 1, 3) + pieces(p1, 0, 3 + count):
            copy.start()

    for copy in first:
        copy.wait()
    for t in range(tokens):
        found[t : t + 1, :] = rows[pl.ds(id_smem[t] // lanes, 1), :]
    same = iota((tokens, tokens), 0) == iota((tokens, tokens), 1)
    id_col = jnp.sum(jnp.where(same, (id_row[0:1, :] % lanes).astype(f32), 0.0), axis=1, keepdims=True)
    hit = iota((tokens, lanes), 1).astype(f32) == id_col
    who = jnp.sum(jnp.where(hit, found[...].astype(f32), 0.0), axis=1, keepdims=True)
    expert = iota((tokens, 128), 1).astype(f32)
    onehot = (who == expert).astype(f32)
    before = (iota((tokens, tokens), 1) < iota((tokens, tokens), 0)).astype(bf16)
    rank = dot(before, onehot.astype(bf16))
    target = jnp.sum(onehot * (expert * cap + rank), axis=1, keepdims=True)
    marks = jnp.sum(jnp.where(same, target, 0.0), axis=0, keepdims=True)
    for p in (p0, p1):
        p[top:, :tokens] = jnp.broadcast_to(marks, (p.shape[0] - top, tokens)).astype(bf16)
    for copy in pieces(p0, 0, 3) + pieces(p1, 1, 3 + count):
        copy.wait()


def fetch_kernel(wg, wu, wd, gain, og, ou, od, ogain, sems):
    copies = [
        pltpu.make_async_copy(src, dst, sems.at[i])
        for i, (src, dst) in enumerate(((wg, og), (wu, ou), (wd, od), (gain, ogain)))
    ]
    for copy in copies:
        copy.start()
    for copy in copies:
        copy.wait()


def units(heads):
    over_z = [(j, h) for j in range(2) for h in range(heads - 1)]
    return over_z, [(j, heads - 1) for j in range(2)]


def attend_kernel(cache, tokens, offset, r0, r1, s0, s1, za, xb0, xb1, xb2, xb3, route, held):
    z, e = lax.axis_index("ctx"), lax.axis_index("exp")
    core = e % 2
    span = cache + tokens
    cap = tokens // 2
    width = r0.shape[1]
    group = HEADS // KV_HEADS
    per_row = width // HEAD_DIM
    top = span + (group // per_row) * tokens
    limit = offset[0:1, 0:1]
    scale = 1.0 / math.sqrt(HEAD_DIM)
    halves = (z % 2, 1 - z % 2)
    keys = [(r, 2 * hi + core) for r, hi in zip((r0, r1), halves)]
    keys += [(s, 2 * hi + 1 - core) for s, hi in zip((s0, s1), halves)]
    rows = group * tokens
    pos = iota((rows, span), 0) % tokens
    col = iota((rows, span), 1)
    for ref, block in keys:
        route[block] = ref[top:, :tokens].astype(f32)
    for r, hi in zip((r0, r1), halves):
        base = (2 * hi + core) * tokens
        q = jnp.concatenate(
            [
                r[span + (g // per_row) * tokens : span + (g // per_row + 1) * tokens,
                  (g % per_row) * HEAD_DIM : (g % per_row + 1) * HEAD_DIM]
                for g in range(group)
            ],
            axis=0,
        )
        scores = []
        for ref, block in keys:
            s = dot_nt(q, ref[0:span, 0:HEAD_DIM]) * scale
            edge = jnp.where(col < cache, limit - block * cache, pos + (base - block * tokens + cache + 1))
            scores.append(jnp.where(col < edge, s, masked_score))
        peak = functools.reduce(jnp.maximum, [jnp.max(s, axis=1, keepdims=True) for s in scores])
        total = jnp.zeros((rows, 1), f32)
        numer = jnp.zeros((rows, HEAD_DIM), f32)
        for (ref, _), s in zip(keys, scores):
            w = jnp.exp(s - peak)
            total += jnp.sum(w, axis=1, keepdims=True)
            numer += dot(w.astype(bf16), ref[0:span, HEAD_DIM:])
        out = (numer / total).astype(bf16)
        held[hi] = jnp.concatenate([out[g * tokens : (g + 1) * tokens] for g in range(group)], axis=1)
    over_z, over_x = units(group)
    for u, (j, h) in enumerate(over_z):
        za[u] = held[j, :, h * HEAD_DIM : (h + 1) * HEAD_DIM]
    for m, xb in enumerate((xb0, xb1, xb2, xb3)):
        for j in range(2):
            pick = expert_rows(route[2 * j + core][0:1], (e ^ m) * cap, cap)
            mine = [(u, h) for u, (i, h) in enumerate(over_x) if i == j]
            lo = mine[0][1] * HEAD_DIM
            got = dot(pick, held[j, :, lo : lo + len(mine) * HEAD_DIM]).astype(bf16)
            for i, (u, _) in enumerate(mine):
                xb[u] = got[:, i * HEAD_DIM : (i + 1) * HEAD_DIM]


def join_kernel(b0, b1, b2, b3, d):
    e = lax.axis_index("exp")
    for m, b in enumerate((b0, b1, b2, b3)):
        d[e ^ m] = b[...]


def regroup_kernel(route, a0, a1, a2, a3, c0, c1, c2, c3):
    e = lax.axis_index("exp")
    core = e % 2
    cap = c0.shape[2]
    over_z, _ = units(HEADS // KV_HEADS)
    for j in range(2):
        marks = route[2 * j + core][0:1]
        pick = jnp.concatenate([expert_rows(marks, (e ^ m) * cap, cap) for m in range(4)], axis=0)
        for u, (i, _) in enumerate(over_z):
            if i == j:
                for n, a in enumerate((a0, a1, a2, a3)):
                    got = dot(pick, a[u]).astype(bf16)
                    for m, c in enumerate((c0, c1, c2, c3)):
                        c[n, u] = got[m * cap : (m + 1) * cap]


def lanes_of(h):
    return slice(h * HEAD_DIM, (h + 1) * HEAD_DIM)


def half_kernel(c0, c1, gain, wg, wu, gate, upper, square, xh):
    z, e = lax.axis_index("ctx"), lax.axis_index("exp")
    slices, blocks, cap, part = xh.shape
    rows = blocks * cap
    over_z, _ = units(HEADS // KV_HEADS)
    wide = gain.shape[1] // KV_HEADS
    for m, c in enumerate((c0, c1)):
        src = e ^ m
        for n in range(slices):
            for u, (j, h) in enumerate(over_z):
                xh[z ^ n, 2 * j + src % 2, :, lanes_of(h)] = c[n, u]
    total, g, u = 0.0, 0.0, 0.0
    for n in range(slices):
        v = xh[n].reshape(rows, part).astype(f32)
        total += jnp.sum(v * v, axis=1, keepdims=True)
        at = pl.ds(pl.multiple_of((slices * (e // 2) + n) * wide, wide), part)
        x = (v * gain[0:1, at]).astype(bf16)
        g += dot_nt(x, wg[:, at])
        u += dot_nt(x, wu[:, at])
    gate[...] = g
    upper[...] = u
    square[...] = jnp.broadcast_to(total, square.shape)


def expert_kernel(
    gate, upper, square, xh, c2, c3, d0, d1, d2, d3, gain, wg, wu, wd,
    y0, y1, y2, y3, t0, t1, t2, t3, xo, xd, nz, sc, ys,
):
    z, e = lax.axis_index("ctx"), lax.axis_index("exp")
    slices, blocks, cap, wide = xo.shape
    rows = blocks * cap
    over_z, over_x = units(HEADS // KV_HEADS)
    mine, other = e // 2, 1 - e // 2
    part = xh.shape[3]
    for m, c in ((2, c2), (3, c3)):
        src = e ^ m
        for n in range(slices):
            for u, (j, h) in enumerate(over_z):
                xo[z ^ n, 2 * j + src % 2, :, lanes_of(h)] = c[n, u]
    for m, d in enumerate((d0, d1, d2, d3)):
        for k in range(2):
            for u, (j, _) in enumerate(over_x):
                xo[z ^ m, 2 * j + k, :, part:] = d[2 * other + k, u]
                xd[z ^ m, 2 * j + k] = d[2 * mine + k, u]
    total, g, u = square[:, 0:1], gate[...], upper[...]
    for x, first, side in ((xo, 0, other), (xd, part, mine)):
        width = x.shape[3]
        for n in range(slices):
            v = x[n].reshape(rows, width).astype(f32)
            total += jnp.sum(v * v, axis=1, keepdims=True)
            at = pl.ds(pl.multiple_of((slices * side + n) * wide + first, HEAD_DIM), width)
            r = (v * gain[0:1, at]).astype(bf16)
            g += dot_nt(r, wg[:, at])
            u += dot_nt(r, wu[:, at])
    scale = lax.rsqrt(total * (1.0 / gain.shape[1]) + 1e-05)
    sc[...] = jnp.broadcast_to(scale, sc.shape)
    g, u = g * scale, u * scale
    hidden = (g / (1.0 + jnp.exp(-g)) * u).astype(bf16)
    own_scale = sc[pl.ds(pl.multiple_of(z * cap, cap), cap), 0:1]
    for n in range(slices):
        for x, first, side in ((xo, 0, other), (xh, 0, mine), (xd, part, mine)):
            width = x.shape[3]
            s = slices * side + n
            at = pl.ds(pl.multiple_of(s * wide + first, HEAD_DIM), width)
            v = x[n, z].astype(f32) * own_scale * gain[0:1, at]
            nz[s, :, first : first + width] = v.astype(bf16)
    owners, _, span = ys.shape
    at_home = iota((rows, span), 0) // cap == z
    for o in range(owners):
        v = dot(hidden, wd[:, o * span : (o + 1) * span])
        per = span // wide
        normed = jnp.concatenate([nz[o * per + i] for i in range(per)], axis=1).astype(f32)
        ys[o] = (v + jnp.where(at_home, jnp.concatenate([normed] * blocks, axis=0), 0.0)).astype(bf16)
    keep = y0.shape[1]
    for m, (y, t) in enumerate(zip((y0, y1, y2, y3), (t0, t1, t2, t3))):
        y[...] = ys[e ^ m, :, 0:keep]
        for o in range(owners):
            t[o] = ys[o, pl.ds(pl.multiple_of((z ^ m) * cap, cap), cap), keep:]


def turn_kernel(route, y0, y1, y2, y3, g0, g1, g2, g3):
    z, e = lax.axis_index("ctx"), lax.axis_index("exp")
    cap = y0.shape[0] // 4
    for m, g in enumerate((g0, g1, g2, g3)):
        block = z ^ m
        marks = route[block][0:1]
        pick = jnp.concatenate([expert_rows(marks, (e ^ n) * cap, cap) for n in range(4)], axis=0)
        at = pl.ds(pl.multiple_of(block * cap, cap), cap)
        got = jnp.concatenate([y[at, :] for y in (y0, y1, y2, y3)], axis=0)
        g[...] = dot_tn(pick, got).astype(bf16)


def total_kernel(t0, t1, t2, t3, h0, h1, h2, h3, ts):
    e = lax.axis_index("exp")
    ts[...] = sum(t[...].astype(f32) for t in (t0, t1, t2, t3)).astype(bf16)
    for m, h in enumerate((h0, h1, h2, h3)):
        h[...] = ts[e ^ m]


def final_kernel(route, g0, g1, g2, g3, h0, h1, h2, h3, out):
    z, e = lax.axis_index("ctx"), lax.axis_index("exp")
    cap = h0.shape[0]
    keep = g0.shape[1]
    out[:, 0:keep] = sum(g[...].astype(f32) for g in (g0, g1, g2, g3)).astype(bf16)
    marks = route[z][0:1]
    pick = jnp.concatenate([expert_rows(marks, (e ^ n) * cap, cap) for n in range(4)], axis=0)
    got = jnp.concatenate([h[...] for h in (h0, h1, h2, h3)], axis=0)
    out[:, keep:] = dot_tn(pick, got).astype(bf16)


def paired_path(*args):
    return paired_steps(*args)


def paired_steps(
    queries,
    new_keys,
    new_values,
    cache_keys,
    cache_values,
    offset,
    token_ids,
    expert_table,
    norm_gain,
    w_gate,
    w_up,
    w_down,
):
    n_ctx, n_exp = lax.axis_size("ctx"), lax.axis_size("exp")
    tokens = queries.shape[0]
    cache = cache_keys.shape[0]
    width = new_keys.shape[1]
    group = HEADS // KV_HEADS
    wide = group * HEAD_DIM
    cap = tokens // 2
    span = cache + tokens
    over_z, over_x = units(group)
    own = queries.shape[1]
    back = own * 3 // 8
    keep = own - back
    rows = n_ctx * cap

    def over_ctx(v, m):
        return lax.ppermute(v, "ctx", [(i, i ^ m) for i in range(n_ctx)])

    def over_exp(v, m):
        return lax.ppermute(v, "exp", [(i, i ^ m) for i in range(n_exp)])

    def head_step(v, o):
        pairs = []
        for z in range(n_ctx):
            for e in range(n_exp):
                core = e % 2
                to_z = 2 * core + ((z // 2) ^ o)
                pairs.append((z * n_exp + e, to_z * n_exp + e - core + z % 2))
        return lax.ppermute(v, ("ctx", "exp"), pairs)

    height = span + tokens * wide // width + 8
    copies = 3 + 2 * (4 + wide // width)
    table_rows = expert_table.reshape(-1, 128)
    p0, p1 = call(
        pack_kernel,
        [((height, width), bf16)] * 2,
        8,
        scratch=[
            pltpu.VMEM((8, tokens), jnp.int32),
            pltpu.SMEM((tokens,), jnp.int32),
            pltpu.VMEM(table_rows.shape, jnp.int32),
            pltpu.VMEM((tokens, table_rows.shape[1]), jnp.int32),
            pltpu.SemaphoreType.DMA((copies,)),
        ],
        hbm=7,
    )(queries, new_keys, new_values, cache_keys, cache_values, token_ids, table_rows)
    limit = jnp.broadcast_to(offset[None, :], (8, 128))
    gate_t, up_t, down = jnp.swapaxes(w_gate[0], 0, 1), jnp.swapaxes(w_up[0], 0, 1), w_down[0]
    weight_bytes = 2 * (gate_t.size + up_t.size + down.size)
    gate_t, up_t, down, gain = call(
        fetch_kernel,
        [(w.shape, bf16) for w in (gate_t, up_t, down)] + [((1, norm_gain.shape[0]), f32)],
        4,
        scratch=[pltpu.SemaphoreType.DMA((4,))],
        hbm=4,
        cost=pl.CostEstimate(flops=1000 * weight_bytes, transcendentals=0, bytes_accessed=2 * weight_bytes),
    )(gate_t, up_t, down, norm_gain.reshape(1, -1))
    r0, r1 = head_step(p0, 0), head_step(p1, 1)
    r0, limit = lax.optimization_barrier((r0, limit))
    s0, s1 = over_exp(r0, 1), over_exp(r1, 1)
    za, xb0, xb1, xb2, xb3, route = call(
        functools.partial(attend_kernel, cache, tokens),
        [((len(over_z), tokens, HEAD_DIM), bf16)]
        + [((len(over_x), cap, HEAD_DIM), bf16)] * 4
        + [((n_ctx, 8, tokens), f32)],
        16,
        scratch=[pltpu.VMEM((2, tokens, wide), bf16)],
    )(limit, r0, r1, s0, s1)
    a = [za] + [over_ctx(za, m) for m in (1, 2, 3)]
    b = [xb0] + [over_exp(v, m) for m, v in ((1, xb1), (2, xb2), (3, xb3))]
    (zd,) = call(join_kernel, [((n_exp, len(over_x), cap, HEAD_DIM), bf16)], 4)(*b)
    d = [zd] + [over_ctx(zd, m) for m in (1, 2, 3)]
    c0, c1, c2, c3 = call(regroup_kernel, [((n_ctx, len(over_z), cap, HEAD_DIM), bf16)] * 4, 8)(route, *a)
    c = [c0] + [over_exp(v, m) for m, v in ((1, c1), (2, c2), (3, c3))]
    units_hidden = gate_t.shape[0]
    part = wide - HEAD_DIM
    gate, upper, square, xh = call(
        half_kernel,
        [((rows, units_hidden), f32)] * 2 + [((rows, 128), f32), ((n_ctx, n_ctx, cap, part), bf16)],
        20,
        cost=pl.CostEstimate(flops=2 * rows * units_hidden * n_ctx * part * 2, transcendentals=0, bytes_accessed=0),
    )(c[0], c[1], gain, gate_t, up_t)
    outs = call(
        expert_kernel,
        [((rows, keep), bf16)] * 4 + [((n_exp, cap, back), bf16)] * 4,
        28,
        scratch=[
            pltpu.VMEM((n_ctx, n_ctx, cap, wide), bf16),
            pltpu.VMEM((n_ctx, n_ctx, cap, HEAD_DIM), bf16),
            pltpu.VMEM((KV_HEADS, cap, wide), bf16),
            pltpu.VMEM((rows, 128), f32),
            pltpu.VMEM((n_exp, rows, own), bf16),
        ],
    )(gate, upper, square, xh, c[2], c[3], *d, gain, gate_t, up_t, down)
    y, t = outs[:4], outs[4:]
    t = [t[0]] + [over_ctx(t[m], m) for m in (1, 2, 3)]
    y = [y[0]] + [over_exp(y[m], m) for m in (1, 2, 3)]
    g = call(turn_kernel, [((tokens, keep), bf16)] * 4, 8)(route, *y)
    g = [g[0]] + [over_ctx(g[m], m) for m in (1, 2, 3)]
    h = call(total_kernel, [((cap, back), bf16)] * 4, 8, scratch=[pltpu.VMEM((n_exp, cap, back), bf16)])(*t)
    h = [h[0]] + [over_exp(h[m], m) for m in (1, 2, 3)]
    (out,) = call(final_kernel, [((tokens, own), bf16)], 8)(route, *g, *h)
    return out


def solution(mesh):
    placed = (
        P(("group", "ctx"), "exp"),
        P(("group", "ctx"), "exp"),
        P(("group", "ctx"), "exp"),
        P(("group", "ctx"), "exp"),
        P(("group", "ctx"), "exp"),
        P("group"),
        P(("group", "ctx")),
        P("group"),
        P(),
        P("exp", None, "ctx"),
        P("exp", None, "ctx"),
        P("exp", "ctx", None),
    )
    n_ctx, n_exp = mesh.shape["ctx"], mesh.shape["exp"]
    paired = n_ctx == n_exp == 4 and KV_HEADS == 2 * n_exp
    return jax.shard_map(
        paired_path if paired else general_path,
        mesh=mesh,
        in_specs=placed,
        out_specs=P(("group", "ctx"), "exp"),
        check_vma=False,
    )
```

```python
import functools
import math

import jax
import jax.numpy as jnp
from jax import lax
from jax.experimental import pallas as pl
from jax.experimental.pallas import tpu as pltpu
from jax.sharding import PartitionSpec as P


HEADS = 32
KV_HEADS = 8
HEAD_DIM = 128


masked_score = -1e30
f32 = jnp.float32
bf16 = jnp.bfloat16


def split_heads(flat, heads):
    return flat.reshape(flat.shape[0], heads, flat.shape[1] // heads)


def partial_attend(query_rows, key_rows, value_rows, allowed):
    width = query_rows.shape[3]
    scores = jnp.einsum("rkgd,skd->rkgs", query_rows, key_rows, preferred_element_type=jnp.float32)
    scores = scores * (1.0 / math.sqrt(width))
    usable = allowed[:, None, None, :]
    peak = jnp.max(jnp.where(usable, scores, masked_score), axis=-1)
    unnorm = jnp.where(usable, jnp.exp(scores - peak[..., None]), 0.0)
    total = jnp.sum(unnorm, axis=-1)
    numer = jnp.einsum(
        "rkgs,skd->rkgd",
        unnorm.astype(jnp.bfloat16),
        value_rows,
        preferred_element_type=jnp.float32,
    )
    return (numer, peak, total)


def general_path(
    queries,
    new_keys,
    new_values,
    cache_keys,
    cache_values,
    offset,
    token_ids,
    expert_table,
    norm_gain,
    w_gate,
    w_up,
    w_down,
):
    owners = lax.axis_size("exp")
    heads_local = HEADS // owners
    kv_local = KV_HEADS // owners
    group = HEADS // KV_HEADS
    tok_count = queries.shape[0]
    cache_len = cache_keys.shape[0]
    shard = lax.axis_index("ctx")
    limit = offset[0]
    key_rows = jnp.concatenate([cache_keys, new_keys], axis=0)
    value_rows = jnp.concatenate([cache_values, new_values], axis=0)
    span = key_rows.shape[0]
    own_index = shard * tok_count + jnp.arange(tok_count, dtype=jnp.int32)
    grouped = queries.reshape(tok_count, kv_local, group, HEAD_DIM)
    piece_keys = lax.all_gather(key_rows, "ctx", axis=0, tiled=True)
    piece_values = lax.all_gather(value_rows, "ctx", axis=0, tiled=True)
    flat = jnp.arange(piece_keys.shape[0], dtype=jnp.int32)
    source = flat // span
    inner = flat % span
    cache_ok = source * cache_len + inner < limit
    stretch_ok = (source * tok_count + inner - cache_len)[None, :] <= own_index[:, None]
    allowed = jnp.where((inner < cache_len)[None, :], cache_ok[None, :], stretch_ok)
    numer, _, total = partial_attend(
        grouped, split_heads(piece_keys, kv_local), split_heads(piece_values, kv_local), allowed
    )
    attended = (numer / total[..., None]).reshape(tok_count, heads_local * HEAD_DIM).astype(jnp.bfloat16)
    capacity = tok_count // 2
    chosen = expert_table[token_ids]
    onehot = (chosen[:, None] == jnp.arange(owners, dtype=jnp.int32)[None, :]).astype(jnp.int32)
    earlier = jnp.cumsum(onehot, axis=0) - onehot
    slot = jnp.sum(earlier * onehot, axis=1)
    target = chosen * capacity + slot
    dispatch = (jnp.arange(owners * capacity, dtype=jnp.int32)[:, None] == target[None, :]).astype(
        jnp.bfloat16
    )
    packed = jnp.dot(dispatch, attended, preferred_element_type=jnp.float32).astype(jnp.bfloat16)
    arrived = lax.all_to_all(packed, "exp", split_axis=0, concat_axis=1, tiled=True)
    values32 = arrived.astype(jnp.float32)
    scale = lax.rsqrt(jnp.mean(values32 * values32, axis=-1, keepdims=True) + 1e-05)
    normed = (values32 * scale * norm_gain).astype(jnp.bfloat16)
    piece = lax.all_gather(normed, "ctx", axis=0, tiled=True)
    gate = jnp.dot(piece, w_gate[0], preferred_element_type=jnp.float32)
    upper = jnp.dot(piece, w_up[0], preferred_element_type=jnp.float32)
    hidden = (jax.nn.silu(gate) * upper).astype(jnp.bfloat16)
    summed = lax.psum_scatter(
        jnp.dot(hidden, w_down[0], preferred_element_type=jnp.float32).astype(jnp.bfloat16),
        "ctx",
        scatter_dimension=0,
        tiled=True,
    ).astype(jnp.float32)
    combined = (normed.astype(jnp.float32) + summed).astype(jnp.bfloat16)
    returned = lax.all_to_all(combined, "exp", split_axis=1, concat_axis=0, tiled=True)
    collect = (target[:, None] == jnp.arange(owners * capacity, dtype=jnp.int32)[None, :]).astype(
        jnp.bfloat16
    )
    return jnp.dot(collect, returned, preferred_element_type=jnp.float32).astype(jnp.bfloat16)


def iota(shape, axis):
    return lax.broadcasted_iota(jnp.int32, shape, axis)


def call(kernel, out_shapes, mib, scratch=(), hbm=0, cost=None):
    def run(*args):
        args = [pltpu.with_memory_space_constraint(v, pltpu.HBM) if i < hbm else v for i, v in enumerate(args)]
        vmem = pl.BlockSpec(memory_space=pltpu.VMEM)
        specs = [pl.BlockSpec(memory_space=pltpu.HBM)] * hbm + [vmem] * (len(args) - hbm)
        return pl.pallas_call(
            kernel,
            out_shape=[jax.ShapeDtypeStruct(s, d) for s, d in out_shapes],
            in_specs=specs,
            out_specs=[vmem] * len(out_shapes),
            scratch_shapes=list(scratch),
            compiler_params=pltpu.CompilerParams(vmem_limit_bytes=mib << 20),
            cost_estimate=cost,
        )(*args)

    return run


def expert_rows(marks, first, cap):
    tokens = marks.shape[1]
    slots = (iota((cap, tokens), 0) + first).astype(f32)
    return (marks == slots).astype(bf16)


def dot(a, b):
    return jnp.dot(a, b, preferred_element_type=f32)


def dot_nt(a, b):
    return lax.dot_general(a, b, (((1,), (1,)), ((), ())), preferred_element_type=f32)


def dot_tn(a, b):
    return lax.dot_general(a, b, (((0,), (0,)), ((), ())), preferred_element_type=f32)


def pack_kernel(q, nk, nv, ck, cv, ids, table, p0, p1, id_row, id_smem, rows, found, sems):
    z = lax.axis_index("ctx")
    tokens, cache = q.shape[0], ck.shape[0]
    span = cache + tokens
    width = p0.shape[1]
    wide = q.shape[1] // 2
    cap = tokens // 2
    top = span + (wide // width) * tokens
    lanes = found.shape[1]
    swap = (z // 2) == 1

    first = [
        pltpu.make_async_copy(ids, id_smem, sems.at[0]),
        pltpu.make_async_copy(ids, id_row.at[0], sems.at[1]),
        pltpu.make_async_copy(table, rows, sems.at[2]),
    ]
    for copy in first:
        copy.start()

    def pieces(p, h, base):
        at = pl.ds(h * HEAD_DIM, HEAD_DIM)
        moves = [
            (ck.at[:, at], p.at[0:cache, 0:HEAD_DIM]),
            (cv.at[:, at], p.at[0:cache, HEAD_DIM:]),
            (nk.at[:, at], p.at[cache:span, 0:HEAD_DIM]),
            (nv.at[:, at], p.at[cache:span, HEAD_DIM:]),
        ]
        for part in range(wide // width):
            lo = h * wide + part * width
            moves.append((q.at[:, pl.ds(lo, width)], p.at[span + part * tokens : span + (part + 1) * tokens, :]))
        return [pltpu.make_async_copy(src, dst, sems.at[base + i]) for i, (src, dst) in enumerate(moves)]

    count = 4 + wide // width

    @pl.when(jnp.logical_not(swap))
    def _():
        for copy in pieces(p0, 0, 3) + pieces(p1, 1, 3 + count):
            copy.start()

    @pl.when(swap)
    def _():
        for copy in pieces(p0, 1, 3) + pieces(p1, 0, 3 + count):
            copy.start()

    for copy in first:
        copy.wait()
    for t in range(tokens):
        found[t : t + 1, :] = rows[pl.ds(id_smem[t] // lanes, 1), :]
    same = iota((tokens, tokens), 0) == iota((tokens, tokens), 1)
    id_col = jnp.sum(jnp.where(same, (id_row[0:1, :] % lanes).astype(f32), 0.0), axis=1, keepdims=True)
    hit = iota((tokens, lanes), 1).astype(f32) == id_col
    who = jnp.sum(jnp.where(hit, found[...].astype(f32), 0.0), axis=1, keepdims=True)
    expert = iota((tokens, 128), 1).astype(f32)
    onehot = (who == expert).astype(f32)
    before = (iota((tokens, tokens), 1) < iota((tokens, tokens), 0)).astype(bf16)
    rank = dot(before, onehot.astype(bf16))
    target = jnp.sum(onehot * (expert * cap + rank), axis=1, keepdims=True)
    marks = jnp.sum(jnp.where(same, target, 0.0), axis=0, keepdims=True)
    for p in (p0, p1):
        p[top:, :tokens] = jnp.broadcast_to(marks, (p.shape[0] - top, tokens)).astype(bf16)
    for copy in pieces(p0, 0, 3) + pieces(p1, 1, 3 + count):
        copy.wait()


def fetch_kernel(wg, wu, wd, gain, og, ou, od, ogain, sems):
    copies = [
        pltpu.make_async_copy(src, dst, sems.at[i])
        for i, (src, dst) in enumerate(((wg, og), (wu, ou), (wd, od), (gain, ogain)))
    ]
    for copy in copies:
        copy.start()
    for copy in copies:
        copy.wait()


def units(heads):
    over_z = [(j, h) for j in range(2) for h in range(heads - 1)]
    return over_z, [(j, heads - 1) for j in range(2)]


def attend_kernel(cache, tokens, offset, r0, r1, s0, s1, za, xb0, xb1, xb2, xb3, route, held):
    z, e = lax.axis_index("ctx"), lax.axis_index("exp")
    core = e % 2
    span = cache + tokens
    cap = tokens // 2
    width = r0.shape[1]
    group = HEADS // KV_HEADS
    per_row = width // HEAD_DIM
    top = span + (group // per_row) * tokens
    limit = offset[0:1, 0:1]
    scale = 1.0 / math.sqrt(HEAD_DIM)
    halves = (z % 2, 1 - z % 2)
    keys = [(r, 2 * hi + core) for r, hi in zip((r0, r1), halves)]
    keys += [(s, 2 * hi + 1 - core) for s, hi in zip((s0, s1), halves)]
    rows = group * tokens
    pos = iota((rows, span), 0) % tokens
    col = iota((rows, span), 1)
    for ref, block in keys:
        route[block] = ref[top:, :tokens].astype(f32)
    for r, hi in zip((r0, r1), halves):
        base = (2 * hi + core) * tokens
        q = jnp.concatenate(
            [
                r[span + (g // per_row) * tokens : span + (g // per_row + 1) * tokens,
                  (g % per_row) * HEAD_DIM : (g % per_row + 1) * HEAD_DIM]
                for g in range(group)
            ],
            axis=0,
        )
        scores = []
        for ref, block in keys:
            s = dot_nt(q, ref[0:span, 0:HEAD_DIM]) * scale
            edge = jnp.where(col < cache, limit - block * cache, pos + (base - block * tokens + cache + 1))
            scores.append(jnp.where(col < edge, s, masked_score))
        peak = functools.reduce(jnp.maximum, [jnp.max(s, axis=1, keepdims=True) for s in scores])
        total = jnp.zeros((rows, 1), f32)
        numer = jnp.zeros((rows, HEAD_DIM), f32)
        for (ref, _), s in zip(keys, scores):
            w = jnp.exp(s - peak)
            total += jnp.sum(w, axis=1, keepdims=True)
            numer += dot(w.astype(bf16), ref[0:span, HEAD_DIM:])
        out = (numer / total).astype(bf16)
        held[hi] = jnp.concatenate([out[g * tokens : (g + 1) * tokens] for g in range(group)], axis=1)
    over_z, over_x = units(group)
    for u, (j, h) in enumerate(over_z):
        za[u] = held[j, :, h * HEAD_DIM : (h + 1) * HEAD_DIM]
    for m, xb in enumerate((xb0, xb1, xb2, xb3)):
        for j in range(2):
            pick = expert_rows(route[2 * j + core][0:1], (e ^ m) * cap, cap)
            mine = [(u, h) for u, (i, h) in enumerate(over_x) if i == j]
            lo = mine[0][1] * HEAD_DIM
            got = dot(pick, held[j, :, lo : lo + len(mine) * HEAD_DIM]).astype(bf16)
            for i, (u, _) in enumerate(mine):
                xb[u] = got[:, i * HEAD_DIM : (i + 1) * HEAD_DIM]


def join_kernel(b0, b1, b2, b3, d):
    e = lax.axis_index("exp")
    for m, b in enumerate((b0, b1, b2, b3)):
        d[e ^ m] = b[...]


def regroup_kernel(route, a0, a1, a2, a3, c0, c1, c2, c3):
    e = lax.axis_index("exp")
    core = e % 2
    cap = c0.shape[2]
    over_z, _ = units(HEADS // KV_HEADS)
    for j in range(2):
        marks = route[2 * j + core][0:1]
        pick = jnp.concatenate([expert_rows(marks, (e ^ m) * cap, cap) for m in range(4)], axis=0)
        for u, (i, _) in enumerate(over_z):
            if i == j:
                for n, a in enumerate((a0, a1, a2, a3)):
                    got = dot(pick, a[u]).astype(bf16)
                    for m, c in enumerate((c0, c1, c2, c3)):
                        c[n, u] = got[m * cap : (m + 1) * cap]


def lanes_of(h):
    return slice(h * HEAD_DIM, (h + 1) * HEAD_DIM)


def half_kernel(c0, c1, gain, wg, wu, gate, upper, square, xh):
    z, e = lax.axis_index("ctx"), lax.axis_index("exp")
    slices, blocks, cap, part = xh.shape
    rows = blocks * cap
    over_z, _ = units(HEADS // KV_HEADS)
    wide = gain.shape[1] // KV_HEADS
    for m, c in enumerate((c0, c1)):
        src = e ^ m
        for n in range(slices):
            for u, (j, h) in enumerate(over_z):
                xh[z ^ n, 2 * j + src % 2, :, lanes_of(h)] = c[n, u]
    total, g, u = 0.0, 0.0, 0.0
    for n in range(slices):
        v = xh[n].reshape(rows, part).astype(f32)
        total += jnp.sum(v * v, axis=1, keepdims=True)
        at = pl.ds(pl.multiple_of((slices * (e // 2) + n) * wide, wide), part)
        x = (v * gain[0:1, at]).astype(bf16)
        g += dot_nt(x, wg[:, at])
        u += dot_nt(x, wu[:, at])
    gate[...] = g
    upper[...] = u
    square[...] = jnp.broadcast_to(total, square.shape)


def expert_kernel(
    gate, upper, square, xh, c2, c3, d0, d1, d2, d3, gain, wg, wu, wd,
    y0, y1, y2, y3, t0, t1, t2, t3, xo, xd, nz, sc, ys,
):
    z, e = lax.axis_index("ctx"), lax.axis_index("exp")
    slices, blocks, cap, wide = xo.shape
    rows = blocks * cap
    over_z, over_x = units(HEADS // KV_HEADS)
    mine, other = e // 2, 1 - e // 2
    part = xh.shape[3]
    for m, c in ((2, c2), (3, c3)):
        src = e ^ m
        for n in range(slices):
            for u, (j, h) in enumerate(over_z):
                xo[z ^ n, 2 * j + src % 2, :, lanes_of(h)] = c[n, u]
    for m, d in enumerate((d0, d1, d2, d3)):
        for k in range(2):
            for u, (j, _) in enumerate(over_x):
                xo[z ^ m, 2 * j + k, :, part:] = d[2 * other + k, u]
                xd[z ^ m, 2 * j + k] = d[2 * mine + k, u]
    total, g, u = square[:, 0:1], gate[...], upper[...]
    for x, first, side in ((xo, 0, other), (xd, part, mine)):
        width = x.shape[3]
        for n in range(slices):
            v = x[n].reshape(rows, width).astype(f32)
            total += jnp.sum(v * v, axis=1, keepdims=True)
            at = pl.ds(pl.multiple_of((slices * side + n) * wide + first, HEAD_DIM), width)
            r = (v * gain[0:1, at]).astype(bf16)
            g += dot_nt(r, wg[:, at])
            u += dot_nt(r, wu[:, at])
    scale = lax.rsqrt(total * (1.0 / gain.shape[1]) + 1e-05)
    sc[...] = jnp.broadcast_to(scale, sc.shape)
    g, u = g * scale, u * scale
    hidden = (g / (1.0 + jnp.exp(-g)) * u).astype(bf16)
    own_scale = sc[pl.ds(pl.multiple_of(z * cap, cap), cap), 0:1]
    for n in range(slices):
        for x, first, side in ((xo, 0, other), (xh, 0, mine), (xd, part, mine)):
            width = x.shape[3]
            s = slices * side + n
            at = pl.ds(pl.multiple_of(s * wide + first, HEAD_DIM), width)
            v = x[n, z].astype(f32) * own_scale * gain[0:1, at]
            nz[s, :, first : first + width] = v.astype(bf16)
    span, keep = ys.shape[1] + y0.shape[1], y0.shape[1]
    per = span // wide
    at_home = iota((rows, span), 0) // cap == z
    for m, y in enumerate((y0, y1, y2, y3)):
        o = e ^ m
        v = dot(hidden, wd[:, pl.ds(pl.multiple_of(o * span, span), span)])
        normed = jnp.concatenate([nz[o * per + i] for i in range(per)], axis=1).astype(f32)
        v = (v + jnp.where(at_home, jnp.concatenate([normed] * blocks, axis=0), 0.0)).astype(bf16)
        y[...] = v[:, :keep]
        ys[...] = v[:, keep:]
        for i, t in enumerate((t0, t1, t2, t3)):
            t[o] = ys[pl.ds(pl.multiple_of((z ^ i) * cap, cap), cap), :]


def turn_kernel(route, y0, y1, y2, y3, g0, g1, g2, g3):
    z, e = lax.axis_index("ctx"), lax.axis_index("exp")
    cap = y0.shape[0] // 4
    for m, g in enumerate((g0, g1, g2, g3)):
        block = z ^ m
        marks = route[block][0:1]
        pick = jnp.concatenate([expert_rows(marks, (e ^ n) * cap, cap) for n in range(4)], axis=0)
        at = pl.ds(pl.multiple_of(block * cap, cap), cap)
        got = jnp.concatenate([y[at, :] for y in (y0, y1, y2, y3)], axis=0)
        g[...] = dot_tn(pick, got).astype(bf16)


def total_kernel(t0, t1, t2, t3, h0, h1, h2, h3, ts):
    e = lax.axis_index("exp")
    ts[...] = sum(t[...].astype(f32) for t in (t0, t1, t2, t3)).astype(bf16)
    for m, h in enumerate((h0, h1, h2, h3)):
        h[...] = ts[e ^ m]


def final_kernel(route, g0, g1, g2, g3, h0, h1, h2, h3, out):
    z, e = lax.axis_index("ctx"), lax.axis_index("exp")
    cap = h0.shape[0]
    keep = g0.shape[1]
    out[:, 0:keep] = sum(g[...].astype(f32) for g in (g0, g1, g2, g3)).astype(bf16)
    marks = route[z][0:1]
    pick = jnp.concatenate([expert_rows(marks, (e ^ n) * cap, cap) for n in range(4)], axis=0)
    got = jnp.concatenate([h[...] for h in (h0, h1, h2, h3)], axis=0)
    out[:, keep:] = dot_tn(pick, got).astype(bf16)


def paired_path(*args):
    return paired_steps(*args)


def paired_steps(
    queries,
    new_keys,
    new_values,
    cache_keys,
    cache_values,
    offset,
    token_ids,
    expert_table,
    norm_gain,
    w_gate,
    w_up,
    w_down,
):
    n_ctx, n_exp = lax.axis_size("ctx"), lax.axis_size("exp")
    tokens = queries.shape[0]
    cache = cache_keys.shape[0]
    width = new_keys.shape[1]
    group = HEADS // KV_HEADS
    wide = group * HEAD_DIM
    cap = tokens // 2
    span = cache + tokens
    over_z, over_x = units(group)
    own = queries.shape[1]
    back = own * 3 // 8
    keep = own - back
    rows = n_ctx * cap

    def over_ctx(v, m):
        return lax.ppermute(v, "ctx", [(i, i ^ m) for i in range(n_ctx)])

    def over_exp(v, m):
        return lax.ppermute(v, "exp", [(i, i ^ m) for i in range(n_exp)])

    def head_step(v, o):
        pairs = []
        for z in range(n_ctx):
            for e in range(n_exp):
                core = e % 2
                to_z = 2 * core + ((z // 2) ^ o)
                pairs.append((z * n_exp + e, to_z * n_exp + e - core + z % 2))
        return lax.ppermute(v, ("ctx", "exp"), pairs)

    height = span + tokens * wide // width + 8
    copies = 3 + 2 * (4 + wide // width)
    table_rows = expert_table.reshape(-1, 128)
    p0, p1 = call(
        pack_kernel,
        [((height, width), bf16)] * 2,
        8,
        scratch=[
            pltpu.VMEM((8, tokens), jnp.int32),
            pltpu.SMEM((tokens,), jnp.int32),
            pltpu.VMEM(table_rows.shape, jnp.int32),
            pltpu.VMEM((tokens, table_rows.shape[1]), jnp.int32),
            pltpu.SemaphoreType.DMA((copies,)),
        ],
        hbm=7,
    )(queries, new_keys, new_values, cache_keys, cache_values, token_ids, table_rows)
    limit = jnp.broadcast_to(offset[None, :], (8, 128))
    gate_t, up_t, down = jnp.swapaxes(w_gate[0], 0, 1), jnp.swapaxes(w_up[0], 0, 1), w_down[0]
    weight_bytes = 2 * (gate_t.size + up_t.size + down.size)
    gate_t, up_t, down, gain = call(
        fetch_kernel,
        [(w.shape, bf16) for w in (gate_t, up_t, down)] + [((1, norm_gain.shape[0]), f32)],
        4,
        scratch=[pltpu.SemaphoreType.DMA((4,))],
        hbm=4,
        cost=pl.CostEstimate(flops=1000 * weight_bytes, transcendentals=0, bytes_accessed=2 * weight_bytes),
    )(gate_t, up_t, down, norm_gain.reshape(1, -1))
    r0, r1 = head_step(p0, 0), head_step(p1, 1)
    r1, limit = lax.optimization_barrier((r1, limit))
    s0, s1 = over_exp(r0, 1), over_exp(r1, 1)
    za, xb0, xb1, xb2, xb3, route = call(
        functools.partial(attend_kernel, cache, tokens),
        [((len(over_z), tokens, HEAD_DIM), bf16)]
        + [((len(over_x), cap, HEAD_DIM), bf16)] * 4
        + [((n_ctx, 8, tokens), f32)],
        16,
        scratch=[pltpu.VMEM((2, tokens, wide), bf16)],
    )(limit, r0, r1, s0, s1)
    a = [za] + [over_ctx(za, m) for m in (1, 2, 3)]
    b = [xb0] + [over_exp(v, m) for m, v in ((1, xb1), (2, xb2), (3, xb3))]
    (zd,) = call(join_kernel, [((n_exp, len(over_x), cap, HEAD_DIM), bf16)], 4)(*b)
    d = [zd] + [over_ctx(zd, m) for m in (1, 2, 3)]
    c0, c1, c2, c3 = call(regroup_kernel, [((n_ctx, len(over_z), cap, HEAD_DIM), bf16)] * 4, 8)(route, *a)
    c = [c0] + [over_exp(v, m) for m, v in ((1, c1), (2, c2), (3, c3))]
    units_hidden = gate_t.shape[0]
    part = wide - HEAD_DIM
    gate, upper, square, xh = call(
        half_kernel,
        [((rows, units_hidden), f32)] * 2 + [((rows, 128), f32), ((n_ctx, n_ctx, cap, part), bf16)],
        20,
        cost=pl.CostEstimate(flops=2 * rows * units_hidden * n_ctx * part * 2, transcendentals=0, bytes_accessed=0),
    )(c[0], c[1], gain, gate_t, up_t)
    outs = call(
        expert_kernel,
        [((rows, keep), bf16)] * 4 + [((n_exp, cap, back), bf16)] * 4,
        28,
        scratch=[
            pltpu.VMEM((n_ctx, n_ctx, cap, wide), bf16),
            pltpu.VMEM((n_ctx, n_ctx, cap, HEAD_DIM), bf16),
            pltpu.VMEM((KV_HEADS, cap, wide), bf16),
            pltpu.VMEM((rows, 128), f32),
            pltpu.VMEM((rows, back), bf16),
        ],
    )(gate, upper, square, xh, c[2], c[3], *d, gain, gate_t, up_t, down)
    y, t = outs[:4], outs[4:]
    t = [t[0]] + [over_ctx(t[m], m) for m in (1, 2, 3)]
    y = [y[0]] + [over_exp(y[m], m) for m in (1, 2, 3)]
    g = call(turn_kernel, [((tokens, keep), bf16)] * 4, 8)(route, *y)
    g = [g[0]] + [over_ctx(g[m], m) for m in (1, 2, 3)]
    h = call(total_kernel, [((cap, back), bf16)] * 4, 8, scratch=[pltpu.VMEM((n_exp, cap, back), bf16)])(*t)
    h = [h[0]] + [over_exp(h[m], m) for m in (1, 2, 3)]
    (out,) = call(final_kernel, [((tokens, own), bf16)], 8)(route, *g, *h)
    return out


def solution(mesh):
    placed = (
        P(("group", "ctx"), "exp"),
        P(("group", "ctx"), "exp"),
        P(("group", "ctx"), "exp"),
        P(("group", "ctx"), "exp"),
        P(("group", "ctx"), "exp"),
        P("group"),
        P(("group", "ctx")),
        P("group"),
        P(),
        P("exp", None, "ctx"),
        P("exp", None, "ctx"),
        P("exp", "ctx", None),
    )
    n_ctx, n_exp = mesh.shape["ctx"], mesh.shape["exp"]
    paired = n_ctx == n_exp == 4 and KV_HEADS == 2 * n_exp
    return jax.shard_map(
        paired_path if paired else general_path,
        mesh=mesh,
        in_specs=placed,
        out_specs=P(("group", "ctx"), "exp"),
        check_vma=False,
    )
```

```python
import functools
import math

import jax
import jax.numpy as jnp
from jax import lax
from jax.experimental import pallas as pl
from jax.experimental.pallas import tpu as pltpu
from jax.sharding import PartitionSpec as P


HEADS = 32
KV_HEADS = 8
HEAD_DIM = 128


masked_score = -1e30
f32 = jnp.float32
bf16 = jnp.bfloat16


def split_heads(flat, heads):
    return flat.reshape(flat.shape[0], heads, flat.shape[1] // heads)


def partial_attend(query_rows, key_rows, value_rows, allowed):
    width = query_rows.shape[3]
    scores = jnp.einsum("rkgd,skd->rkgs", query_rows, key_rows, preferred_element_type=jnp.float32)
    scores = scores * (1.0 / math.sqrt(width))
    usable = allowed[:, None, None, :]
    peak = jnp.max(jnp.where(usable, scores, masked_score), axis=-1)
    unnorm = jnp.where(usable, jnp.exp(scores - peak[..., None]), 0.0)
    total = jnp.sum(unnorm, axis=-1)
    numer = jnp.einsum(
        "rkgs,skd->rkgd",
        unnorm.astype(jnp.bfloat16),
        value_rows,
        preferred_element_type=jnp.float32,
    )
    return (numer, peak, total)


def general_path(
    queries,
    new_keys,
    new_values,
    cache_keys,
    cache_values,
    offset,
    token_ids,
    expert_table,
    norm_gain,
    w_gate,
    w_up,
    w_down,
):
    owners = lax.axis_size("exp")
    heads_local = HEADS // owners
    kv_local = KV_HEADS // owners
    group = HEADS // KV_HEADS
    tok_count = queries.shape[0]
    cache_len = cache_keys.shape[0]
    shard = lax.axis_index("ctx")
    limit = offset[0]
    key_rows = jnp.concatenate([cache_keys, new_keys], axis=0)
    value_rows = jnp.concatenate([cache_values, new_values], axis=0)
    span = key_rows.shape[0]
    own_index = shard * tok_count + jnp.arange(tok_count, dtype=jnp.int32)
    grouped = queries.reshape(tok_count, kv_local, group, HEAD_DIM)
    piece_keys = lax.all_gather(key_rows, "ctx", axis=0, tiled=True)
    piece_values = lax.all_gather(value_rows, "ctx", axis=0, tiled=True)
    flat = jnp.arange(piece_keys.shape[0], dtype=jnp.int32)
    source = flat // span
    inner = flat % span
    cache_ok = source * cache_len + inner < limit
    stretch_ok = (source * tok_count + inner - cache_len)[None, :] <= own_index[:, None]
    allowed = jnp.where((inner < cache_len)[None, :], cache_ok[None, :], stretch_ok)
    numer, _, total = partial_attend(
        grouped, split_heads(piece_keys, kv_local), split_heads(piece_values, kv_local), allowed
    )
    attended = (numer / total[..., None]).reshape(tok_count, heads_local * HEAD_DIM).astype(jnp.bfloat16)
    capacity = tok_count // 2
    chosen = expert_table[token_ids]
    onehot = (chosen[:, None] == jnp.arange(owners, dtype=jnp.int32)[None, :]).astype(jnp.int32)
    earlier = jnp.cumsum(onehot, axis=0) - onehot
    slot = jnp.sum(earlier * onehot, axis=1)
    target = chosen * capacity + slot
    dispatch = (jnp.arange(owners * capacity, dtype=jnp.int32)[:, None] == target[None, :]).astype(
        jnp.bfloat16
    )
    packed = jnp.dot(dispatch, attended, preferred_element_type=jnp.float32).astype(jnp.bfloat16)
    arrived = lax.all_to_all(packed, "exp", split_axis=0, concat_axis=1, tiled=True)
    values32 = arrived.astype(jnp.float32)
    scale = lax.rsqrt(jnp.mean(values32 * values32, axis=-1, keepdims=True) + 1e-05)
    normed = (values32 * scale * norm_gain).astype(jnp.bfloat16)
    piece = lax.all_gather(normed, "ctx", axis=0, tiled=True)
    gate = jnp.dot(piece, w_gate[0], preferred_element_type=jnp.float32)
    upper = jnp.dot(piece, w_up[0], preferred_element_type=jnp.float32)
    hidden = (jax.nn.silu(gate) * upper).astype(jnp.bfloat16)
    summed = lax.psum_scatter(
        jnp.dot(hidden, w_down[0], preferred_element_type=jnp.float32).astype(jnp.bfloat16),
        "ctx",
        scatter_dimension=0,
        tiled=True,
    ).astype(jnp.float32)
    combined = (normed.astype(jnp.float32) + summed).astype(jnp.bfloat16)
    returned = lax.all_to_all(combined, "exp", split_axis=1, concat_axis=0, tiled=True)
    collect = (target[:, None] == jnp.arange(owners * capacity, dtype=jnp.int32)[None, :]).astype(
        jnp.bfloat16
    )
    return jnp.dot(collect, returned, preferred_element_type=jnp.float32).astype(jnp.bfloat16)


def iota(shape, axis):
    return lax.broadcasted_iota(jnp.int32, shape, axis)


def call(kernel, out_shapes, mib, scratch=(), hbm=0, cost=None):
    def run(*args):
        args = [pltpu.with_memory_space_constraint(v, pltpu.HBM) if i < hbm else v for i, v in enumerate(args)]
        vmem = pl.BlockSpec(memory_space=pltpu.VMEM)
        specs = [pl.BlockSpec(memory_space=pltpu.HBM)] * hbm + [vmem] * (len(args) - hbm)
        return pl.pallas_call(
            kernel,
            out_shape=[jax.ShapeDtypeStruct(s, d) for s, d in out_shapes],
            in_specs=specs,
            out_specs=[vmem] * len(out_shapes),
            scratch_shapes=list(scratch),
            compiler_params=pltpu.CompilerParams(vmem_limit_bytes=mib << 20),
            cost_estimate=cost,
        )(*args)

    return run


def expert_rows(marks, first, cap):
    tokens = marks.shape[1]
    slots = (iota((cap, tokens), 0) + first).astype(f32)
    return (marks == slots).astype(bf16)


def dot(a, b):
    return jnp.dot(a, b, preferred_element_type=f32)


def dot_nt(a, b):
    return lax.dot_general(a, b, (((1,), (1,)), ((), ())), preferred_element_type=f32)


def dot_tn(a, b):
    return lax.dot_general(a, b, (((0,), (0,)), ((), ())), preferred_element_type=f32)


def pack_kernel(q, nk, nv, ck, cv, ids, table, p0, p1, id_smem, rows, found, sems):
    z = lax.axis_index("ctx")
    tokens, cache = q.shape[0], ck.shape[0]
    span = cache + tokens
    width = p0.shape[1]
    wide = q.shape[1] // 2
    cap = tokens // 2
    top = span + (wide // width) * tokens
    lanes = found.shape[1]
    swap = (z // 2) == 1

    first = [
        pltpu.make_async_copy(ids, id_smem, sems.at[0]),
        pltpu.make_async_copy(table, rows, sems.at[1]),
    ]
    for copy in first:
        copy.start()

    def pieces(p, h, base):
        at = pl.ds(h * HEAD_DIM, HEAD_DIM)
        moves = [
            (ck.at[:, at], p.at[0:cache, 0:HEAD_DIM]),
            (cv.at[:, at], p.at[0:cache, HEAD_DIM:]),
            (nk.at[:, at], p.at[cache:span, 0:HEAD_DIM]),
            (nv.at[:, at], p.at[cache:span, HEAD_DIM:]),
        ]
        for part in range(wide // width):
            lo = h * wide + part * width
            moves.append((q.at[:, pl.ds(lo, width)], p.at[span + part * tokens : span + (part + 1) * tokens, :]))
        return [pltpu.make_async_copy(src, dst, sems.at[base + i]) for i, (src, dst) in enumerate(moves)]

    count = 4 + wide // width

    @pl.when(jnp.logical_not(swap))
    def _():
        for copy in pieces(p0, 0, 2) + pieces(p1, 1, 2 + count):
            copy.start()

    @pl.when(swap)
    def _():
        for copy in pieces(p0, 1, 2) + pieces(p1, 0, 2 + count):
            copy.start()

    for copy in first:
        copy.wait()
    lane = iota((1, lanes), 1)
    for t in range(tokens):
        at = id_smem[t]
        row = rows[pl.ds(lax.shift_right_logical(at, lanes.bit_length() - 1), 1), :]
        found[t : t + 1, :] = jnp.where(lane == (at & (lanes - 1)), row, 0)
    here, there = iota((tokens, tokens), 0), iota((tokens, tokens), 1)
    who = jnp.sum(found[...].astype(f32), axis=1, keepdims=True)
    who_row = jnp.sum(jnp.where(here == there, who, 0.0), axis=0, keepdims=True)
    ahead = jnp.where((who == who_row) & (here < there), 1.0, 0.0)
    marks = who_row * cap + jnp.sum(ahead, axis=0, keepdims=True)
    for p in (p0, p1):
        p[top:, :tokens] = jnp.broadcast_to(marks, (p.shape[0] - top, tokens)).astype(bf16)
    for copy in pieces(p0, 0, 2) + pieces(p1, 1, 2 + count):
        copy.wait()


def fetch_kernel(wg, wu, wd, gain, og, ou, od, ogain, sems):
    copies = [
        pltpu.make_async_copy(src, dst, sems.at[i])
        for i, (src, dst) in enumerate(((wg, og), (wu, ou), (wd, od), (gain, ogain)))
    ]
    for copy in copies:
        copy.start()
    for copy in copies:
        copy.wait()


def units(heads):
    over_z = [(j, h) for j in range(2) for h in range(heads - 1)]
    return over_z, [(j, heads - 1) for j in range(2)]


def attend_kernel(cache, tokens, offset, r0, r1, s0, s1, za, xb0, xb1, xb2, xb3, route, held):
    z, e = lax.axis_index("ctx"), lax.axis_index("exp")
    core = e % 2
    span = cache + tokens
    cap = tokens // 2
    width = r0.shape[1]
    group = HEADS // KV_HEADS
    per_row = width // HEAD_DIM
    top = span + (group // per_row) * tokens
    limit = offset[0:1, 0:1]
    scale = math.log2(math.e) / math.sqrt(HEAD_DIM)
    halves = (z % 2, 1 - z % 2)
    keys = [(r, 2 * hi + core) for r, hi in zip((r0, r1), halves)]
    keys += [(s, 2 * hi + 1 - core) for s, hi in zip((s0, s1), halves)]
    rows = group * tokens
    pos = iota((rows, span), 0) % tokens
    col = iota((rows, span), 1)
    for ref, block in keys:
        route[block] = ref[top:, :tokens].astype(f32)
    for r, hi in zip((r0, r1), halves):
        base = (2 * hi + core) * tokens
        q = jnp.concatenate(
            [
                r[span + (g // per_row) * tokens : span + (g // per_row + 1) * tokens,
                  (g % per_row) * HEAD_DIM : (g % per_row + 1) * HEAD_DIM]
                for g in range(group)
            ],
            axis=0,
        )
        scores = []
        for ref, block in keys:
            s = dot_nt(q, ref[0:span, 0:HEAD_DIM]) * scale
            edge = jnp.where(col < cache, limit - block * cache, pos + (base - block * tokens + cache + 1))
            scores.append(jnp.where(col < edge, s, masked_score))
        peak = functools.reduce(jnp.maximum, [jnp.max(s, axis=1, keepdims=True) for s in scores])
        total = jnp.zeros((rows, 1), f32)
        numer = jnp.zeros((rows, HEAD_DIM), f32)
        for (ref, _), s in zip(keys, scores):
            w = jnp.exp2(s - peak)
            total += jnp.sum(w, axis=1, keepdims=True)
            numer += dot(w.astype(bf16), ref[0:span, HEAD_DIM:])
        out = (numer / total).astype(bf16)
        held[hi] = jnp.concatenate([out[g * tokens : (g + 1) * tokens] for g in range(group)], axis=1)
    over_z, over_x = units(group)
    for u, (j, h) in enumerate(over_z):
        za[u] = held[j, :, h * HEAD_DIM : (h + 1) * HEAD_DIM]
    for m, xb in enumerate((xb0, xb1, xb2, xb3)):
        for j in range(2):
            pick = expert_rows(route[2 * j + core][0:1], (e ^ m) * cap, cap)
            mine = [(u, h) for u, (i, h) in enumerate(over_x) if i == j]
            lo = mine[0][1] * HEAD_DIM
            got = dot(pick, held[j, :, lo : lo + len(mine) * HEAD_DIM]).astype(bf16)
            for i, (u, _) in enumerate(mine):
                xb[u] = got[:, i * HEAD_DIM : (i + 1) * HEAD_DIM]


def join_kernel(b0, b1, b2, b3, d):
    e = lax.axis_index("exp")
    for m, b in enumerate((b0, b1, b2, b3)):
        d[e ^ m] = b[...]


def regroup_kernel(route, a0, a1, a2, a3, c0, c1, c2, c3):
    e = lax.axis_index("exp")
    core = e % 2
    cap = c0.shape[2]
    over_z, _ = units(HEADS // KV_HEADS)
    for j in range(2):
        marks = route[2 * j + core][0:1]
        pick = jnp.concatenate([expert_rows(marks, (e ^ m) * cap, cap) for m in range(4)], axis=0)
        for u, (i, _) in enumerate(over_z):
            if i == j:
                for n, a in enumerate((a0, a1, a2, a3)):
                    got = dot(pick, a[u]).astype(bf16)
                    for m, c in enumerate((c0, c1, c2, c3)):
                        c[n, u] = got[m * cap : (m + 1) * cap]


def lanes_of(h):
    return slice(h * HEAD_DIM, (h + 1) * HEAD_DIM)


def half_kernel(c0, c1, gain, wg, wu, gate, upper, square, xh):
    z, e = lax.axis_index("ctx"), lax.axis_index("exp")
    slices, blocks, cap, part = xh.shape
    rows = blocks * cap
    over_z, _ = units(HEADS // KV_HEADS)
    wide = gain.shape[1] // KV_HEADS
    for m, c in enumerate((c0, c1)):
        src = e ^ m
        for n in range(slices):
            for u, (j, h) in enumerate(over_z):
                xh[z ^ n, 2 * j + src % 2, :, lanes_of(h)] = c[n, u]
    total, g, u = 0.0, 0.0, 0.0
    for n in range(slices):
        v = xh[n].reshape(rows, part).astype(f32)
        total += jnp.sum(v * v, axis=1, keepdims=True)
        at = pl.ds(pl.multiple_of((slices * (e // 2) + n) * wide, wide), part)
        x = (v * gain[0:1, at]).astype(bf16)
        g += dot_nt(x, wg[:, at])
        u += dot_nt(x, wu[:, at])
    gate[...] = g
    upper[...] = u
    square[...] = jnp.broadcast_to(total, square.shape)


def expert_kernel(
    gate, upper, square, xh, c2, c3, d0, d1, d2, d3, gain, wg, wu, wd,
    y0, y1, y2, y3, t0, t1, t2, t3, xo, xd, nz, sc, ys,
):
    z, e = lax.axis_index("ctx"), lax.axis_index("exp")
    slices, blocks, cap, wide = xo.shape
    rows = blocks * cap
    over_z, over_x = units(HEADS // KV_HEADS)
    mine, other = e // 2, 1 - e // 2
    part = xh.shape[3]
    for m, c in ((2, c2), (3, c3)):
        src = e ^ m
        for n in range(slices):
            for u, (j, h) in enumerate(over_z):
                xo[z ^ n, 2 * j + src % 2, :, lanes_of(h)] = c[n, u]
    for m, d in enumerate((d0, d1, d2, d3)):
        for k in range(2):
            for u, (j, _) in enumerate(over_x):
                xo[z ^ m, 2 * j + k, :, part:] = d[2 * other + k, u]
                xd[z ^ m, 2 * j + k] = d[2 * mine + k, u]
    total, g, u = square[:, 0:1], gate[...], upper[...]
    for x, first, side in ((xo, 0, other), (xd, part, mine)):
        width = x.shape[3]
        for n in range(slices):
            v = x[n].reshape(rows, width).astype(f32)
            total += jnp.sum(v * v, axis=1, keepdims=True)
            at = pl.ds(pl.multiple_of((slices * side + n) * wide + first, HEAD_DIM), width)
            r = (v * gain[0:1, at]).astype(bf16)
            g += dot_nt(r, wg[:, at])
            u += dot_nt(r, wu[:, at])
    scale = lax.rsqrt(total * (1.0 / gain.shape[1]) + 1e-05)
    sc[...] = jnp.broadcast_to(scale, sc.shape)
    g, u = g * scale, u * scale
    hidden = (g / (1.0 + jnp.exp(-g)) * u).astype(bf16)
    own_scale = sc[pl.ds(pl.multiple_of(z * cap, cap), cap), 0:1]
    for n in range(slices):
        for x, first, side in ((xo, 0, other), (xh, 0, mine), (xd, part, mine)):
            width = x.shape[3]
            s = slices * side + n
            at = pl.ds(pl.multiple_of(s * wide + first, HEAD_DIM), width)
            v = x[n, z].astype(f32) * own_scale * gain[0:1, at]
            nz[s, :, first : first + width] = v.astype(bf16)
    span, keep = ys.shape[1] + y0.shape[1], y0.shape[1]
    per = span // wide
    at_home = iota((rows, span), 0) // cap == z
    for m, y in enumerate((y0, y1, y2, y3)):
        o = e ^ m
        v = dot(hidden, wd[:, pl.ds(pl.multiple_of(o * span, span), span)])
        normed = jnp.concatenate([nz[o * per + i] for i in range(per)], axis=1).astype(f32)
        v = (v + jnp.where(at_home, jnp.concatenate([normed] * blocks, axis=0), 0.0)).astype(bf16)
        y[...] = v[:, :keep]
        ys[...] = v[:, keep:]
        for i, t in enumerate((t0, t1, t2, t3)):
            t[o] = ys[pl.ds(pl.multiple_of((z ^ i) * cap, cap), cap), :]


def turn_kernel(route, y0, y1, y2, y3, g0, g1, g2, g3):
    z, e = lax.axis_index("ctx"), lax.axis_index("exp")
    cap = y0.shape[0] // 4
    for m, g in enumerate((g0, g1, g2, g3)):
        block = z ^ m
        marks = route[block][0:1]
        pick = jnp.concatenate([expert_rows(marks, (e ^ n) * cap, cap) for n in range(4)], axis=0)
        at = pl.ds(pl.multiple_of(block * cap, cap), cap)
        got = jnp.concatenate([y[at, :] for y in (y0, y1, y2, y3)], axis=0)
        g[...] = dot_tn(pick, got).astype(bf16)


def total_kernel(t0, t1, t2, t3, h0, h1, h2, h3, ts):
    e = lax.axis_index("exp")
    ts[...] = sum(t[...].astype(f32) for t in (t0, t1, t2, t3)).astype(bf16)
    for m, h in enumerate((h0, h1, h2, h3)):
        h[...] = ts[e ^ m]


def final_kernel(route, g0, g1, g2, g3, h0, h1, h2, h3, out):
    z, e = lax.axis_index("ctx"), lax.axis_index("exp")
    cap = h0.shape[0]
    keep = g0.shape[1]
    out[:, 0:keep] = sum(g[...].astype(f32) for g in (g0, g1, g2, g3)).astype(bf16)
    marks = route[z][0:1]
    pick = jnp.concatenate([expert_rows(marks, (e ^ n) * cap, cap) for n in range(4)], axis=0)
    got = jnp.concatenate([h[...] for h in (h0, h1, h2, h3)], axis=0)
    out[:, keep:] = dot_tn(pick, got).astype(bf16)


def paired_path(*args):
    return paired_steps(*args)


def paired_steps(
    queries,
    new_keys,
    new_values,
    cache_keys,
    cache_values,
    offset,
    token_ids,
    expert_table,
    norm_gain,
    w_gate,
    w_up,
    w_down,
):
    n_ctx, n_exp = lax.axis_size("ctx"), lax.axis_size("exp")
    tokens = queries.shape[0]
    cache = cache_keys.shape[0]
    width = new_keys.shape[1]
    group = HEADS // KV_HEADS
    wide = group * HEAD_DIM
    cap = tokens // 2
    span = cache + tokens
    over_z, over_x = units(group)
    own = queries.shape[1]
    back = own * 3 // 8
    keep = own - back
    rows = n_ctx * cap

    def over_ctx(v, m):
        return lax.ppermute(v, "ctx", [(i, i ^ m) for i in range(n_ctx)])

    def over_exp(v, m):
        return lax.ppermute(v, "exp", [(i, i ^ m) for i in range(n_exp)])

    def head_step(v, o):
        pairs = []
        for z in range(n_ctx):
            for e in range(n_exp):
                core = e % 2
                to_z = 2 * core + ((z // 2) ^ o)
                pairs.append((z * n_exp + e, to_z * n_exp + e - core + z % 2))
        return lax.ppermute(v, ("ctx", "exp"), pairs)

    height = span + tokens * wide // width + 8
    copies = 2 + 2 * (4 + wide // width)
    table_rows = expert_table.reshape(-1, 128)
    p0, p1 = call(
        pack_kernel,
        [((height, width), bf16)] * 2,
        8,
        scratch=[
            pltpu.SMEM((tokens,), jnp.int32),
            pltpu.VMEM(table_rows.shape, jnp.int32),
            pltpu.VMEM((tokens, table_rows.shape[1]), jnp.int32),
            pltpu.SemaphoreType.DMA((copies,)),
        ],
        hbm=7,
    )(queries, new_keys, new_values, cache_keys, cache_values, token_ids, table_rows)
    limit = jnp.broadcast_to(offset[None, :], (8, 128))
    gate_t, up_t, down = jnp.swapaxes(w_gate[0], 0, 1), jnp.swapaxes(w_up[0], 0, 1), w_down[0]
    weight_bytes = 2 * (gate_t.size + up_t.size + down.size)
    gate_t, up_t, down, gain = call(
        fetch_kernel,
        [(w.shape, bf16) for w in (gate_t, up_t, down)] + [((1, norm_gain.shape[0]), f32)],
        4,
        scratch=[pltpu.SemaphoreType.DMA((4,))],
        hbm=4,
        cost=pl.CostEstimate(flops=1000 * weight_bytes, transcendentals=0, bytes_accessed=2 * weight_bytes),
    )(gate_t, up_t, down, norm_gain.reshape(1, -1))
    r0, r1 = head_step(p0, 0), head_step(p1, 1)
    r1, limit = lax.optimization_barrier((r1, limit))
    s0, s1 = over_exp(r0, 1), over_exp(r1, 1)
    za, xb0, xb1, xb2, xb3, route = call(
        functools.partial(attend_kernel, cache, tokens),
        [((len(over_z), tokens, HEAD_DIM), bf16)]
        + [((len(over_x), cap, HEAD_DIM), bf16)] * 4
        + [((n_ctx, 8, tokens), f32)],
        16,
        scratch=[pltpu.VMEM((2, tokens, wide), bf16)],
    )(limit, r0, r1, s0, s1)
    a = [za] + [over_ctx(za, m) for m in (1, 2, 3)]
    b = [xb0] + [over_exp(v, m) for m, v in ((1, xb1), (2, xb2), (3, xb3))]
    (zd,) = call(join_kernel, [((n_exp, len(over_x), cap, HEAD_DIM), bf16)], 4)(*b)
    d = [zd] + [over_ctx(zd, m) for m in (1, 2, 3)]
    c0, c1, c2, c3 = call(
        regroup_kernel, [((n_ctx, len(over_z), cap, HEAD_DIM), bf16)] * 4, 8
    )(route, *a)
    c = [c0] + [over_exp(v, m) for m, v in ((1, c1), (2, c2), (3, c3))]
    units_hidden = gate_t.shape[0]
    part = wide - HEAD_DIM
    gate, upper, square, xh = call(
        half_kernel,
        [((rows, units_hidden), f32)] * 2 + [((rows, 128), f32), ((n_ctx, n_ctx, cap, part), bf16)],
        20,
        cost=pl.CostEstimate(flops=2 * rows * units_hidden * n_ctx * part * 2, transcendentals=0, bytes_accessed=0),
    )(c[0], c[1], gain, gate_t, up_t)
    outs = call(
        expert_kernel,
        [((rows, keep), bf16)] * 4 + [((n_exp, cap, back), bf16)] * 4,
        28,
        scratch=[
            pltpu.VMEM((n_ctx, n_ctx, cap, wide), bf16),
            pltpu.VMEM((n_ctx, n_ctx, cap, HEAD_DIM), bf16),
            pltpu.VMEM((KV_HEADS, cap, wide), bf16),
            pltpu.VMEM((rows, 128), f32),
            pltpu.VMEM((rows, back), bf16),
        ],
    )(gate, upper, square, xh, c[2], c[3], *d, gain, gate_t, up_t, down)
    y, t = outs[:4], outs[4:]
    t = [t[0]] + [over_ctx(t[m], m) for m in (1, 2, 3)]
    y = [y[0]] + [over_exp(y[m], m) for m in (1, 2, 3)]
    g = call(turn_kernel, [((tokens, keep), bf16)] * 4, 8)(route, *y)
    g = [g[0]] + [over_ctx(g[m], m) for m in (1, 2, 3)]
    h = call(
        total_kernel, [((cap, back), bf16)] * 4, 8, scratch=[pltpu.VMEM((n_exp, cap, back), bf16)]
    )(*t)
    h = [h[0]] + [over_exp(h[m], m) for m in (1, 2, 3)]
    (out,) = call(final_kernel, [((tokens, own), bf16)], 8)(route, *g, *h)
    return out


def solution(mesh):
    placed = (
        P(("group", "ctx"), "exp"),
        P(("group", "ctx"), "exp"),
        P(("group", "ctx"), "exp"),
        P(("group", "ctx"), "exp"),
        P(("group", "ctx"), "exp"),
        P("group"),
        P(("group", "ctx")),
        P("group"),
        P(),
        P("exp", None, "ctx"),
        P("exp", None, "ctx"),
        P("exp", "ctx", None),
    )
    n_ctx, n_exp = mesh.shape["ctx"], mesh.shape["exp"]
    paired = n_ctx == n_exp == 4 and KV_HEADS == 2 * n_exp
    return jax.shard_map(
        paired_path if paired else general_path,
        mesh=mesh,
        in_specs=placed,
        out_specs=P(("group", "ctx"), "exp"),
        check_vma=False,
    )
```

```python
import functools
import math

import jax
import jax.numpy as jnp
from jax import lax
from jax.experimental import pallas as pl
from jax.experimental.pallas import tpu as pltpu
from jax.sharding import PartitionSpec as P


HEADS = 32
KV_HEADS = 8
HEAD_DIM = 128


masked_score = -1e30
f32 = jnp.float32
bf16 = jnp.bfloat16


def split_heads(flat, heads):
    return flat.reshape(flat.shape[0], heads, flat.shape[1] // heads)


def partial_attend(query_rows, key_rows, value_rows, allowed):
    width = query_rows.shape[3]
    scores = jnp.einsum("rkgd,skd->rkgs", query_rows, key_rows, preferred_element_type=jnp.float32)
    scores = scores * (1.0 / math.sqrt(width))
    usable = allowed[:, None, None, :]
    peak = jnp.max(jnp.where(usable, scores, masked_score), axis=-1)
    unnorm = jnp.where(usable, jnp.exp(scores - peak[..., None]), 0.0)
    total = jnp.sum(unnorm, axis=-1)
    numer = jnp.einsum(
        "rkgs,skd->rkgd",
        unnorm.astype(jnp.bfloat16),
        value_rows,
        preferred_element_type=jnp.float32,
    )
    return (numer, peak, total)


def general_path(
    queries,
    new_keys,
    new_values,
    cache_keys,
    cache_values,
    offset,
    token_ids,
    expert_table,
    norm_gain,
    w_gate,
    w_up,
    w_down,
):
    owners = lax.axis_size("exp")
    heads_local = HEADS // owners
    kv_local = KV_HEADS // owners
    group = HEADS // KV_HEADS
    tok_count = queries.shape[0]
    cache_len = cache_keys.shape[0]
    shard = lax.axis_index("ctx")
    limit = offset[0]
    key_rows = jnp.concatenate([cache_keys, new_keys], axis=0)
    value_rows = jnp.concatenate([cache_values, new_values], axis=0)
    span = key_rows.shape[0]
    own_index = shard * tok_count + jnp.arange(tok_count, dtype=jnp.int32)
    grouped = queries.reshape(tok_count, kv_local, group, HEAD_DIM)
    piece_keys = lax.all_gather(key_rows, "ctx", axis=0, tiled=True)
    piece_values = lax.all_gather(value_rows, "ctx", axis=0, tiled=True)
    flat = jnp.arange(piece_keys.shape[0], dtype=jnp.int32)
    source = flat // span
    inner = flat % span
    cache_ok = source * cache_len + inner < limit
    stretch_ok = (source * tok_count + inner - cache_len)[None, :] <= own_index[:, None]
    allowed = jnp.where((inner < cache_len)[None, :], cache_ok[None, :], stretch_ok)
    numer, _, total = partial_attend(
        grouped, split_heads(piece_keys, kv_local), split_heads(piece_values, kv_local), allowed
    )
    attended = (numer / total[..., None]).reshape(tok_count, heads_local * HEAD_DIM).astype(jnp.bfloat16)
    capacity = tok_count // 2
    chosen = expert_table[token_ids]
    onehot = (chosen[:, None] == jnp.arange(owners, dtype=jnp.int32)[None, :]).astype(jnp.int32)
    earlier = jnp.cumsum(onehot, axis=0) - onehot
    slot = jnp.sum(earlier * onehot, axis=1)
    target = chosen * capacity + slot
    dispatch = (jnp.arange(owners * capacity, dtype=jnp.int32)[:, None] == target[None, :]).astype(
        jnp.bfloat16
    )
    packed = jnp.dot(dispatch, attended, preferred_element_type=jnp.float32).astype(jnp.bfloat16)
    arrived = lax.all_to_all(packed, "exp", split_axis=0, concat_axis=1, tiled=True)
    values32 = arrived.astype(jnp.float32)
    scale = lax.rsqrt(jnp.mean(values32 * values32, axis=-1, keepdims=True) + 1e-05)
    normed = (values32 * scale * norm_gain).astype(jnp.bfloat16)
    piece = lax.all_gather(normed, "ctx", axis=0, tiled=True)
    gate = jnp.dot(piece, w_gate[0], preferred_element_type=jnp.float32)
    upper = jnp.dot(piece, w_up[0], preferred_element_type=jnp.float32)
    hidden = (jax.nn.silu(gate) * upper).astype(jnp.bfloat16)
    summed = lax.psum_scatter(
        jnp.dot(hidden, w_down[0], preferred_element_type=jnp.float32).astype(jnp.bfloat16),
        "ctx",
        scatter_dimension=0,
        tiled=True,
    ).astype(jnp.float32)
    combined = (normed.astype(jnp.float32) + summed).astype(jnp.bfloat16)
    returned = lax.all_to_all(combined, "exp", split_axis=1, concat_axis=0, tiled=True)
    collect = (target[:, None] == jnp.arange(owners * capacity, dtype=jnp.int32)[None, :]).astype(
        jnp.bfloat16
    )
    return jnp.dot(collect, returned, preferred_element_type=jnp.float32).astype(jnp.bfloat16)


def iota(shape, axis):
    return lax.broadcasted_iota(jnp.int32, shape, axis)


def call(kernel, out_shapes, mib, scratch=(), hbm=0, cost=None):
    def run(*args):
        args = [pltpu.with_memory_space_constraint(v, pltpu.HBM) if i < hbm else v for i, v in enumerate(args)]
        vmem = pl.BlockSpec(memory_space=pltpu.VMEM)
        specs = [pl.BlockSpec(memory_space=pltpu.HBM)] * hbm + [vmem] * (len(args) - hbm)
        return pl.pallas_call(
            kernel,
            out_shape=[jax.ShapeDtypeStruct(s, d) for s, d in out_shapes],
            in_specs=specs,
            out_specs=[vmem] * len(out_shapes),
            scratch_shapes=list(scratch),
            compiler_params=pltpu.CompilerParams(vmem_limit_bytes=mib << 20),
            cost_estimate=cost,
        )(*args)

    return run


def expert_rows(marks, first, cap):
    tokens = marks.shape[1]
    slots = (iota((cap, tokens), 0) + first).astype(f32)
    return (marks == slots).astype(bf16)


def dot(a, b):
    return jnp.dot(a, b, preferred_element_type=f32)


def dot_nt(a, b):
    return lax.dot_general(a, b, (((1,), (1,)), ((), ())), preferred_element_type=f32)


def dot_tn(a, b):
    return lax.dot_general(a, b, (((0,), (0,)), ((), ())), preferred_element_type=f32)


def pack_kernel(q, nk, nv, ck, cv, ids, table, p0, p1, id_smem, rows, found, sems):
    z = lax.axis_index("ctx")
    tokens, cache = q.shape[0], ck.shape[0]
    span = cache + tokens
    width = p0.shape[1]
    wide = q.shape[1] // 2
    cap = tokens // 2
    top = span + (wide // width) * tokens
    lanes = found.shape[1]
    swap = (z // 2) == 1

    first = [
        pltpu.make_async_copy(ids, id_smem, sems.at[0]),
        pltpu.make_async_copy(table, rows, sems.at[1]),
    ]
    for copy in first:
        copy.start()

    def pieces(p, h, base):
        at = pl.ds(h * HEAD_DIM, HEAD_DIM)
        moves = [
            (ck.at[:, at], p.at[0:cache, 0:HEAD_DIM]),
            (cv.at[:, at], p.at[0:cache, HEAD_DIM:]),
            (nk.at[:, at], p.at[cache:span, 0:HEAD_DIM]),
            (nv.at[:, at], p.at[cache:span, HEAD_DIM:]),
        ]
        for part in range(wide // width):
            lo = h * wide + part * width
            moves.append((q.at[:, pl.ds(lo, width)], p.at[span + part * tokens : span + (part + 1) * tokens, :]))
        return [pltpu.make_async_copy(src, dst, sems.at[base + i]) for i, (src, dst) in enumerate(moves)]

    count = 4 + wide // width

    @pl.when(jnp.logical_not(swap))
    def _():
        for copy in pieces(p0, 0, 2) + pieces(p1, 1, 2 + count):
            copy.start()

    @pl.when(swap)
    def _():
        for copy in pieces(p0, 1, 2) + pieces(p1, 0, 2 + count):
            copy.start()

    for copy in first:
        copy.wait()
    lane = iota((1, lanes), 1)
    for t in range(tokens):
        at = id_smem[t]
        row = rows[pl.ds(lax.shift_right_logical(at, lanes.bit_length() - 1), 1), :]
        found[t : t + 1, :] = jnp.where(lane == (at & (lanes - 1)), row, 0)
    here, there = iota((tokens, tokens), 0), iota((tokens, tokens), 1)
    who = jnp.sum(found[...].astype(f32), axis=1, keepdims=True)
    who_row = jnp.sum(jnp.where(here == there, who, 0.0), axis=0, keepdims=True)
    ahead = jnp.where((who == who_row) & (here < there), 1.0, 0.0)
    marks = who_row * cap + jnp.sum(ahead, axis=0, keepdims=True)
    for p in (p0, p1):
        p[top:, :tokens] = jnp.broadcast_to(marks, (p.shape[0] - top, tokens)).astype(bf16)
    for copy in pieces(p0, 0, 2) + pieces(p1, 1, 2 + count):
        copy.wait()


def fetch_kernel(wg, wu, wd, gain, og, ou, od, ogain, sems):
    copies = [
        pltpu.make_async_copy(src, dst, sems.at[i])
        for i, (src, dst) in enumerate(((wg, og), (wu, ou), (wd, od), (gain, ogain)))
    ]
    for copy in copies:
        copy.start()
    for copy in copies:
        copy.wait()


def units(heads):
    over_z = [(j, h) for j in range(2) for h in range(heads - 1)]
    return over_z, [(j, heads - 1) for j in range(2)]


def attend_kernel(cache, tokens, offset, r0, r1, s0, s1, za, xb0, xb1, xb2, xb3, route, held):
    z, e = lax.axis_index("ctx"), lax.axis_index("exp")
    core = e % 2
    span = cache + tokens
    cap = tokens // 2
    width = r0.shape[1]
    group = HEADS // KV_HEADS
    per_row = width // HEAD_DIM
    top = span + (group // per_row) * tokens
    limit = offset[0:1, 0:1]
    scale = math.log2(math.e) / math.sqrt(HEAD_DIM)
    halves = (z % 2, 1 - z % 2)
    keys = [(r, 2 * hi + core) for r, hi in zip((r0, r1), halves)]
    keys += [(s, 2 * hi + 1 - core) for s, hi in zip((s0, s1), halves)]
    rows = group * tokens
    pos = iota((rows, span), 0) % tokens
    col = iota((rows, span), 1)
    for ref, block in keys:
        route[block] = ref[top:, :tokens].astype(f32)
    for r, hi in zip((r0, r1), halves):
        base = (2 * hi + core) * tokens
        q = jnp.concatenate(
            [
                r[span + (g // per_row) * tokens : span + (g // per_row + 1) * tokens,
                  (g % per_row) * HEAD_DIM : (g % per_row + 1) * HEAD_DIM]
                for g in range(group)
            ],
            axis=0,
        )
        scores = []
        for ref, block in keys:
            s = dot_nt(q, ref[0:span, 0:HEAD_DIM]) * scale
            edge = jnp.where(col < cache, limit - block * cache, pos + (base - block * tokens + cache + 1))
            scores.append(jnp.where(col < edge, s, masked_score))
        peak = functools.reduce(jnp.maximum, [jnp.max(s, axis=1, keepdims=True) for s in scores])
        total = jnp.zeros((rows, 1), f32)
        numer = jnp.zeros((rows, HEAD_DIM), f32)
        for (ref, _), s in zip(keys, scores):
            w = jnp.exp2(s - peak)
            total += jnp.sum(w, axis=1, keepdims=True)
            numer += dot(w.astype(bf16), ref[0:span, HEAD_DIM:])
        out = (numer / total).astype(bf16)
        held[hi] = jnp.concatenate([out[g * tokens : (g + 1) * tokens] for g in range(group)], axis=1)
    over_z, over_x = units(group)
    for u, (j, h) in enumerate(over_z):
        za[u] = held[j, :, h * HEAD_DIM : (h + 1) * HEAD_DIM]
    for m, xb in enumerate((xb0, xb1, xb2, xb3)):
        for j in range(2):
            pick = expert_rows(route[2 * j + core][0:1], (e ^ m) * cap, cap)
            got = dot(pick, held[j]).astype(bf16)
            for u, (i, h) in enumerate(over_x + over_z):
                if i == j:
                    xb[u] = got[:, h * HEAD_DIM : (h + 1) * HEAD_DIM]


def join_kernel(b0, b1, b2, b3, d):
    e = lax.axis_index("exp")
    for m, b in enumerate((b0, b1, b2, b3)):
        d[e ^ m] = b[0 : d.shape[1]]


def regroup_kernel(route, a1, a2, a3, c0, c1, c2, c3):
    e = lax.axis_index("exp")
    core = e % 2
    cap = c0.shape[2]
    over_z, _ = units(HEADS // KV_HEADS)
    for j in range(2):
        marks = route[2 * j + core][0:1]
        pick = jnp.concatenate([expert_rows(marks, (e ^ m) * cap, cap) for m in range(4)], axis=0)
        for u, (i, _) in enumerate(over_z):
            if i == j:
                for n, a in enumerate((a1, a2, a3)):
                    got = dot(pick, a[u]).astype(bf16)
                    for m, c in enumerate((c0, c1, c2, c3)):
                        c[n, u] = got[m * cap : (m + 1) * cap]


def lanes_of(h):
    return slice(h * HEAD_DIM, (h + 1) * HEAD_DIM)


def half_kernel(c0, c1, b0, b1, gain, wg, wu, gate, upper, square, xh):
    z, e = lax.axis_index("ctx"), lax.axis_index("exp")
    slices, blocks, cap, part = xh.shape
    rows = blocks * cap
    over_z, over_x = units(HEADS // KV_HEADS)
    wide = gain.shape[1] // KV_HEADS
    for m, (c, b) in enumerate(((c0, b0), (c1, b1))):
        src = e ^ m
        for u, (j, h) in enumerate(over_z):
            xh[z, 2 * j + src % 2, :, lanes_of(h)] = b[len(over_x) + u]
            for n in range(1, slices):
                xh[z ^ n, 2 * j + src % 2, :, lanes_of(h)] = c[n - 1, u]
    total, g, u = 0.0, 0.0, 0.0
    for n in range(slices):
        v = xh[n].reshape(rows, part).astype(f32)
        total += jnp.sum(v * v, axis=1, keepdims=True)
        at = pl.ds(pl.multiple_of((slices * (e // 2) + n) * wide, wide), part)
        x = (v * gain[0:1, at]).astype(bf16)
        g += dot_nt(x, wg[:, at])
        u += dot_nt(x, wu[:, at])
    gate[...] = g
    upper[...] = u
    square[...] = jnp.broadcast_to(total, square.shape)


def expert_kernel(
    gate, upper, square, xh, c2, c3, b2, b3, d0, d1, d2, d3, gain, wg, wu, wd,
    y0, y1, y2, y3, t0, t1, t2, t3, xo, xd, nz, sc, ys,
):
    z, e = lax.axis_index("ctx"), lax.axis_index("exp")
    slices, blocks, cap, wide = xo.shape
    rows = blocks * cap
    over_z, over_x = units(HEADS // KV_HEADS)
    mine, other = e // 2, 1 - e // 2
    part = xh.shape[3]
    for m, c, b in ((2, c2, b2), (3, c3, b3)):
        src = e ^ m
        for u, (j, h) in enumerate(over_z):
            xo[z, 2 * j + src % 2, :, lanes_of(h)] = b[len(over_x) + u]
            for n in range(1, slices):
                xo[z ^ n, 2 * j + src % 2, :, lanes_of(h)] = c[n - 1, u]
    for m, d in enumerate((d0, d1, d2, d3)):
        for k in range(2):
            for u, (j, _) in enumerate(over_x):
                xo[z ^ m, 2 * j + k, :, part:] = d[2 * other + k, u]
                xd[z ^ m, 2 * j + k] = d[2 * mine + k, u]
    total, g, u = square[:, 0:1], gate[...], upper[...]
    for x, first, side in ((xo, 0, other), (xd, part, mine)):
        width = x.shape[3]
        for n in range(slices):
            v = x[n].reshape(rows, width).astype(f32)
            total += jnp.sum(v * v, axis=1, keepdims=True)
            at = pl.ds(pl.multiple_of((slices * side + n) * wide + first, HEAD_DIM), width)
            r = (v * gain[0:1, at]).astype(bf16)
            g += dot_nt(r, wg[:, at])
            u += dot_nt(r, wu[:, at])
    scale = lax.rsqrt(total * (1.0 / gain.shape[1]) + 1e-05)
    sc[...] = jnp.broadcast_to(scale, sc.shape)
    g, u = g * scale, u * scale
    hidden = (g / (1.0 + jnp.exp(-g)) * u).astype(bf16)
    own_scale = sc[pl.ds(pl.multiple_of(z * cap, cap), cap), 0:1]
    for n in range(slices):
        for x, first, side in ((xo, 0, other), (xh, 0, mine), (xd, part, mine)):
            width = x.shape[3]
            s = slices * side + n
            at = pl.ds(pl.multiple_of(s * wide + first, HEAD_DIM), width)
            v = x[n, z].astype(f32) * own_scale * gain[0:1, at]
            nz[s, :, first : first + width] = v.astype(bf16)
    span, keep = ys.shape[1] + y0.shape[1], y0.shape[1]
    per = span // wide
    at_home = iota((rows, span), 0) // cap == z
    for m, y in enumerate((y0, y1, y2, y3)):
        o = e ^ m
        v = dot(hidden, wd[:, pl.ds(pl.multiple_of(o * span, span), span)])
        normed = jnp.concatenate([nz[o * per + i] for i in range(per)], axis=1).astype(f32)
        v = (v + jnp.where(at_home, jnp.concatenate([normed] * blocks, axis=0), 0.0)).astype(bf16)
        y[...] = v[:, :keep]
        ys[...] = v[:, keep:]
        for i, t in enumerate((t0, t1, t2, t3)):
            t[o] = ys[pl.ds(pl.multiple_of((z ^ i) * cap, cap), cap), :]


def turn_kernel(route, y0, y1, y2, y3, g0, g1, g2, g3):
    z, e = lax.axis_index("ctx"), lax.axis_index("exp")
    cap = y0.shape[0] // 4
    for m, g in enumerate((g0, g1, g2, g3)):
        block = z ^ m
        marks = route[block][0:1]
        pick = jnp.concatenate([expert_rows(marks, (e ^ n) * cap, cap) for n in range(4)], axis=0)
        at = pl.ds(pl.multiple_of(block * cap, cap), cap)
        got = jnp.concatenate([y[at, :] for y in (y0, y1, y2, y3)], axis=0)
        g[...] = dot_tn(pick, got).astype(bf16)


def total_kernel(t0, t1, t2, t3, h0, h1, h2, h3, ts):
    e = lax.axis_index("exp")
    ts[...] = sum(t[...].astype(f32) for t in (t0, t1, t2, t3)).astype(bf16)
    for m, h in enumerate((h0, h1, h2, h3)):
        h[...] = ts[e ^ m]


def final_kernel(route, g0, g1, g2, g3, h0, h1, h2, h3, out):
    z, e = lax.axis_index("ctx"), lax.axis_index("exp")
    cap = h0.shape[0]
    keep = g0.shape[1]
    out[:, 0:keep] = sum(g[...].astype(f32) for g in (g0, g1, g2, g3)).astype(bf16)
    marks = route[z][0:1]
    pick = jnp.concatenate([expert_rows(marks, (e ^ n) * cap, cap) for n in range(4)], axis=0)
    got = jnp.concatenate([h[...] for h in (h0, h1, h2, h3)], axis=0)
    out[:, keep:] = dot_tn(pick, got).astype(bf16)


def paired_path(*args):
    return paired_steps(*args)


def paired_steps(
    queries,
    new_keys,
    new_values,
    cache_keys,
    cache_values,
    offset,
    token_ids,
    expert_table,
    norm_gain,
    w_gate,
    w_up,
    w_down,
):
    n_ctx, n_exp = lax.axis_size("ctx"), lax.axis_size("exp")
    tokens = queries.shape[0]
    cache = cache_keys.shape[0]
    width = new_keys.shape[1]
    group = HEADS // KV_HEADS
    wide = group * HEAD_DIM
    cap = tokens // 2
    span = cache + tokens
    over_z, over_x = units(group)
    own = queries.shape[1]
    back = own * 3 // 8
    keep = own - back
    rows = n_ctx * cap

    def over_ctx(v, m):
        return lax.ppermute(v, "ctx", [(i, i ^ m) for i in range(n_ctx)])

    def over_exp(v, m):
        return lax.ppermute(v, "exp", [(i, i ^ m) for i in range(n_exp)])

    def head_step(v, o):
        pairs = []
        for z in range(n_ctx):
            for e in range(n_exp):
                core = e % 2
                to_z = 2 * core + ((z // 2) ^ o)
                pairs.append((z * n_exp + e, to_z * n_exp + e - core + z % 2))
        return lax.ppermute(v, ("ctx", "exp"), pairs)

    height = span + tokens * wide // width + 8
    copies = 2 + 2 * (4 + wide // width)
    table_rows = expert_table.reshape(-1, 128)
    p0, p1 = call(
        pack_kernel,
        [((height, width), bf16)] * 2,
        8,
        scratch=[
            pltpu.SMEM((tokens,), jnp.int32),
            pltpu.VMEM(table_rows.shape, jnp.int32),
            pltpu.VMEM((tokens, table_rows.shape[1]), jnp.int32),
            pltpu.SemaphoreType.DMA((copies,)),
        ],
        hbm=7,
    )(queries, new_keys, new_values, cache_keys, cache_values, token_ids, table_rows)
    limit = jnp.broadcast_to(offset[None, :], (8, 128))
    gate_t, up_t, down = jnp.swapaxes(w_gate[0], 0, 1), jnp.swapaxes(w_up[0], 0, 1), w_down[0]
    weight_bytes = 2 * (gate_t.size + up_t.size + down.size)
    gate_t, up_t, down, gain = call(
        fetch_kernel,
        [(w.shape, bf16) for w in (gate_t, up_t, down)] + [((1, norm_gain.shape[0]), f32)],
        4,
        scratch=[pltpu.SemaphoreType.DMA((4,))],
        hbm=4,
        cost=pl.CostEstimate(flops=1000 * weight_bytes, transcendentals=0, bytes_accessed=2 * weight_bytes),
    )(gate_t, up_t, down, norm_gain.reshape(1, -1))
    r0, r1 = head_step(p0, 0), head_step(p1, 1)
    r1, limit = lax.optimization_barrier((r1, limit))
    s0, s1 = over_exp(r0, 1), over_exp(r1, 1)
    za, xb0, xb1, xb2, xb3, route = call(
        functools.partial(attend_kernel, cache, tokens),
        [((len(over_z), tokens, HEAD_DIM), bf16)]
        + [((2 * group, cap, HEAD_DIM), bf16)] * 4
        + [((n_ctx, 8, tokens), f32)],
        16,
        scratch=[pltpu.VMEM((2, tokens, wide), bf16)],
    )(limit, r0, r1, s0, s1)
    a = [za] + [over_ctx(za, m) for m in (1, 2, 3)]
    b = [xb0] + [over_exp(v, m) for m, v in ((1, xb1), (2, xb2), (3, xb3))]
    (zd,) = call(join_kernel, [((n_exp, len(over_x), cap, HEAD_DIM), bf16)], 4)(*b)
    d = [zd] + [over_ctx(zd, m) for m in (1, 2, 3)]
    c0, c1, c2, c3 = call(
        regroup_kernel, [((n_ctx - 1, len(over_z), cap, HEAD_DIM), bf16)] * 4, 8
    )(route, *a[1:])
    c = [c0] + [over_exp(v, m) for m, v in ((1, c1), (2, c2), (3, c3))]
    units_hidden = gate_t.shape[0]
    part = wide - HEAD_DIM
    gate, upper, square, xh = call(
        half_kernel,
        [((rows, units_hidden), f32)] * 2 + [((rows, 128), f32), ((n_ctx, n_ctx, cap, part), bf16)],
        20,
        cost=pl.CostEstimate(flops=2 * rows * units_hidden * n_ctx * part * 2, transcendentals=0, bytes_accessed=0),
    )(c[0], c[1], b[0], b[1], gain, gate_t, up_t)
    outs = call(
        expert_kernel,
        [((rows, keep), bf16)] * 4 + [((n_exp, cap, back), bf16)] * 4,
        28,
        scratch=[
            pltpu.VMEM((n_ctx, n_ctx, cap, wide), bf16),
            pltpu.VMEM((n_ctx, n_ctx, cap, HEAD_DIM), bf16),
            pltpu.VMEM((KV_HEADS, cap, wide), bf16),
            pltpu.VMEM((rows, 128), f32),
            pltpu.VMEM((rows, back), bf16),
        ],
    )(gate, upper, square, xh, c[2], c[3], b[2], b[3], *d, gain, gate_t, up_t, down)
    y, t = outs[:4], outs[4:]
    t = [t[0]] + [over_ctx(t[m], m) for m in (1, 2, 3)]
    y = [y[0]] + [over_exp(y[m], m) for m in (1, 2, 3)]
    g = call(turn_kernel, [((tokens, keep), bf16)] * 4, 8)(route, *y)
    g = [g[0]] + [over_ctx(g[m], m) for m in (1, 2, 3)]
    h = call(
        total_kernel, [((cap, back), bf16)] * 4, 8, scratch=[pltpu.VMEM((n_exp, cap, back), bf16)]
    )(*t)
    h = [h[0]] + [over_exp(h[m], m) for m in (1, 2, 3)]
    (out,) = call(final_kernel, [((tokens, own), bf16)], 8)(route, *g, *h)
    return out


def solution(mesh):
    placed = (
        P(("group", "ctx"), "exp"),
        P(("group", "ctx"), "exp"),
        P(("group", "ctx"), "exp"),
        P(("group", "ctx"), "exp"),
        P(("group", "ctx"), "exp"),
        P("group"),
        P(("group", "ctx")),
        P("group"),
        P(),
        P("exp", None, "ctx"),
        P("exp", None, "ctx"),
        P("exp", "ctx", None),
    )
    n_ctx, n_exp = mesh.shape["ctx"], mesh.shape["exp"]
    paired = n_ctx == n_exp == 4 and KV_HEADS == 2 * n_exp
    return jax.shard_map(
        paired_path if paired else general_path,
        mesh=mesh,
        in_specs=placed,
        out_specs=P(("group", "ctx"), "exp"),
        check_vma=False,
    )
```

```python
import functools
import math

import jax
import jax.numpy as jnp
from jax import lax
from jax.experimental import pallas as pl
from jax.experimental.pallas import tpu as pltpu
from jax.sharding import PartitionSpec as P


HEADS = 32
KV_HEADS = 8
HEAD_DIM = 128


masked_score = -1e30
f32 = jnp.float32
bf16 = jnp.bfloat16


def split_heads(flat, heads):
    return flat.reshape(flat.shape[0], heads, flat.shape[1] // heads)


def partial_attend(query_rows, key_rows, value_rows, allowed):
    width = query_rows.shape[3]
    scores = jnp.einsum("rkgd,skd->rkgs", query_rows, key_rows, preferred_element_type=jnp.float32)
    scores = scores * (1.0 / math.sqrt(width))
    usable = allowed[:, None, None, :]
    peak = jnp.max(jnp.where(usable, scores, masked_score), axis=-1)
    unnorm = jnp.where(usable, jnp.exp(scores - peak[..., None]), 0.0)
    total = jnp.sum(unnorm, axis=-1)
    numer = jnp.einsum(
        "rkgs,skd->rkgd",
        unnorm.astype(jnp.bfloat16),
        value_rows,
        preferred_element_type=jnp.float32,
    )
    return (numer, peak, total)


def general_path(
    queries,
    new_keys,
    new_values,
    cache_keys,
    cache_values,
    offset,
    token_ids,
    expert_table,
    norm_gain,
    w_gate,
    w_up,
    w_down,
):
    owners = lax.axis_size("exp")
    heads_local = HEADS // owners
    kv_local = KV_HEADS // owners
    group = HEADS // KV_HEADS
    tok_count = queries.shape[0]
    cache_len = cache_keys.shape[0]
    shard = lax.axis_index("ctx")
    limit = offset[0]
    key_rows = jnp.concatenate([cache_keys, new_keys], axis=0)
    value_rows = jnp.concatenate([cache_values, new_values], axis=0)
    span = key_rows.shape[0]
    own_index = shard * tok_count + jnp.arange(tok_count, dtype=jnp.int32)
    grouped = queries.reshape(tok_count, kv_local, group, HEAD_DIM)
    piece_keys = lax.all_gather(key_rows, "ctx", axis=0, tiled=True)
    piece_values = lax.all_gather(value_rows, "ctx", axis=0, tiled=True)
    flat = jnp.arange(piece_keys.shape[0], dtype=jnp.int32)
    source = flat // span
    inner = flat % span
    cache_ok = source * cache_len + inner < limit
    stretch_ok = (source * tok_count + inner - cache_len)[None, :] <= own_index[:, None]
    allowed = jnp.where((inner < cache_len)[None, :], cache_ok[None, :], stretch_ok)
    numer, _, total = partial_attend(
        grouped, split_heads(piece_keys, kv_local), split_heads(piece_values, kv_local), allowed
    )
    attended = (numer / total[..., None]).reshape(tok_count, heads_local * HEAD_DIM).astype(jnp.bfloat16)
    capacity = tok_count // 2
    chosen = expert_table[token_ids]
    onehot = (chosen[:, None] == jnp.arange(owners, dtype=jnp.int32)[None, :]).astype(jnp.int32)
    earlier = jnp.cumsum(onehot, axis=0) - onehot
    slot = jnp.sum(earlier * onehot, axis=1)
    target = chosen * capacity + slot
    dispatch = (jnp.arange(owners * capacity, dtype=jnp.int32)[:, None] == target[None, :]).astype(
        jnp.bfloat16
    )
    packed = jnp.dot(dispatch, attended, preferred_element_type=jnp.float32).astype(jnp.bfloat16)
    arrived = lax.all_to_all(packed, "exp", split_axis=0, concat_axis=1, tiled=True)
    values32 = arrived.astype(jnp.float32)
    scale = lax.rsqrt(jnp.mean(values32 * values32, axis=-1, keepdims=True) + 1e-05)
    normed = (values32 * scale * norm_gain).astype(jnp.bfloat16)
    piece = lax.all_gather(normed, "ctx", axis=0, tiled=True)
    gate = jnp.dot(piece, w_gate[0], preferred_element_type=jnp.float32)
    upper = jnp.dot(piece, w_up[0], preferred_element_type=jnp.float32)
    hidden = (jax.nn.silu(gate) * upper).astype(jnp.bfloat16)
    summed = lax.psum_scatter(
        jnp.dot(hidden, w_down[0], preferred_element_type=jnp.float32).astype(jnp.bfloat16),
        "ctx",
        scatter_dimension=0,
        tiled=True,
    ).astype(jnp.float32)
    combined = (normed.astype(jnp.float32) + summed).astype(jnp.bfloat16)
    returned = lax.all_to_all(combined, "exp", split_axis=1, concat_axis=0, tiled=True)
    collect = (target[:, None] == jnp.arange(owners * capacity, dtype=jnp.int32)[None, :]).astype(
        jnp.bfloat16
    )
    return jnp.dot(collect, returned, preferred_element_type=jnp.float32).astype(jnp.bfloat16)


def iota(shape, axis):
    return lax.broadcasted_iota(jnp.int32, shape, axis)


def call(kernel, out_shapes, mib, scratch=(), hbm=0, cost=None):
    def run(*args):
        args = [pltpu.with_memory_space_constraint(v, pltpu.HBM) if i < hbm else v for i, v in enumerate(args)]
        vmem = pl.BlockSpec(memory_space=pltpu.VMEM)
        specs = [pl.BlockSpec(memory_space=pltpu.HBM)] * hbm + [vmem] * (len(args) - hbm)
        return pl.pallas_call(
            kernel,
            out_shape=[jax.ShapeDtypeStruct(s, d) for s, d in out_shapes],
            in_specs=specs,
            out_specs=[vmem] * len(out_shapes),
            scratch_shapes=list(scratch),
            compiler_params=pltpu.CompilerParams(vmem_limit_bytes=mib << 20),
            cost_estimate=cost,
        )(*args)

    return run


def expert_rows(marks, first, cap):
    tokens = marks.shape[1]
    slots = (iota((cap, tokens), 0) + first).astype(f32)
    return (marks == slots).astype(bf16)


def dot(a, b):
    return jnp.dot(a, b, preferred_element_type=f32)


def dot_nt(a, b):
    return lax.dot_general(a, b, (((1,), (1,)), ((), ())), preferred_element_type=f32)


def dot_tn(a, b):
    return lax.dot_general(a, b, (((0,), (0,)), ((), ())), preferred_element_type=f32)


def pack_kernel(q, nk, nv, ck, cv, ids, table, p0, p1, id_smem, rows, found, sems):
    z = lax.axis_index("ctx")
    tokens, cache = q.shape[0], ck.shape[0]
    span = cache + tokens
    width = p0.shape[1]
    wide = q.shape[1] // 2
    cap = tokens // 2
    top = span + (wide // width) * tokens
    lanes = found.shape[1]
    swap = (z // 2) == 1

    first = [
        pltpu.make_async_copy(ids, id_smem, sems.at[0]),
        pltpu.make_async_copy(table, rows, sems.at[1]),
    ]
    for copy in first:
        copy.start()

    def pieces(p, h, base):
        at = pl.ds(h * HEAD_DIM, HEAD_DIM)
        moves = [
            (ck.at[:, at], p.at[0:cache, 0:HEAD_DIM]),
            (cv.at[:, at], p.at[0:cache, HEAD_DIM:]),
            (nk.at[:, at], p.at[cache:span, 0:HEAD_DIM]),
            (nv.at[:, at], p.at[cache:span, HEAD_DIM:]),
        ]
        for part in range(wide // width):
            lo = h * wide + part * width
            moves.append((q.at[:, pl.ds(lo, width)], p.at[span + part * tokens : span + (part + 1) * tokens, :]))
        return [pltpu.make_async_copy(src, dst, sems.at[base + i]) for i, (src, dst) in enumerate(moves)]

    count = 4 + wide // width

    @pl.when(jnp.logical_not(swap))
    def _():
        for copy in pieces(p0, 0, 2) + pieces(p1, 1, 2 + count):
            copy.start()

    @pl.when(swap)
    def _():
        for copy in pieces(p0, 1, 2) + pieces(p1, 0, 2 + count):
            copy.start()

    for copy in first:
        copy.wait()
    lane = iota((1, lanes), 1)
    for t in range(tokens):
        at = id_smem[t]
        row = rows[pl.ds(lax.shift_right_logical(at, lanes.bit_length() - 1), 1), :]
        found[t : t + 1, :] = jnp.where(lane == (at & (lanes - 1)), row, 0)
    here, there = iota((tokens, tokens), 0), iota((tokens, tokens), 1)
    who = jnp.sum(found[...].astype(f32), axis=1, keepdims=True)
    who_row = jnp.sum(jnp.where(here == there, who, 0.0), axis=0, keepdims=True)
    ahead = jnp.where((who == who_row) & (here < there), 1.0, 0.0)
    marks = who_row * cap + jnp.sum(ahead, axis=0, keepdims=True)
    for p in (p0, p1):
        p[top:, :tokens] = jnp.broadcast_to(marks, (p.shape[0] - top, tokens)).astype(bf16)
    for copy in pieces(p0, 0, 2) + pieces(p1, 1, 2 + count):
        copy.wait()


def fetch_kernel(wg, wu, wd, gain, og, ou, od, ogain, sems):
    copies = [
        pltpu.make_async_copy(src, dst, sems.at[i])
        for i, (src, dst) in enumerate(((wg, og), (wu, ou), (wd, od), (gain, ogain)))
    ]
    for copy in copies:
        copy.start()
    for copy in copies:
        copy.wait()


def units(heads):
    over_z = [(j, h) for j in range(2) for h in range(heads - 1)]
    return over_z, [(j, heads - 1) for j in range(2)]


def attend_kernel(cache, tokens, offset, r0, r1, s0, s1, za, xb0, xb1, xb2, xb3, route, held):
    z, e = lax.axis_index("ctx"), lax.axis_index("exp")
    core = e % 2
    span = cache + tokens
    cap = tokens // 2
    width = r0.shape[1]
    group = HEADS // KV_HEADS
    per_row = width // HEAD_DIM
    top = span + (group // per_row) * tokens
    limit = offset[0:1, 0:1]
    scale = math.log2(math.e) / math.sqrt(HEAD_DIM)
    halves = (z % 2, 1 - z % 2)
    keys = [(r, 2 * hi + core) for r, hi in zip((r0, r1), halves)]
    keys += [(s, 2 * hi + 1 - core) for s, hi in zip((s0, s1), halves)]
    rows = group * tokens
    pos = iota((rows, span), 0) % tokens
    col = iota((rows, span), 1)
    for ref, block in keys:
        route[block] = ref[top:, :tokens].astype(f32)
    for r, hi in zip((r0, r1), halves):
        base = (2 * hi + core) * tokens
        q = jnp.concatenate(
            [
                r[span + (g // per_row) * tokens : span + (g // per_row + 1) * tokens,
                  (g % per_row) * HEAD_DIM : (g % per_row + 1) * HEAD_DIM]
                for g in range(group)
            ],
            axis=0,
        )
        scores = []
        for ref, block in keys:
            s = dot_nt(q, ref[0:span, 0:HEAD_DIM]) * scale
            edge = jnp.where(col < cache, limit - block * cache, pos + (base - block * tokens + cache + 1))
            scores.append(jnp.where(col < edge, s, masked_score))
        peak = functools.reduce(jnp.maximum, [jnp.max(s, axis=1, keepdims=True) for s in scores])
        total = jnp.zeros((rows, 1), f32)
        weights = []
        for s in scores:
            w = jnp.exp2(s - peak)
            total += jnp.sum(w, axis=1, keepdims=True)
            weights.append(w.astype(bf16))
        numer = sum(dot(w, ref[0:span, HEAD_DIM:]) for (ref, _), w in zip(keys, weights))
        out = (numer / total).astype(bf16)
        held[hi] = jnp.concatenate([out[g * tokens : (g + 1) * tokens] for g in range(group)], axis=1)
    over_z, over_x = units(group)
    for u, (j, h) in enumerate(over_z):
        za[u] = held[j, :, h * HEAD_DIM : (h + 1) * HEAD_DIM]
    for m, xb in enumerate((xb0, xb1, xb2, xb3)):
        for j in range(2):
            pick = expert_rows(route[2 * j + core][0:1], (e ^ m) * cap, cap)
            got = dot(pick, held[j]).astype(bf16)
            for u, (i, h) in enumerate(over_x + over_z):
                if i == j:
                    xb[u] = got[:, h * HEAD_DIM : (h + 1) * HEAD_DIM]


def join_kernel(b0, b1, b2, b3, d):
    e = lax.axis_index("exp")
    for m, b in enumerate((b0, b1, b2, b3)):
        d[e ^ m] = b[0 : d.shape[1]]


def regroup_kernel(route, a1, a2, a3, c0, c1, c2, c3):
    e = lax.axis_index("exp")
    core = e % 2
    cap = c0.shape[2]
    over_z, _ = units(HEADS // KV_HEADS)
    for j in range(2):
        marks = route[2 * j + core][0:1]
        pick = jnp.concatenate([expert_rows(marks, (e ^ m) * cap, cap) for m in range(4)], axis=0)
        for u, (i, _) in enumerate(over_z):
            if i == j:
                for n, a in enumerate((a1, a2, a3)):
                    got = dot(pick, a[u]).astype(bf16)
                    for m, c in enumerate((c0, c1, c2, c3)):
                        c[n, u] = got[m * cap : (m + 1) * cap]


def lanes_of(h):
    return slice(h * HEAD_DIM, (h + 1) * HEAD_DIM)


def half_kernel(c0, c1, b0, b1, gain, wg, wu, gate, upper, square, xh):
    z, e = lax.axis_index("ctx"), lax.axis_index("exp")
    slices, blocks, cap, part = xh.shape
    rows = blocks * cap
    over_z, over_x = units(HEADS // KV_HEADS)
    wide = gain.shape[1] // KV_HEADS
    for m, (c, b) in enumerate(((c0, b0), (c1, b1))):
        src = e ^ m
        for u, (j, h) in enumerate(over_z):
            xh[z, 2 * j + src % 2, :, lanes_of(h)] = b[len(over_x) + u]
            for n in range(1, slices):
                xh[z ^ n, 2 * j + src % 2, :, lanes_of(h)] = c[n - 1, u]
    total, g, u = 0.0, 0.0, 0.0
    for n in range(slices):
        v = xh[n].reshape(rows, part).astype(f32)
        total += jnp.sum(v * v, axis=1, keepdims=True)
        at = pl.ds(pl.multiple_of((slices * (e // 2) + n) * wide, wide), part)
        x = (v * gain[0:1, at]).astype(bf16)
        g += dot_nt(x, wg[:, at])
        u += dot_nt(x, wu[:, at])
    gate[...] = g
    upper[...] = u
    square[...] = jnp.broadcast_to(total, square.shape)


def expert_kernel(
    gate, upper, square, xh, c2, c3, b2, b3, d0, d1, d2, d3, gain, wg, wu, wd,
    y0, y1, y2, y3, t0, t1, t2, t3, xo, xd, nz, sc, ys,
):
    z, e = lax.axis_index("ctx"), lax.axis_index("exp")
    slices, blocks, cap, wide = xo.shape
    rows = blocks * cap
    over_z, over_x = units(HEADS // KV_HEADS)
    mine, other = e // 2, 1 - e // 2
    part = xh.shape[3]
    for m, c, b in ((2, c2, b2), (3, c3, b3)):
        src = e ^ m
        for u, (j, h) in enumerate(over_z):
            xo[z, 2 * j + src % 2, :, lanes_of(h)] = b[len(over_x) + u]
            for n in range(1, slices):
                xo[z ^ n, 2 * j + src % 2, :, lanes_of(h)] = c[n - 1, u]
    for m, d in enumerate((d0, d1, d2, d3)):
        for k in range(2):
            for u, (j, _) in enumerate(over_x):
                xo[z ^ m, 2 * j + k, :, part:] = d[2 * other + k, u]
                xd[z ^ m, 2 * j + k] = d[2 * mine + k, u]
    total, g, u = square[:, 0:1], gate[...], upper[...]
    for x, first, side in ((xo, 0, other), (xd, part, mine)):
        width = x.shape[3]
        for n in range(slices):
            v = x[n].reshape(rows, width).astype(f32)
            total += jnp.sum(v * v, axis=1, keepdims=True)
            at = pl.ds(pl.multiple_of((slices * side + n) * wide + first, HEAD_DIM), width)
            r = (v * gain[0:1, at]).astype(bf16)
            g += dot_nt(r, wg[:, at])
            u += dot_nt(r, wu[:, at])
    scale = lax.rsqrt(total * (1.0 / gain.shape[1]) + 1e-05)
    sc[...] = jnp.broadcast_to(scale, sc.shape)
    g, u = g * scale, u * scale
    hidden = (g / (1.0 + jnp.exp(-g)) * u).astype(bf16)
    own_scale = sc[pl.ds(pl.multiple_of(z * cap, cap), cap), 0:1]
    for n in range(slices):
        for x, first, side in ((xo, 0, other), (xh, 0, mine), (xd, part, mine)):
            width = x.shape[3]
            s = slices * side + n
            at = pl.ds(pl.multiple_of(s * wide + first, HEAD_DIM), width)
            v = x[n, z].astype(f32) * own_scale * gain[0:1, at]
            nz[s, :, first : first + width] = v.astype(bf16)
    span, keep = ys.shape[1] + y0.shape[1], y0.shape[1]
    per = span // wide
    at_home = iota((rows, span), 0) // cap == z
    for m, y in enumerate((y0, y1, y2, y3)):
        o = e ^ m
        v = dot(hidden, wd[:, pl.ds(pl.multiple_of(o * span, span), span)])
        normed = jnp.concatenate([nz[o * per + i] for i in range(per)], axis=1).astype(f32)
        v = (v + jnp.where(at_home, jnp.concatenate([normed] * blocks, axis=0), 0.0)).astype(bf16)
        y[...] = v[:, :keep]
        ys[...] = v[:, keep:]
        for i, t in enumerate((t0, t1, t2, t3)):
            t[o] = ys[pl.ds(pl.multiple_of((z ^ i) * cap, cap), cap), :]


def turn_kernel(route, y0, y1, y2, y3, g0, g1, g2, g3):
    z, e = lax.axis_index("ctx"), lax.axis_index("exp")
    cap = y0.shape[0] // 4
    for m, g in enumerate((g0, g1, g2, g3)):
        block = z ^ m
        marks = route[block][0:1]
        pick = jnp.concatenate([expert_rows(marks, (e ^ n) * cap, cap) for n in range(4)], axis=0)
        at = pl.ds(pl.multiple_of(block * cap, cap), cap)
        got = jnp.concatenate([y[at, :] for y in (y0, y1, y2, y3)], axis=0)
        g[...] = dot_tn(pick, got).astype(bf16)


def total_kernel(t0, t1, t2, t3, h0, h1, h2, h3, ts):
    e = lax.axis_index("exp")
    ts[...] = sum(t[...].astype(f32) for t in (t0, t1, t2, t3)).astype(bf16)
    for m, h in enumerate((h0, h1, h2, h3)):
        h[...] = ts[e ^ m]


def final_kernel(route, g0, g1, g2, g3, h0, h1, h2, h3, out):
    z, e = lax.axis_index("ctx"), lax.axis_index("exp")
    cap = h0.shape[0]
    keep = g0.shape[1]
    out[:, 0:keep] = sum(g[...].astype(f32) for g in (g0, g1, g2, g3)).astype(bf16)
    marks = route[z][0:1]
    pick = jnp.concatenate([expert_rows(marks, (e ^ n) * cap, cap) for n in range(4)], axis=0)
    got = jnp.concatenate([h[...] for h in (h0, h1, h2, h3)], axis=0)
    out[:, keep:] = dot_tn(pick, got).astype(bf16)


def paired_path(*args):
    return paired_steps(*args)


def paired_steps(
    queries,
    new_keys,
    new_values,
    cache_keys,
    cache_values,
    offset,
    token_ids,
    expert_table,
    norm_gain,
    w_gate,
    w_up,
    w_down,
):
    n_ctx, n_exp = lax.axis_size("ctx"), lax.axis_size("exp")
    tokens = queries.shape[0]
    cache = cache_keys.shape[0]
    width = new_keys.shape[1]
    group = HEADS // KV_HEADS
    wide = group * HEAD_DIM
    cap = tokens // 2
    span = cache + tokens
    over_z, over_x = units(group)
    own = queries.shape[1]
    back = own * 3 // 8
    keep = own - back
    rows = n_ctx * cap

    def over_ctx(v, m):
        return lax.ppermute(v, "ctx", [(i, i ^ m) for i in range(n_ctx)])

    def over_exp(v, m):
        return lax.ppermute(v, "exp", [(i, i ^ m) for i in range(n_exp)])

    def head_step(v, o):
        pairs = []
        for z in range(n_ctx):
            for e in range(n_exp):
                core = e % 2
                to_z = 2 * core + ((z // 2) ^ o)
                pairs.append((z * n_exp + e, to_z * n_exp + e - core + z % 2))
        return lax.ppermute(v, ("ctx", "exp"), pairs)

    height = span + tokens * wide // width + 8
    copies = 2 + 2 * (4 + wide // width)
    table_rows = expert_table.reshape(-1, 128)
    p0, p1 = call(
        pack_kernel,
        [((height, width), bf16)] * 2,
        8,
        scratch=[
            pltpu.SMEM((tokens,), jnp.int32),
            pltpu.VMEM(table_rows.shape, jnp.int32),
            pltpu.VMEM((tokens, table_rows.shape[1]), jnp.int32),
            pltpu.SemaphoreType.DMA((copies,)),
        ],
        hbm=7,
    )(queries, new_keys, new_values, cache_keys, cache_values, token_ids, table_rows)
    limit = jnp.broadcast_to(offset[None, :], (8, 128))
    gate_t, up_t, down = jnp.swapaxes(w_gate[0], 0, 1), jnp.swapaxes(w_up[0], 0, 1), w_down[0]
    weight_bytes = 2 * (gate_t.size + up_t.size + down.size)
    gate_t, up_t, down, gain = call(
        fetch_kernel,
        [(w.shape, bf16) for w in (gate_t, up_t, down)] + [((1, norm_gain.shape[0]), f32)],
        4,
        scratch=[pltpu.SemaphoreType.DMA((4,))],
        hbm=4,
        cost=pl.CostEstimate(flops=1000 * weight_bytes, transcendentals=0, bytes_accessed=2 * weight_bytes),
    )(gate_t, up_t, down, norm_gain.reshape(1, -1))
    r0, r1 = head_step(p0, 0), head_step(p1, 1)
    r1, limit = lax.optimization_barrier((r1, limit))
    s0, s1 = over_exp(r0, 1), over_exp(r1, 1)
    za, xb0, xb1, xb2, xb3, route = call(
        functools.partial(attend_kernel, cache, tokens),
        [((len(over_z), tokens, HEAD_DIM), bf16)]
        + [((2 * group, cap, HEAD_DIM), bf16)] * 4
        + [((n_ctx, 8, tokens), f32)],
        16,
        scratch=[pltpu.VMEM((2, tokens, wide), bf16)],
    )(limit, r0, r1, s0, s1)
    a = [za] + [over_ctx(za, m) for m in (1, 2, 3)]
    b = [xb0] + [over_exp(v, m) for m, v in ((1, xb1), (2, xb2), (3, xb3))]
    (zd,) = call(join_kernel, [((n_exp, len(over_x), cap, HEAD_DIM), bf16)], 4)(*b)
    d = [zd] + [over_ctx(zd, m) for m in (1, 2, 3)]
    c0, c1, c2, c3 = call(
        regroup_kernel, [((n_ctx - 1, len(over_z), cap, HEAD_DIM), bf16)] * 4, 8
    )(route, *a[1:])
    c = [c0] + [over_exp(v, m) for m, v in ((1, c1), (2, c2), (3, c3))]
    units_hidden = gate_t.shape[0]
    part = wide - HEAD_DIM
    gate, upper, square, xh = call(
        half_kernel,
        [((rows, units_hidden), f32)] * 2 + [((rows, 128), f32), ((n_ctx, n_ctx, cap, part), bf16)],
        20,
        cost=pl.CostEstimate(flops=2 * rows * units_hidden * n_ctx * part * 2, transcendentals=0, bytes_accessed=0),
    )(c[0], c[1], b[0], b[1], gain, gate_t, up_t)
    outs = call(
        expert_kernel,
        [((rows, keep), bf16)] * 4 + [((n_exp, cap, back), bf16)] * 4,
        28,
        scratch=[
            pltpu.VMEM((n_ctx, n_ctx, cap, wide), bf16),
            pltpu.VMEM((n_ctx, n_ctx, cap, HEAD_DIM), bf16),
            pltpu.VMEM((KV_HEADS, cap, wide), bf16),
            pltpu.VMEM((rows, 128), f32),
            pltpu.VMEM((rows, back), bf16),
        ],
    )(gate, upper, square, xh, c[2], c[3], b[2], b[3], *d, gain, gate_t, up_t, down)
    y, t = outs[:4], outs[4:]
    t = [t[0]] + [over_ctx(t[m], m) for m in (1, 2, 3)]
    y = [y[0]] + [over_exp(y[m], m) for m in (1, 2, 3)]
    g = call(turn_kernel, [((tokens, keep), bf16)] * 4, 8)(route, *y)
    g = [g[0]] + [over_ctx(g[m], m) for m in (1, 2, 3)]
    h = call(
        total_kernel, [((cap, back), bf16)] * 4, 8, scratch=[pltpu.VMEM((n_exp, cap, back), bf16)]
    )(*t)
    h = [h[0]] + [over_exp(h[m], m) for m in (1, 2, 3)]
    (out,) = call(final_kernel, [((tokens, own), bf16)], 8)(route, *g, *h)
    return out


def solution(mesh):
    placed = (
        P(("group", "ctx"), "exp"),
        P(("group", "ctx"), "exp"),
        P(("group", "ctx"), "exp"),
        P(("group", "ctx"), "exp"),
        P(("group", "ctx"), "exp"),
        P("group"),
        P(("group", "ctx")),
        P("group"),
        P(),
        P("exp", None, "ctx"),
        P("exp", None, "ctx"),
        P("exp", "ctx", None),
    )
    n_ctx, n_exp = mesh.shape["ctx"], mesh.shape["exp"]
    paired = n_ctx == n_exp == 4 and KV_HEADS == 2 * n_exp
    return jax.shard_map(
        paired_path if paired else general_path,
        mesh=mesh,
        in_specs=placed,
        out_specs=P(("group", "ctx"), "exp"),
        check_vma=False,
    )
```
